256 devices in a mesh: groups: 2 (over z), expert: 64 (over x, y), replica: 2 (over core).
Axes of the slice: x: 8, y: 8, z: 2, core: 2. Of those that a mesh axis runs over, the one named last changes fastest.
The devices are a block of a 8x8x16 slice.
Arguments:
- queries: bfloat16 [1024, 8192], P(('groups', 'expert', 'replica')), parts along dimension 0, may hold values from -250 to 250
- token_keys: bfloat16 [1024, 512], P(('groups', 'expert', 'replica')), parts along dimension 0, may hold values from -6 to 6
- token_values: bfloat16 [1024, 512], P(('groups', 'expert', 'replica')), parts along dimension 0, may hold values from -6 to 6
- stored_keys: bfloat16 [1024, 256, 512], P(('groups', 'expert', 'replica')), parts along dimension 0, may hold values from -7 to 7
- stored_values: bfloat16 [1024, 256, 512], P(('groups', 'expert', 'replica')), parts along dimension 0, may hold values from -6 to 6
- kv_len: int32 [1024], P(('groups', 'expert', 'replica')), parts along dimension 0, may hold values from 2 to 256, as said below
- residual: bfloat16 [1024, 4096], P(('groups', 'expert', 'replica')), parts along dimension 0, may hold values from -6 to 6
- out_weight: bfloat16 [8192, 4096], P(('expert', 'replica')), may hold values from -0.1875 to 0.1875
- norm_gain: bfloat16 [4096], replicated, may hold values from 0.25 to 1.75
- expert_ids: int32 [1024, 8], P(('groups', 'expert')), parts along dimension 0, may hold values from 0 to 63, all different within a row; in each aligned block of 8 rows (0 to 7, 8 to 15, ...) at most 2 rows name the same one
- route_weight: float32 [1024, 8], P(('groups', 'expert')), parts along dimension 0, may hold values from 0.05 to 1
- w_gate: bfloat16 [64, 4096, 768], P('expert', None, 'replica'), may hold values from -0.09375 to 0.09375
- w_up: bfloat16 [64, 4096, 768], P('expert', None, 'replica'), may hold values from -0.09375 to 0.09375
- w_down: bfloat16 [64, 768, 4096], P('expert', 'replica'), may hold values from -0.4375 to 0.4375
Outputs:
- updated: bfloat16 [1024, 4096], P(('groups', 'expert', 'replica')), parts along dimension 0
The draws below stay inside these ranges and needn't reach their ends.
There are 2 independent parts, one for each index of `groups`. The reference program is written for one: setup_inputs(seed, part) draws one part's arguments, and reference() takes and returns one part's arrays. A program takes and returns all parts, laid end to end along the dimension named above; an argument that names none is the same for every part. Nothing has to cross between parts.
Inputs may be any that keep to these rules, and one draw needn't show every extreme that they name: `kv_len`: at least 2; some sequence uses all 256 positions. `expert_ids`: each token names 8 different experts; in each aligned block of 8 tokens no expert is named by more than 2 tokens, and some block reaches it.
All inputs are finite; a program needn't handle non-finite values.
Results may differ from the reference program's by a relative error of at most 0.01.
Values may be sent and summed in bfloat16 or wider, within the bound.
No kernel may reach another device: no remote copies, remote signals or barrier semaphores. Data moves between devices by JAX's collectives and lax.ppermute only.
A program may use at most 64 MiB of HBM per device.

```python
import math
import jax
import jax.numpy as jnp
import numpy as np
from jax import lax

D = 4096
QUERY_HEADS = 64
KEY_VALUE_HEADS = 4
HEAD_WIDTH = 128
FF = 768
TOPK = 8
SEQ_DEV = 4
CACHE_POSITIONS = 256
EXPERTS = 64
SEQUENCE_TOTAL = 512
MOST = 2
N_EXPERT = 64
N_REPLICA = 2


def key_lookup(key):
    return jnp.clip(jax.random.normal(jax.random.fold_in(key, 11), (SEQUENCE_TOTAL, CACHE_POSITIONS, KEY_VALUE_HEADS * HEAD_WIDTH), jnp.float32), -6.0, 6.0)


def draw_queries(key, part):
    base = jnp.clip(jax.random.normal(jax.random.fold_in(key, 5), (SEQUENCE_TOTAL, QUERY_HEADS * HEAD_WIDTH), jnp.float32), -6.0, 6.0)
    return base.astype(jnp.bfloat16)


def draw_stored_keys(key, part):
    table = key_lookup(key)
    return table.astype(jnp.bfloat16)


def draw_kv_len(key, part):
    lengths = jax.random.randint(jax.random.fold_in(key, 3), (SEQUENCE_TOTAL,), 2, CACHE_POSITIONS + 1, jnp.int32)
    chosen = jax.random.randint(jax.random.fold_in(key, 4), (), 0, SEQUENCE_TOTAL, jnp.int32)
    return jnp.where(jnp.arange(SEQUENCE_TOTAL, dtype=jnp.int32) == chosen, CACHE_POSITIONS, lengths).astype(jnp.int32)


def shard_levels(own_key, shape, cuts, least, high):
    gain, own = 1.0, jax.random.fold_in(own_key, 6)
    for dim, parts in cuts:
        heights = jnp.exp(jax.random.uniform(jax.random.fold_in(own, dim), (parts,), jnp.float32, least / len(cuts), high / len(cuts)))
        gain = gain * jnp.repeat(heights, shape[dim] // parts).reshape([-1 if axis == dim else 1 for axis in range(len(shape))])
    return gain


def shared_out(own_key, own, number, rows, number_of, top, most, slope):
    ranking = jax.random.permutation(own_key, number_of)
    heavy_load, common = portions_of(number_of, rows * top, most, slope, True), portions_of(number_of, rows * top, most, slope, False)
    places = jnp.arange(number_of)

    def named(tallies, turn):
        used = int((tallies > 0).sum())
        fixed = max(1, used // 4)
        shifted = fixed + (places - fixed + turn * (used - fixed)) % max(1, number_of - fixed)
        return jnp.zeros((number_of,), jnp.int32).at[ranking[jnp.where(places < fixed, places, shifted)]].set(jnp.asarray(tallies, jnp.int32))

    tallies = jnp.where(number % 4 == 0, named(heavy_load, number // 4), named(common, number - number // 4 - 1))
    mixed = jax.random.permutation(jax.random.fold_in(own, 3), number_of)
    donor, receiver = mixed[0:number_of // 2 * 2:2], mixed[1:number_of // 2 * 2:2]
    margin = jnp.minimum(tallies[donor] - 1, most - tallies[receiver]) // 2
    margin = jnp.where((donor == ranking[0]) | (receiver == ranking[0]) | (tallies[receiver] == 0), 0, jnp.maximum(margin, 0))
    shifted = jax.random.randint(jax.random.fold_in(own, 4), (number_of // 2,), 0, 1 << 20) % (margin + 1)
    tallies = tallies.at[donor].add(-shifted).at[receiver].add(shifted)
    items = jnp.searchsorted(jnp.cumsum(tallies), jnp.arange(rows * top), side="right").astype(jnp.int32)
    listing = items.reshape(top, rows).T
    listing = listing[jax.random.permutation(jax.random.fold_in(own, 1), rows)]
    turn = jax.random.randint(jax.random.fold_in(own, 2), (rows, 1), 0, top)
    return jnp.take_along_axis(listing, (jnp.arange(top)[None, :] + turn) % top, axis=1)


def portions_of(number_of, total, limit, lean, full):
    portions = [(1 << 20) // math.isqrt(grade ** lean) + 1 for grade in range(1, number_of + 1)]
    largest = limit if full else min(limit, max(-(-total // number_of), total * portions[0] // sum(portions)))
    least = 1 if total - largest >= number_of - 1 else 0
    given, rest = [largest] + [least] * (number_of - 1), total - largest - least * (number_of - 1)
    while rest > 0:
        movable = [i for i in range(1, number_of) if given[i] < largest] or [i for i in range(1, number_of) if given[i] < limit]
        whole, remaining = sum([portions[i] for i in movable]), rest
        for i in movable:
            addition = min(limit - given[i], max(1, remaining * portions[i] // whole), rest)
            given[i] = given[i] + addition
            rest = rest - addition
    return np.array(given)


def normal_values(key, shape, width, reach, pieces=(), held_as=jnp.bfloat16):
    entries = width * jax.random.normal(key, shape, jnp.float32)
    if pieces:
        entries = entries * shard_levels(key, shape, pieces, -0.22, 0.18)
    return jnp.clip(entries, -reach, reach).astype(held_as)


def setup_inputs(seed: int = 0, part: int = 0) -> dict:
    key_list = jax.random.split(jax.random.key(seed), 15)
    part_splits = jax.random.split(jax.random.fold_in(key_list[14], part), 15)
    queries = draw_queries(jax.random.fold_in(jax.random.fold_in(key_list[14], part), 71), part)
    token_keys = normal_values(part_splits[1], (SEQUENCE_TOTAL, KEY_VALUE_HEADS * HEAD_WIDTH), 1.0, 6.0, ((0, 128),))
    token_values = normal_values(part_splits[2], (SEQUENCE_TOTAL, KEY_VALUE_HEADS * HEAD_WIDTH), 1.0, 6.0, ((0, 128),))
    stored_keys = draw_stored_keys(jax.random.fold_in(jax.random.fold_in(key_list[14], part), 71), part)
    stored_values = normal_values(part_splits[4], (SEQUENCE_TOTAL, CACHE_POSITIONS, KEY_VALUE_HEADS * HEAD_WIDTH), 1.0, 6.0, ((0, 128),))
    kv_len = draw_kv_len(jax.random.fold_in(jax.random.fold_in(key_list[14], part), 71), part)
    residual = normal_values(part_splits[6], (SEQUENCE_TOTAL, D), 1.0, 6.0, ((0, 128),))
    out_weight = normal_values(key_list[7], (QUERY_HEADS * HEAD_WIDTH, D), (QUERY_HEADS * HEAD_WIDTH // 8) ** -0.5, 0.1875, ((0, 128),))
    norm_gain = jnp.clip(1.0 + 0.15 * jax.random.normal(key_list[8], (D,), jnp.float32), 0.25, 1.75).astype(jnp.bfloat16)
    expert_ids_keys = jax.random.split(jax.random.fold_in(part_splits[9], 1), SEQUENCE_TOTAL // (N_REPLICA * SEQ_DEV))
    expert_ids_turns = jax.random.permutation(jax.random.fold_in(part_splits[9], 3), SEQUENCE_TOTAL // (N_REPLICA * SEQ_DEV))
    expert_ids = jax.vmap(lambda own, number: shared_out(jax.random.fold_in(part_splits[9], 2), own, number, N_REPLICA * SEQ_DEV, EXPERTS, TOPK, MOST, 2))(expert_ids_keys, expert_ids_turns).reshape((SEQUENCE_TOTAL, TOPK))
    route_weight = jnp.clip(jnp.exp(math.log(1.0) - 2.9957323 * jax.random.uniform(part_splits[10], (SEQUENCE_TOTAL, TOPK), jnp.float32) ** shard_levels(part_splits[10], (SEQUENCE_TOTAL, TOPK), ((0, 64),), -0.2, 0.2)), 0.05, 1.0)
    w_gate = normal_values(key_list[11], (EXPERTS, D, FF), D ** -0.5, 0.09375, ((0, 64), (2, 2)))
    w_up = normal_values(key_list[12], (EXPERTS, D, FF), D ** -0.5, 0.09375, ((0, 64), (2, 2)))
    w_down = normal_values(key_list[13], (EXPERTS, FF, D), (FF // 4) ** -0.5, 0.4375, ((0, 64), (1, 2)))
    return dict(queries=queries, token_keys=token_keys, token_values=token_values, stored_keys=stored_keys, stored_values=stored_values, kv_len=kv_len, residual=residual, out_weight=out_weight, norm_gain=norm_gain, expert_ids=expert_ids, route_weight=route_weight, w_gate=w_gate, w_up=w_up, w_down=w_down)


def attend(queries, token_keys, token_values, stored_keys, stored_values, kv_len):
    sequence_rows = queries.shape[0]
    query_group_width = QUERY_HEADS // KEY_VALUE_HEADS
    query_head_rows = queries.astype(jnp.float32).reshape(sequence_rows, KEY_VALUE_HEADS, query_group_width, HEAD_WIDTH)
    keys_from_cache = stored_keys.astype(jnp.float32).reshape(sequence_rows, CACHE_POSITIONS, KEY_VALUE_HEADS, HEAD_WIDTH)
    values_from_cache = stored_values.astype(jnp.float32).reshape(sequence_rows, CACHE_POSITIONS, KEY_VALUE_HEADS, HEAD_WIDTH)
    keys_latest = token_keys.astype(jnp.float32).reshape(sequence_rows, KEY_VALUE_HEADS, HEAD_WIDTH)
    values_latest = token_values.astype(jnp.float32).reshape(sequence_rows, KEY_VALUE_HEADS, HEAD_WIDTH)
    inv_root = 1.0 / math.sqrt(HEAD_WIDTH)
    cached_scores = jnp.einsum('bgqd,bpgd->bgqp', query_head_rows, keys_from_cache) * inv_root
    positions = jnp.arange(CACHE_POSITIONS, dtype=jnp.int32)
    visible = positions[None, :] < kv_len[:, None]
    cached_scores = jnp.where(visible[:, None, None, :], cached_scores, -jnp.inf)
    fresh_score = jnp.einsum('bgqd,bgd->bgq', query_head_rows, keys_latest) * inv_root
    highest = jnp.maximum(lax.optimization_barrier(jnp.max(cached_scores, axis=-1)), fresh_score)
    cached_exp = jnp.exp(cached_scores - highest[..., None])
    fresh_exp = jnp.exp(fresh_score - highest)
    totals = lax.optimization_barrier(jnp.sum(cached_exp, axis=-1)) + fresh_exp
    cached_prob = lax.optimization_barrier((cached_exp / totals[..., None]).astype(jnp.bfloat16)).astype(jnp.float32)
    fresh_prob = lax.optimization_barrier((fresh_exp / totals).astype(jnp.bfloat16)).astype(jnp.float32)
    mixed = jnp.einsum('bgqp,bpgd->bgqd', cached_prob, values_from_cache)
    mixed = mixed + fresh_prob[..., None] * values_latest[:, :, None, :]
    return mixed.reshape(sequence_rows, QUERY_HEADS * HEAD_WIDTH).astype(jnp.bfloat16)

def reference(queries, token_keys, token_values, stored_keys, stored_values, kv_len, residual, out_weight, norm_gain, expert_ids, route_weight, w_gate, w_up, w_down):
    attended = attend(queries, token_keys, token_values, stored_keys, stored_values, kv_len)
    hidden_state = residual.astype(jnp.float32) + jnp.dot(attended, out_weight, preferred_element_type=jnp.float32)
    mean_square = lax.optimization_barrier(jnp.mean(hidden_state * hidden_state, axis=-1, keepdims=True))
    normed = (hidden_state * lax.rsqrt(mean_square + 1e-06) * norm_gain.astype(jnp.float32)).astype(jnp.bfloat16)
    mixing = route_weight / lax.optimization_barrier(jnp.sum(route_weight, axis=1, keepdims=True))
    flat_ids = expert_ids.reshape(-1).astype(jnp.int32)
    row_total = flat_ids.shape[0]
    sorted_rows = jnp.argsort(flat_ids, stable=True).astype(jnp.int32)
    member = flat_ids[None, :] == jnp.arange(EXPERTS, dtype=jnp.int32)[:, None]
    counts = lax.optimization_barrier(jnp.sum(member.astype(jnp.int32), axis=1)).astype(jnp.int32)
    starts = (jnp.cumsum(counts) - counts).astype(jnp.int32)
    capacity = MOST * N_EXPERT

    def one_expert(expert):
        offsets = jnp.arange(capacity, dtype=jnp.int32)
        taken_rows = sorted_rows[jnp.clip(starts[expert] + offsets, 0, row_total - 1)]
        alive_slot = offsets < counts[expert]
        inputs = normed[taken_rows // TOPK]
        gate_act = jnp.dot(inputs, w_gate[expert], preferred_element_type=jnp.float32)
        up_act = jnp.dot(inputs, w_up[expert], preferred_element_type=jnp.float32)
        hidden_act = (jax.nn.silu(gate_act) * up_act).astype(jnp.bfloat16)
        output = jnp.dot(hidden_act, w_down[expert], preferred_element_type=jnp.float32)
        return (jnp.where(alive_slot[:, None], output, 0.0), taken_rows)
    outputs, taken_all = lax.map(one_expert, jnp.arange(EXPERTS, dtype=jnp.int32))
    weights = mixing.reshape(-1)[taken_all]
    moe_out = jnp.zeros((SEQUENCE_TOTAL, D), jnp.float32).at[(taken_all // TOPK).reshape(-1)].add((weights[..., None] * outputs).reshape(-1, D))
    return (hidden_state + moe_out).astype(jnp.bfloat16)
```

```python
import math

import jax
import jax.numpy as jnp
from jax import lax
from jax.sharding import PartitionSpec as P

HEAD_WIDTH = 128
CHIPS, CORES = "expert", "replica"


def swapped(x):
    return lax.ppermute(x, CORES, [(0, 1), (1, 0)])


def by_core(core, own, other, axis):
    return jnp.where(
        core == 0,
        jnp.concatenate([own, other], axis=axis),
        jnp.concatenate([other, own], axis=axis),
    )


def attend_local(queries, token_keys, token_values, stored_keys, stored_values, kv_len):
    seq_count = queries.shape[0]
    cache_len = stored_keys.shape[1]
    kv_count = token_keys.shape[1] // HEAD_WIDTH
    query_group_width = queries.shape[1] // HEAD_WIDTH // kv_count
    query_head_rows = queries.reshape(seq_count, kv_count, query_group_width, HEAD_WIDTH)
    keys_from_cache = stored_keys.reshape(seq_count, cache_len, kv_count, HEAD_WIDTH)
    values_from_cache = stored_values.reshape(seq_count, cache_len, kv_count, HEAD_WIDTH)
    keys_latest = token_keys.reshape(seq_count, kv_count, HEAD_WIDTH)
    values_latest = token_values.astype(jnp.float32).reshape(seq_count, kv_count, HEAD_WIDTH)
    inv_root = 1.0 / math.sqrt(HEAD_WIDTH)
    cached_scores = (
        jnp.einsum(
            "bgqd,bpgd->bgqp", query_head_rows, keys_from_cache, preferred_element_type=jnp.float32
        )
        * inv_root
    )
    positions = lax.broadcasted_iota(jnp.int32, (seq_count, cache_len), 1)
    visible = positions < kv_len[:, None]
    cached_scores = jnp.where(visible[:, None, None, :], cached_scores, -jnp.inf)
    fresh_score = (
        jnp.einsum(
            "bgqd,bgd->bgq", query_head_rows, keys_latest, preferred_element_type=jnp.float32
        )
        * inv_root
    )
    highest = jnp.maximum(jnp.max(cached_scores, axis=-1), fresh_score)
    cached_exp = jnp.exp(cached_scores - highest[..., None])
    fresh_exp = jnp.exp(fresh_score - highest)
    totals = jnp.sum(cached_exp, axis=-1) + fresh_exp
    cached_prob = (cached_exp / totals[..., None]).astype(jnp.bfloat16)
    fresh_prob = lax.optimization_barrier((fresh_exp / totals).astype(jnp.bfloat16)).astype(
        jnp.float32
    )
    mixed = jnp.einsum(
        "bgqp,bpgd->bgqd", cached_prob, values_from_cache, preferred_element_type=jnp.float32
    )
    mixed = mixed + fresh_prob[..., None] * values_latest[:, :, None, :]
    return mixed.reshape(seq_count, -1).astype(jnp.bfloat16)


def quad_step(side, dx, dy):
    return [
        (x * side + y, (x ^ dx) * side + (y ^ dy)) for x in range(side) for y in range(side)
    ]


def on_device(
    queries,
    token_keys,
    token_values,
    stored_keys,
    stored_values,
    kv_len,
    residual,
    out_weight,
    norm_gain,
    expert_ids,
    route_weight,
    w_gate,
    w_up,
    w_down,
):
    chips = lax.axis_size(CHIPS)
    side = math.isqrt(chips)
    chip = lax.axis_index(CHIPS)
    core = lax.axis_index(CORES)
    place = (chip // side) % 2 * 2 + chip % 2
    row_count, model_width = out_weight.shape
    seq_count, feature_total = queries.shape
    col_width = model_width // 4
    half_width = model_width // 2
    pieces = []
    for d in range(4):
        piece = lax.dynamic_slice_in_dim(out_weight, (place ^ d) * col_width, col_width, 1)
        pieces.append(lax.ppermute(piece, CHIPS, quad_step(side, d // 2, d % 2)) if d else piece)
    weight_own = jnp.stack(pieces)
    weight_other = swapped(weight_own)

    attended = attend_local(queries, token_keys, token_values, stored_keys, stored_values, kv_len)
    attended = attended.reshape(seq_count, chips, 2, row_count)
    attended = jnp.where(core == 0, attended, attended[:, :, ::-1])
    squares = attended.reshape(seq_count, side // 2, 2, side // 2, 2, 2, row_count)
    squares = squares.transpose(1, 3, 0, 5, 2, 4, 6)
    by_place = jnp.stack(
        [
            jnp.stack(
                [squares[:, :, :, :, (p ^ d) // 2, (p ^ d) % 2] for d in range(4)], axis=4
            )
            for p in range(4)
        ]
    )
    by_place = by_place.reshape(2, 2, side // 2, side // 2, seq_count, -1)
    outgoing = by_place.transpose(2, 0, 3, 1, 4, 5).reshape(chips, seq_count, -1)
    tokens = lax.all_to_all(outgoing, CHIPS, 0, 0, tiled=True)
    weight = jnp.concatenate(
        [weight_own.reshape(-1, col_width), weight_other.reshape(-1, col_width)]
    )
    partial_cols = jnp.dot(
        tokens.reshape(chips * seq_count, -1), weight, preferred_element_type=jnp.float32
    ).astype(jnp.bfloat16)
    came_back = lax.all_to_all(
        partial_cols.reshape(chips, seq_count, col_width), CHIPS, 0, 0, tiled=True
    )
    came_back = came_back.reshape(side // 2, 2, side // 2, 2, seq_count, col_width)
    projected = jnp.sum(came_back.astype(jnp.float32), axis=(0, 2))
    projected = projected.transpose(2, 0, 1, 3).reshape(seq_count, model_width)
    hidden_state = residual.astype(jnp.float32) + projected
    mean_square = jnp.mean(hidden_state * hidden_state, axis=-1, keepdims=True)
    normed = (hidden_state * lax.rsqrt(mean_square + 1e-06) * norm_gain.astype(jnp.float32)).astype(
        jnp.bfloat16
    )

    token_count, topk_count = expert_ids.shape
    capacity = 2
    flat_ids = expert_ids.reshape(-1)
    row_total = flat_ids.shape[0]
    same_expert = flat_ids[:, None] == flat_ids[None, :]
    row_iota = lax.broadcasted_iota(jnp.int32, (row_total, row_total), 0)
    col_iota = lax.broadcasted_iota(jnp.int32, (row_total, row_total), 1)
    slot_ranks = jnp.sum(jnp.where(same_expert & (col_iota < row_iota), 1, 0), axis=1).astype(
        jnp.int32
    )
    slot_of = (flat_ids * capacity + slot_ranks).reshape(token_count, topk_count)
    mixing = route_weight / jnp.sum(route_weight, axis=1, keepdims=True)
    slot_of = jnp.where(core == 0, slot_of, jnp.roll(slot_of, -seq_count, axis=0))
    mixing = jnp.where(core == 0, mixing, jnp.roll(mixing, -seq_count, axis=0))
    slot_total = chips * capacity
    slot_iota = jnp.arange(slot_total, dtype=jnp.int32)
    slot_hits = slot_of[None, :, :] == slot_iota[:, None, None]
    pick_table = jnp.sum(slot_hits.astype(jnp.float32), axis=2).astype(jnp.bfloat16)
    combine_rows = jnp.sum(jnp.where(slot_hits, mixing[None, :, :], 0.0), axis=2).T

    normed_halves = normed.reshape(seq_count, 2, half_width)
    kept = jnp.where(core == 0, normed_halves[:, 0], normed_halves[:, 1])
    given = jnp.where(core == 0, normed_halves[:, 1], normed_halves[:, 0])
    pair_tokens = jnp.concatenate([kept, swapped(given)])
    dispatched = jnp.dot(pick_table, pair_tokens, preferred_element_type=jnp.float32).astype(
        jnp.bfloat16
    )
    incoming = lax.all_to_all(
        dispatched.reshape(chips, capacity, half_width), CHIPS, 0, 0, tiled=True
    )
    incoming = incoming.reshape(slot_total, half_width)
    slot_rows = by_core(core, incoming, swapped(incoming), 1)
    gate_act = jnp.dot(slot_rows, w_gate[0], preferred_element_type=jnp.float32)
    up_act = jnp.dot(slot_rows, w_up[0], preferred_element_type=jnp.float32)
    hidden_act = (jax.nn.silu(gate_act) * up_act).astype(jnp.bfloat16)
    partial_out = jnp.dot(hidden_act, w_down[0], preferred_element_type=jnp.float32)
    out_halves = partial_out.reshape(slot_total, 2, half_width)
    out_kept = jnp.where(core == 0, out_halves[:, 0], out_halves[:, 1])
    out_given = jnp.where(core == 0, out_halves[:, 1], out_halves[:, 0]).astype(jnp.bfloat16)
    expert_out = (out_kept + swapped(out_given).astype(jnp.float32)).astype(jnp.bfloat16)
    returned = lax.all_to_all(
        expert_out.reshape(chips, capacity, half_width), CHIPS, 0, 0, tiled=True
    ).reshape(slot_total, half_width)
    pair_moe = jnp.dot(
        combine_rows, returned.astype(jnp.float32), preferred_element_type=jnp.float32
    )
    moe_out = by_core(core, pair_moe[:seq_count], swapped(pair_moe[seq_count:]), 1)
    return (hidden_state + moe_out).astype(jnp.bfloat16)


def solution(mesh):
    in_specs = (
        P(("groups", "expert", "replica"), None),
        P(("groups", "expert", "replica"), None),
        P(("groups", "expert", "replica"), None),
        P(("groups", "expert", "replica"), None, None),
        P(("groups", "expert", "replica"), None, None),
        P(("groups", "expert", "replica")),
        P(("groups", "expert", "replica"), None),
        P(("expert", "replica"), None),
        P(),
        P(("groups", "expert"), None),
        P(("groups", "expert"), None),
        P("expert", None, "replica"),
        P("expert", None, "replica"),
        P("expert", "replica", None),
    )
    out_specs = P(("groups", "expert", "replica"), None)
    return jax.shard_map(
        on_device, mesh=mesh, in_specs=in_specs, out_specs=out_specs, check_vma=False
    )
```

```python
import math

import jax
import jax.numpy as jnp
from jax import lax
from jax.experimental import pallas as pl
from jax.experimental.pallas import tpu as pltpu
from jax.sharding import PartitionSpec as P

HEAD_WIDTH = 128
CHIPS, CORES = "expert", "replica"
F32, BF16 = jnp.float32, jnp.bfloat16
IN_VMEM = pl.BlockSpec(memory_space=pltpu.VMEM)
IN_SMEM = pl.BlockSpec(memory_space=pltpu.SMEM)
IN_HBM = pl.BlockSpec(memory_space=pltpu.HBM)


def swapped(x):
    return lax.ppermute(x, CORES, [(0, 1), (1, 0)])


def quad_step(side, dx, dy):
    return [
        (x * side + y, (x ^ dx) * side + (y ^ dy)) for x in range(side) for y in range(side)
    ]


MIB = 1 << 20


def in_hbm(x):
    return pltpu.with_memory_space_constraint(x, pltpu.HBM)


def in_vmem(x):
    return pltpu.with_memory_space_constraint(x, pltpu.VMEM)


def kernel_call(body, name, outs, in_specs, limit, scratch=()):
    return pl.pallas_call(
        body,
        name=name,
        out_shape=outs,
        in_specs=in_specs,
        out_specs=jax.tree.map(lambda _: IN_VMEM, outs),
        scratch_shapes=list(scratch),
        compiler_params=pltpu.CompilerParams(vmem_limit_bytes=limit * MIB),
    )


def shape(*dims, dtype=BF16):
    return jax.ShapeDtypeStruct(dims, dtype)


def attend_body(
    q_ref, tk_ref, tv_ref, len_ref, keys_hbm, values_hbm, out_ref, keys, values, rows, mixed, sems
):
    core = lax.axis_index(CORES)
    seq_count, cache_len, kv_width = keys_hbm.shape
    kv_count = kv_width // HEAD_WIDTH
    head_count = q_ref.shape[1] // HEAD_WIDTH
    group = head_count // kv_count
    side = group // 2
    copies = []
    for b in range(seq_count):
        pair = []
        for j, (source, target) in enumerate(((keys_hbm, keys), (values_hbm, values))):
            copy = pltpu.make_async_copy(source.at[b], target.at[b], sems.at[j, b])
            copy.start()
            pair.append(copy)
        copies.append(pair)
    for h in range(head_count):
        piece = q_ref[:, h * HEAD_WIDTH : (h + 1) * HEAD_WIDTH].astype(F32)
        rows[pl.ds(h, seq_count, stride=head_count), :] = piece
    inv_root = 1.0 / math.sqrt(HEAD_WIDTH)
    positions = lax.broadcasted_iota(jnp.int32, (group, cache_len), 1)
    for b in range(seq_count):
        for copy in copies[b]:
            copy.wait()
        visible = positions < len_ref[b]
        for g in range(kv_count):
            lanes = slice(g * HEAD_WIDTH, (g + 1) * HEAD_WIDTH)
            first = b * head_count + g * group
            query = rows[first : first + group, :]
            scores = lax.dot_general(
                query.astype(BF16),
                keys[b, :, lanes],
                (((1,), (1,)), ((), ())),
                preferred_element_type=F32,
            )
            scores = jnp.where(visible, scores * inv_root, -jnp.inf)
            fresh = jnp.sum(query * tk_ref[b : b + 1, lanes].astype(F32), axis=1, keepdims=True)
            fresh = fresh * inv_root
            highest = jnp.maximum(jnp.max(scores, axis=1, keepdims=True), fresh)
            cached_exp = jnp.exp(scores - highest)
            fresh_exp = jnp.exp(fresh - highest)
            totals = jnp.sum(cached_exp, axis=1, keepdims=True) + fresh_exp
            prob = (cached_exp / totals).astype(BF16)
            fresh_prob = (fresh_exp / totals).astype(BF16).astype(F32)
            out = jnp.dot(prob, values[b, :, lanes], preferred_element_type=F32)
            out = out + fresh_prob * tv_ref[b : b + 1, lanes].astype(F32)
            out = pltpu.roll(out, core * (HEAD_WIDTH // 2), 1)
            for a in range(2):
                start = g * group * seq_count + a * seq_count + b
                mixed[pl.ds(start, side, stride=2 * seq_count), :] = out[a * side : (a + 1) * side]
    tile = 2 * seq_count
    for g in range(kv_count):
        for y in range(side):
            for part, source in enumerate((y, y ^ 1)):
                at = (g * side + source) * tile
                near = mixed[at : at + tile, :]
                far = pltpu.roll(near, seq_count, 0)
                lanes = slice(part * HEAD_WIDTH, (part + 1) * HEAD_WIDTH)
                out_ref[2 * g * side + y, :, lanes] = near.astype(BF16)
                out_ref[(2 * g + 1) * side + y, :, lanes] = far.astype(BF16)


def attend(queries, token_keys, token_values, kv_len, stored_keys, stored_values):
    seq_count, feature_total = queries.shape
    heads = feature_total // HEAD_WIDTH
    return kernel_call(
        attend_body,
        "attend",
        shape(heads, 2 * seq_count, 2 * HEAD_WIDTH),
        [IN_VMEM, IN_VMEM, IN_VMEM, IN_SMEM, IN_HBM, IN_HBM],
        8,
        [
            pltpu.VMEM(stored_keys.shape, BF16),
            pltpu.VMEM(stored_values.shape, BF16),
            pltpu.VMEM((seq_count * heads, HEAD_WIDTH), F32),
            pltpu.VMEM((seq_count * heads, HEAD_WIDTH), F32),
            pltpu.SemaphoreType.DMA((2, seq_count)),
        ],
    )(
        in_hbm(queries),
        in_hbm(token_keys),
        in_hbm(token_values),
        kv_len,
        in_hbm(stored_keys),
        in_hbm(stored_values),
    )


def project_body(x_ref, *refs):
    own, other, out_ref = refs[:4], refs[4:8], refs[8]
    chips, tile, width = x_ref.shape
    cols = own[0].shape[1]
    half = cols // 2
    weights = [
        jnp.concatenate([own[d][...], other[d][...], own[d + 1][...], other[d + 1][...]])
        for d in (0, 2)
    ]
    step = 16
    low = lax.broadcasted_iota(jnp.int32, (step, tile, half), 1) < tile // 2
    for at in range(0, chips, step):
        x = x_ref[at : at + step].reshape(step * tile, width)
        near = jnp.dot(x, weights[0], preferred_element_type=F32).reshape(step, tile, cols)
        far = jnp.dot(x, weights[1], preferred_element_type=F32).reshape(step, tile, cols)
        kept = jnp.where(low, near[:, :, :half], far[:, :, half:])
        moved = jnp.where(low, near[:, :, half:], far[:, :, :half])
        moved = pltpu.roll(moved, tile // 2, 1)
        out_ref[at : at + step] = (kept + moved).astype(BF16)


def project(x, own, other):
    cols = own[0].shape[1]
    return kernel_call(
        project_body, "project", shape(x.shape[0], x.shape[1], cols // 2), [IN_VMEM] * 9, 12
    )(x, *map(in_hbm, own), *map(in_hbm, other))


def settle_body(x_ref, residual_ref, gain_ref, hidden_ref, kept_ref, given_ref, normed):
    core = lax.axis_index(CORES)
    chips, tile, half = x_ref.shape
    side = math.isqrt(chips)
    blocks = 4
    seq_count = tile // 2
    width = residual_ref.shape[1]

    def rows_of(ref, k):
        low, high = (ref[:, (2 * k + q) * half : (2 * k + q + 1) * half].astype(F32) for q in (0, 1))
        low, high = (jnp.broadcast_to(v, (seq_count, half)) for v in (low, high))
        return jnp.concatenate([low, high])

    square = jnp.zeros((tile, 1), F32)
    for k in range(blocks):
        total = rows_of(residual_ref, k)
        for x in range(k // 2, side, 2):
            for y in range(k % 2, side, 2):
                total = total + x_ref[x * side + y].astype(F32)
        hidden_ref[k] = total
        square = square + jnp.sum(total * total, axis=1, keepdims=True)
    square = jnp.broadcast_to(square, (tile, HEAD_WIDTH))
    square = square + pltpu.roll(square, seq_count, 0)
    scale = lax.rsqrt(square[:, :1] / width + 1e-06)
    for k in range(blocks):
        normed[k] = (hidden_ref[k] * scale * rows_of(gain_ref, k)).astype(BF16)
    kept_ref[...] = normed[pl.ds(core * 2, 2)]
    given_ref[...] = normed[pl.ds(2 - core * 2, 2)]


def settle(x, residual, gain):
    tile, half = x.shape[1:]
    return kernel_call(
        settle_body,
        "settle",
        (shape(4, tile, half, dtype=F32), shape(2, tile, half), shape(2, tile, half)),
        [IN_VMEM] * 3,
        6,
        [pltpu.VMEM((4, tile, half), BF16)],
    )(x, residual, gain)


def route_body(ids_ref, weight_ref, pick_ref, mix_ref):
    core = lax.axis_index(CORES)
    tokens, topk = ids_ref.shape
    seq_count = tokens // 2
    lanes = pick_ref.shape[1]
    lane = lax.broadcasted_iota(jnp.int32, (tokens, lanes), 1)
    row = lax.broadcasted_iota(jnp.int32, (tokens, lanes), 0)
    weight = weight_ref[...]
    mixing = weight / jnp.sum(weight, axis=1, keepdims=True)
    ids = ids_ref[...]
    hit = jnp.zeros((tokens, lanes), F32)
    share = jnp.zeros((tokens, lanes), F32)
    for k in range(topk):
        same = ids[:, k : k + 1] == lane // 8
        hit = jnp.where(same, 1.0, hit)
        share = jnp.where(same, mixing[:, k : k + 1], share)
    rank = jnp.zeros((tokens, lanes), F32)
    for t in range(tokens - 1):
        rank = rank + jnp.where(row > t, jnp.broadcast_to(hit[t : t + 1], (tokens, lanes)), 0.0)
    taken = jnp.where(rank == (lane % 2).astype(F32), hit, 0.0)
    share = share * taken
    own_low = (row < seq_count) == (core == 0)
    quarter = lane // 2 % 4
    for src in range(2):
        low = own_low if src == 0 else jnp.logical_not(own_low)
        chosen = jnp.where(low, taken, pltpu.roll(taken, seq_count, 0))
        shares = jnp.where(low, share, pltpu.roll(share, seq_count, 0))
        for kk in range(2):
            at = (src * 2 + kk) * tokens
            mine = quarter == kk * 2 + row // seq_count
            pick_ref[at : at + tokens, :] = jnp.where(mine, chosen, 0.0).astype(BF16)
            value = jnp.where(mine, shares, 0.0)
            coarse = value.astype(BF16)
            mix_ref[at : at + tokens, :] = coarse
            mix_ref[4 * tokens + at : 5 * tokens + at, :] = (value - coarse.astype(F32)).astype(BF16)


def route(expert_ids, route_weight, chips):
    tokens = expert_ids.shape[0]
    return kernel_call(
        route_body,
        "route",
        (shape(4 * tokens, 8 * chips), shape(8 * tokens, 8 * chips)),
        [IN_VMEM] * 2,
        4,
    )(expert_ids, route_weight)


def dispatch_body(kept_ref, other_ref, pick_ref, out_ref):
    pieces = [r[...].reshape(-1, r.shape[2]) for r in (kept_ref, other_ref)]
    rows = lax.dot_general(
        pick_ref[...],
        jnp.concatenate(pieces),
        (((0,), (0,)), ((), ())),
        preferred_element_type=F32,
    )
    out_ref[...] = rows.astype(BF16).reshape(out_ref.shape)


def dispatch(kept, other, pick):
    tile, half = kept.shape[1:]
    return kernel_call(
        dispatch_body, "dispatch", shape(pick.shape[1] // tile, tile, half), [IN_VMEM] * 3, 6
    )(kept, other, pick)


def slot_order(size, back=False):
    sorted_row = lax.broadcasted_iota(jnp.int32, (size, size), 1 if back else 0)
    row = lax.broadcasted_iota(jnp.int32, (size, size), 0 if back else 1)
    slot = sorted_row % (size // 4)
    quarter = sorted_row // (size // 4)
    return jnp.where(row == slot // 2 * 8 + quarter * 2 + slot % 2, 1.0, 0.0).astype(BF16)


def gate_body(own_ref, other_ref, gate_ref, up_ref, out_ref):
    core = lax.axis_index(CORES)
    chips, tile, part = own_ref.shape
    size = 256
    groups = chips * tile // size
    order = slot_order(size)
    slots = size // 4
    gate = up = None
    for half, ref in ((core, own_ref), (1 - core, other_ref)):
        sorted_rows = []
        for g in range(groups):
            rows = ref[g * size // tile : (g + 1) * size // tile].reshape(size, part)
            sorted_rows.append(jnp.dot(order, rows, preferred_element_type=F32).astype(BF16))
        for p in range(4):
            x = jnp.concatenate([r[p * slots : (p + 1) * slots] for r in sorted_rows])
            at = pl.multiple_of(half * (4 * part) + p * part, part)
            gate_part = jnp.dot(x, gate_ref[0, pl.ds(at, part), :], preferred_element_type=F32)
            up_part = jnp.dot(x, up_ref[0, pl.ds(at, part), :], preferred_element_type=F32)
            gate = gate_part if gate is None else gate + gate_part
            up = up_part if up is None else up + up_part
    out_ref[...] = (gate / (1.0 + jnp.exp(-gate)) * up).astype(BF16)


def gate_up(own, other, w_gate, w_up):
    chips, tile, _ = own.shape
    return kernel_call(
        gate_body, "gate_up", shape(chips * tile // 4, w_gate.shape[2]), [IN_VMEM] * 4, 16
    )(own, other, in_hbm(w_gate), in_hbm(w_up))


def down_body(own_ref, other_ref, down_ref, moved_ref, out_ref):
    core = lax.axis_index(CORES)
    chips, tile, part = out_ref.shape
    size = 256
    groups = chips * tile // size
    order = slot_order(size, back=True)
    slots = size // 4
    own, other = own_ref[...], other_ref[...]
    quarters = []
    for p in range(4):
        at = pl.multiple_of(core * (4 * part) + p * part, part)
        value = jnp.dot(own, down_ref[0, :, pl.ds(at, part)], preferred_element_type=F32)
        value = value + jnp.dot(
            other, moved_ref[:, p * part : (p + 1) * part], preferred_element_type=F32
        )
        quarters.append(value.astype(BF16))
    for g in range(groups):
        rows = jnp.concatenate([v[g * slots : (g + 1) * slots] for v in quarters])
        rows = jnp.dot(order, rows, preferred_element_type=F32).astype(BF16)
        out_ref[g * size // tile : (g + 1) * size // tile] = rows.reshape(size // tile, tile, part)


def down(own, other, w_down, moved_down, tile):
    slots = own.shape[0]
    part = moved_down.shape[1] // 4
    return kernel_call(
        down_body, "down", shape(slots * 4 // tile, tile, part), [IN_VMEM] * 4, 14
    )(own, other, w_down, moved_down)


def combine_body(x_ref, mix_ref, own_ref, other_ref):
    x = x_ref[...].reshape(-1, x_ref.shape[2])
    rows = jnp.dot(mix_ref[...], x, preferred_element_type=F32)
    count = rows.shape[0] // 2
    rows = rows[:count] + rows[count:]
    own_ref[...] = rows[: count // 2].reshape(own_ref.shape)
    other_ref[...] = rows[count // 2 :].reshape(other_ref.shape)


def combine(x, mix):
    out = shape(2, x.shape[1], x.shape[2], dtype=F32)
    return kernel_call(combine_body, "combine", (out, out), [IN_VMEM] * 2, 4)(x, mix)


def finish_body(hidden_ref, own_ref, other_ref, out_ref, total):
    core = lax.axis_index(CORES)
    blocks, tile, half = hidden_ref.shape
    total[pl.ds(core * 2, 2)] = own_ref[...]
    total[pl.ds(2 - core * 2, 2)] = other_ref[...]
    for k in range(blocks):
        value = (hidden_ref[k] + total[k]).astype(BF16)
        for q in range(2):
            at = (2 * k + q) * half
            out_ref[:, at : at + half] = value[q * tile // 2 : (q + 1) * tile // 2]


def finish(hidden, own, other):
    blocks, tile, half = hidden.shape
    return kernel_call(
        finish_body,
        "finish",
        shape(tile // 2, 2 * blocks * half),
        [IN_VMEM] * 3,
        2,
        [pltpu.VMEM(hidden.shape, F32)],
    )(hidden, own, other)


def on_device(
    queries,
    token_keys,
    token_values,
    stored_keys,
    stored_values,
    kv_len,
    residual,
    out_weight,
    norm_gain,
    expert_ids,
    route_weight,
    w_gate,
    w_up,
    w_down,
):
    chips = lax.axis_size(CHIPS)
    side = math.isqrt(chips)
    chip = lax.axis_index(CHIPS)
    core = lax.axis_index(CORES)
    place = chip // side % 2 * 2 + chip % 2
    model_width = out_weight.shape[1]
    col_width = model_width // 4
    half_width = model_width // 2

    outgoing = attend(queries, token_keys, token_values, kv_len, stored_keys, stored_values)
    tokens = lax.all_to_all(outgoing, CHIPS, 0, 0, tiled=True)
    own = []
    for d in range(4):
        piece = lax.dynamic_slice_in_dim(out_weight, (place ^ d) * col_width, col_width, 1)
        own.append(lax.ppermute(piece, CHIPS, quad_step(side, d // 2, d % 2)) if d else piece)
    other = [swapped(piece) for piece in own]
    given_down = lax.dynamic_slice_in_dim(w_down[0], (1 - core) * half_width, half_width, 1)
    moved_down = swapped(given_down)
    pick, mix = route(expert_ids, route_weight, chips)

    came_back = lax.all_to_all(project(tokens, own, other), CHIPS, 0, 0, tiled=True)
    hidden, kept, given = settle(came_back, residual, norm_gain[None])
    incoming = lax.all_to_all(dispatch(kept, swapped(given), pick), CHIPS, 0, 0, tiled=True)
    act = gate_up(incoming, swapped(incoming), w_gate, w_up)
    expert_out = down(act, swapped(act), w_down, moved_down, incoming.shape[1])
    returned = lax.all_to_all(expert_out, CHIPS, 0, 0, tiled=True)
    moe_own, moe_given = combine(returned, mix)
    return finish(hidden, moe_own, swapped(moe_given))


def solution(mesh):
    in_specs = (
        P(("groups", "expert", "replica"), None),
        P(("groups", "expert", "replica"), None),
        P(("groups", "expert", "replica"), None),
        P(("groups", "expert", "replica"), None, None),
        P(("groups", "expert", "replica"), None, None),
        P(("groups", "expert", "replica")),
        P(("groups", "expert", "replica"), None),
        P(("expert", "replica"), None),
        P(),
        P(("groups", "expert"), None),
        P(("groups", "expert"), None),
        P("expert", None, "replica"),
        P("expert", None, "replica"),
        P("expert", "replica", None),
    )
    out_specs = P(("groups", "expert", "replica"), None)
    return jax.shard_map(
        on_device, mesh=mesh, in_specs=in_specs, out_specs=out_specs, check_vma=False
    )
```

```python
import math

import jax
import jax.numpy as jnp
from jax import lax
from jax.experimental import pallas as pl
from jax.experimental.pallas import tpu as pltpu
from jax.sharding import PartitionSpec as P

HEAD_WIDTH = 128
CHIPS, CORES = "expert", "replica"
F32, BF16 = jnp.float32, jnp.bfloat16
IN_VMEM = pl.BlockSpec(memory_space=pltpu.VMEM)
IN_SMEM = pl.BlockSpec(memory_space=pltpu.SMEM)
IN_HBM = pl.BlockSpec(memory_space=pltpu.HBM)


def swapped(x):
    return lax.ppermute(x, CORES, [(0, 1), (1, 0)])


def quad_step(side, dx, dy):
    return [
        (x * side + y, (x ^ dx) * side + (y ^ dy)) for x in range(side) for y in range(side)
    ]


MIB = 1 << 20


def in_hbm(x):
    return pltpu.with_memory_space_constraint(x, pltpu.HBM)


def in_vmem(x):
    return pltpu.with_memory_space_constraint(x, pltpu.VMEM)


def kernel_call(body, outs, in_specs, limit, scratch=()):
    return pl.pallas_call(
        body,
        out_shape=outs,
        in_specs=in_specs,
        out_specs=jax.tree.map(lambda _: IN_VMEM, outs),
        scratch_shapes=list(scratch),
        compiler_params=pltpu.CompilerParams(vmem_limit_bytes=limit * MIB),
    )


def shape(*dims, dtype=BF16):
    return jax.ShapeDtypeStruct(dims, dtype)


def attend_body(
    q_hbm,
    tk_hbm,
    tv_hbm,
    len_hbm,
    keys_hbm,
    values_hbm,
    weight_hbm,
    out_ref,
    piece0,
    piece1,
    piece2,
    piece3,
    q_ref,
    tk_ref,
    tv_ref,
    len_ref,
    keys,
    values,
    rows,
    mixed,
    sems,
    few,
):
    core = lax.axis_index(CORES)
    seq_count, cache_len, kv_width = keys_hbm.shape
    kv_count = kv_width // HEAD_WIDTH
    head_count = q_hbm.shape[1] // HEAD_WIDTH
    group = head_count // kv_count
    side = group // 2
    small = [
        pltpu.make_async_copy(source, target, few.at[j])
        for j, (source, target) in enumerate(
            ((q_hbm, q_ref), (tk_hbm, tk_ref), (tv_hbm, tv_ref), (len_hbm, len_ref))
        )
    ]
    for copy in small:
        copy.start()
    copies = []
    for b in range(seq_count):
        pair = []
        for j, (source, target) in enumerate(((keys_hbm, keys), (values_hbm, values))):
            copy = pltpu.make_async_copy(source.at[b], target.at[b], sems.at[j, b])
            copy.start()
            pair.append(copy)
        copies.append(pair)
    chip = lax.axis_index(CHIPS)
    place = chip // side % 2 * 2 + chip % 2
    sliced = []
    for d, piece in enumerate((piece0, piece1, piece2, piece3)):
        cols = piece.shape[1]
        at = pl.multiple_of((place ^ d) * cols, cols)
        sliced.append(
            pltpu.make_async_copy(weight_hbm.at[:, pl.ds(at, cols)], piece, few.at[len(small) + d])
        )
        sliced[-1].start()
    for copy in small:
        copy.wait()
    for h in range(head_count):
        piece = q_ref[:, h * HEAD_WIDTH : (h + 1) * HEAD_WIDTH].astype(F32)
        rows[pl.ds(h, seq_count, stride=head_count), :] = piece
    inv_root = 1.0 / math.sqrt(HEAD_WIDTH)
    positions = lax.broadcasted_iota(jnp.int32, (head_count, cache_len), 1)
    lanes = [slice(g * HEAD_WIDTH, (g + 1) * HEAD_WIDTH) for g in range(kv_count)]
    for b in range(seq_count):
        query = rows[b * head_count : (b + 1) * head_count, :]
        latest = [tk_ref[b : b + 1, lanes[g]].astype(F32) for g in range(kv_count)]
        latest = jnp.concatenate([jnp.broadcast_to(v, (group, HEAD_WIDTH)) for v in latest])
        fresh = jnp.sum(query * latest, axis=1, keepdims=True) * inv_root
        query = query.astype(BF16)
        copies[b][0].wait()
        scores = [
            lax.dot_general(
                query[g * group : (g + 1) * group],
                keys[b, :, lanes[g]],
                (((1,), (1,)), ((), ())),
                preferred_element_type=F32,
            )
            for g in range(kv_count)
        ]
        scores = jnp.where(positions < len_ref[b], jnp.concatenate(scores) * inv_root, -jnp.inf)
        highest = jnp.maximum(jnp.max(scores, axis=1, keepdims=True), fresh)
        cached_exp = jnp.exp(scores - highest)
        fresh_exp = jnp.exp(fresh - highest)
        totals = jnp.sum(cached_exp, axis=1, keepdims=True) + fresh_exp
        prob = (cached_exp / totals).astype(BF16)
        fresh_prob = (fresh_exp / totals).astype(BF16).astype(F32)
        copies[b][1].wait()
        for g in range(kv_count):
            heads = slice(g * group, (g + 1) * group)
            out = jnp.dot(prob[heads], values[b, :, lanes[g]], preferred_element_type=F32)
            out = out + fresh_prob[heads] * tv_ref[b : b + 1, lanes[g]].astype(F32)
            out = pltpu.roll(out, core * (HEAD_WIDTH // 2), 1)
            for a in range(2):
                start = g * group * seq_count + a * seq_count + b
                mixed[pl.ds(start, side, stride=2 * seq_count), :] = out[a * side : (a + 1) * side]
    tile = 2 * seq_count
    for g in range(kv_count):
        for y in range(side):
            for part, source in enumerate((y, y ^ 1)):
                at = (g * side + source) * tile
                near = mixed[at : at + tile, :]
                far = pltpu.roll(near, seq_count, 0)
                out_ref[2 * g * side + y, :, lanes[part]] = near.astype(BF16)
                out_ref[(2 * g + 1) * side + y, :, lanes[part]] = far.astype(BF16)
    for copy in sliced:
        copy.wait()


def attend(queries, token_keys, token_values, kv_len, stored_keys, stored_values, out_weight):
    seq_count, feature_total = queries.shape
    heads = feature_total // HEAD_WIDTH
    rows, cols = out_weight.shape
    return pl.pallas_call(
        attend_body,
        name="attend",
        out_shape=[pltpu.HBM((heads, 2 * seq_count, 2 * HEAD_WIDTH), BF16)]
        + [pltpu.HBM((rows, cols // 4), BF16)] * 4,
        in_specs=[IN_HBM] * 7,
        out_specs=[IN_VMEM] + [IN_HBM] * 4,
        scratch_shapes=[
            pltpu.VMEM(queries.shape, BF16),
            pltpu.VMEM(token_keys.shape, BF16),
            pltpu.VMEM(token_values.shape, BF16),
            pltpu.SMEM(kv_len.shape, jnp.int32),
            pltpu.VMEM(stored_keys.shape, BF16),
            pltpu.VMEM(stored_values.shape, BF16),
            pltpu.VMEM((seq_count * heads, HEAD_WIDTH), F32),
            pltpu.VMEM((seq_count * heads, HEAD_WIDTH), F32),
            pltpu.SemaphoreType.DMA((2, seq_count)),
            pltpu.SemaphoreType.DMA((8,)),
        ],
        compiler_params=pltpu.CompilerParams(vmem_limit_bytes=8 * MIB),
    )(
        *map(
            in_hbm,
            (queries, token_keys, token_values, kv_len, stored_keys, stored_values, out_weight),
        )
    )


def copy_all(pairs, sems):
    copies = [pltpu.make_async_copy(*pair, sems.at[j]) for j, pair in enumerate(pairs)]
    for copy in copies:
        copy.start()
    for copy in copies:
        copy.wait()


def stack_body(*refs):
    own, other, out_ref, sems = refs[:4], refs[4:8], refs[8], refs[9]
    rows = own[0].shape[0]
    pairs = []
    for d in range(4):
        for half, source in enumerate((own[d], other[d])):
            at = (d % 2 * 2 + half) * rows
            pairs.append((source, out_ref.at[d // 2, at : at + rows]))
    copy_all(pairs, sems)


def stack(own, other):
    rows, cols = own[0].shape
    return pl.pallas_call(
        stack_body,
        name="stack",
        out_shape=pltpu.VMEM((2, 4 * rows, cols), BF16),
        in_specs=[IN_HBM] * 8,
        out_specs=IN_VMEM,
        scratch_shapes=[pltpu.SemaphoreType.DMA((8,))],
        compiler_params=pltpu.CompilerParams(vmem_limit_bytes=2 * MIB),
    )(*map(in_hbm, own), *map(in_hbm, other))


def halves_body(gate_hbm, up_hbm, down_hbm, kept_ref, *refs):
    outs, sems = refs[:3], refs[3]
    core = lax.axis_index(CORES)
    half = kept_ref.shape[0]
    kept, given = (pl.ds(pl.multiple_of(j * half, half), half) for j in (core, 1 - core))
    copy_all(
        (
            (gate_hbm.at[0, kept, :], kept_ref),
            (gate_hbm.at[0, given, :], outs[0]),
            (up_hbm.at[0, given, :], outs[1]),
            (down_hbm.at[0, :, given], outs[2]),
        ),
        sems,
    )


def halves(w_gate, w_up, w_down):
    _, width, units = w_gate.shape
    tall, wide = (width // 2, units), (units, width // 2)
    return pl.pallas_call(
        halves_body,
        name="halves",
        out_shape=[pltpu.VMEM(tall, BF16)] + [pltpu.HBM(dims, BF16) for dims in (tall, tall, wide)],
        in_specs=[IN_HBM] * 3,
        out_specs=[IN_VMEM] + [IN_HBM] * 3,
        scratch_shapes=[pltpu.SemaphoreType.DMA((4,))],
        compiler_params=pltpu.CompilerParams(vmem_limit_bytes=2 * MIB),
    )(*map(in_hbm, (w_gate, w_up, w_down)))


def project_body(x_ref, weight_ref, out_ref):
    chips, tile, width = x_ref.shape
    cols = weight_ref.shape[2]
    half = cols // 2
    step = 16
    low = lax.broadcasted_iota(jnp.int32, (step, tile, half), 1) < tile // 2
    for at in range(0, chips, step):
        x = x_ref[at : at + step].reshape(step * tile, width)
        near, far = (
            jnp.dot(x, weight_ref[j], preferred_element_type=F32).reshape(step, tile, cols)
            for j in range(2)
        )
        kept = jnp.where(low, near[:, :, :half], far[:, :, half:])
        moved = jnp.where(low, near[:, :, half:], far[:, :, :half])
        moved = pltpu.roll(moved, tile // 2, 1)
        out_ref[at : at + step] = (kept + moved).astype(BF16)


def project(x, weight):
    cols = weight.shape[2]
    return kernel_call(
        project_body, pltpu.HBM((x.shape[0], x.shape[1], cols // 2), BF16), [IN_VMEM] * 2, 12
    )(x, in_vmem(weight))


def settle_body(x_ref, residual_ref, gain_ref, hidden_ref, kept_ref, given_ref, normed):
    core = lax.axis_index(CORES)
    chips, tile, half = x_ref.shape
    side = math.isqrt(chips)
    blocks = 4
    seq_count = tile // 2
    width = residual_ref.shape[1]

    def rows_of(ref, k):
        low, high = (ref[:, (2 * k + q) * half : (2 * k + q + 1) * half].astype(F32) for q in (0, 1))
        low, high = (jnp.broadcast_to(v, (seq_count, half)) for v in (low, high))
        return jnp.concatenate([low, high])

    square = jnp.zeros((tile, 1), F32)
    for k in range(blocks):
        total = rows_of(residual_ref, k)
        for x in range(k // 2, side, 2):
            for y in range(k % 2, side, 2):
                total = total + x_ref[x * side + y].astype(F32)
        hidden_ref[k] = total
        square = square + jnp.sum(total * total, axis=1, keepdims=True)
    square = jnp.broadcast_to(square, (tile, HEAD_WIDTH))
    square = square + pltpu.roll(square, seq_count, 0)
    scale = lax.rsqrt(square[:, :1] / width + 1e-06)
    for k in range(blocks):
        normed[k] = (hidden_ref[k] * scale * rows_of(gain_ref, k)).astype(BF16)
    kept_ref[...] = normed[pl.ds(core * 2, 2)]
    given_ref[...] = normed[pl.ds(2 - core * 2, 2)]


def settle(x, residual, gain):
    tile, half = x.shape[1:]
    return kernel_call(
        settle_body,
        (shape(4, tile, half, dtype=F32), shape(2, tile, half), shape(2, tile, half)),
        [IN_VMEM] * 3,
        6,
        [pltpu.VMEM((4, tile, half), BF16)],
    )(x, residual, gain)


def route_body(ids_ref, weight_ref, pick_ref, mix_ref):
    core = lax.axis_index(CORES)
    tokens, topk = ids_ref.shape
    seq_count = tokens // 2
    lanes = pick_ref.shape[1]
    lane = lax.broadcasted_iota(jnp.int32, (tokens, lanes), 1)
    row = lax.broadcasted_iota(jnp.int32, (tokens, lanes), 0)
    weight = weight_ref[...]
    mixing = weight / jnp.sum(weight, axis=1, keepdims=True)
    ids = ids_ref[...]
    hit = jnp.zeros((tokens, lanes), F32)
    share = jnp.zeros((tokens, lanes), F32)
    for k in range(topk):
        same = ids[:, k : k + 1] == lane // 8
        hit = jnp.where(same, 1.0, hit)
        share = jnp.where(same, mixing[:, k : k + 1], share)
    rank = jnp.zeros((tokens, lanes), F32)
    for t in range(tokens - 1):
        rank = rank + jnp.where(row > t, jnp.broadcast_to(hit[t : t + 1], (tokens, lanes)), 0.0)
    taken = jnp.where(rank == (lane % 2).astype(F32), hit, 0.0)
    share = share * taken
    own_low = (row < seq_count) == (core == 0)
    quarter = lane // 2 % 4
    for src in range(2):
        low = own_low if src == 0 else jnp.logical_not(own_low)
        chosen = jnp.where(low, taken, pltpu.roll(taken, seq_count, 0))
        shares = jnp.where(low, share, pltpu.roll(share, seq_count, 0))
        for kk in range(2):
            at = (src * 2 + kk) * tokens
            mine = quarter == kk * 2 + row // seq_count
            pick_ref[at : at + tokens, :] = jnp.where(mine, chosen, 0.0).astype(BF16)
            value = jnp.where(mine, shares, 0.0)
            coarse = value.astype(BF16)
            mix_ref[at : at + tokens, :] = coarse
            mix_ref[4 * tokens + at : 5 * tokens + at, :] = (value - coarse.astype(F32)).astype(BF16)


def route(expert_ids, route_weight, chips):
    tokens = expert_ids.shape[0]
    return kernel_call(
        route_body, (shape(4 * tokens, 8 * chips), shape(8 * tokens, 8 * chips)), [IN_VMEM] * 2, 4
    )(expert_ids, route_weight)


def dispatch_body(kept_ref, other_ref, pick_ref, out_ref):
    pieces = [r[...].reshape(-1, r.shape[2]) for r in (kept_ref, other_ref)]
    rows = lax.dot_general(
        pick_ref[...],
        jnp.concatenate(pieces),
        (((0,), (0,)), ((), ())),
        preferred_element_type=F32,
    )
    out_ref[...] = rows.astype(BF16).reshape(out_ref.shape)


def dispatch(kept, other, pick):
    tile, half = kept.shape[1:]
    return kernel_call(
        dispatch_body, pltpu.HBM((pick.shape[1] // tile, tile, half), BF16), [IN_VMEM] * 3, 6
    )(kept, other, pick)


def slot_order(size, back=False):
    sorted_row = lax.broadcasted_iota(jnp.int32, (size, size), 1 if back else 0)
    row = lax.broadcasted_iota(jnp.int32, (size, size), 0 if back else 1)
    slot = sorted_row % (size // 4)
    quarter = sorted_row // (size // 4)
    return jnp.where(row == slot // 2 * 8 + quarter * 2 + slot % 2, 1.0, 0.0).astype(BF16)


def gate_body(
    x_ref,
    gate_ref,
    up_hbm,
    down_hbm,
    gate_moved,
    up_moved,
    down_moved,
    part_ref,
    sent_ref,
    down_ref,
    buffers,
    sems,
):
    core = lax.axis_index(CORES)
    chips, tile, part = x_ref.shape
    half, units = gate_ref.shape
    kept = pl.ds(pl.multiple_of(core * half, half), half)
    pairs = (
        (up_hbm.at[0, kept, :], buffers.at[0]),
        (gate_moved, buffers.at[1]),
        (up_moved, buffers.at[2]),
        (down_hbm.at[0, :, kept], down_ref.at[:units]),
        (down_moved, down_ref.at[units:]),
    )
    copies = [pltpu.make_async_copy(*pair, sems.at[j]) for j, pair in enumerate(pairs)]
    for copy in copies:
        copy.start()
    size = 256
    groups = chips * tile // size
    order = slot_order(size)
    slots = size // 4
    sorted_rows = []
    for g in range(groups):
        rows = x_ref[g * size // tile : (g + 1) * size // tile].reshape(size, part)
        sorted_rows.append(jnp.dot(order, rows, preferred_element_type=F32).astype(BF16))
    quarters = [
        jnp.concatenate([r[p * slots : (p + 1) * slots] for r in sorted_rows]) for p in range(4)
    ]
    x = jnp.concatenate(quarters, axis=1)
    for j in range(4):
        if j:
            copies[j - 1].wait()
        weight = buffers[j - 1] if j else gate_ref[...]
        value = jnp.dot(x, weight, preferred_element_type=F32)
        part_ref[:, j * units : (j + 1) * units] = value
        at = (j + 2) % 4 * units
        sent_ref[:, at : at + units] = value.astype(BF16)
    for copy in copies[3:]:
        copy.wait()


def gate_up(x, gate_own, w_up, w_down, moved):
    chips, tile, _ = x.shape
    half, units = gate_own.shape
    dims = chips * tile // 4, 4 * units
    return pl.pallas_call(
        gate_body,
        name="gate_up",
        out_shape=[
            pltpu.VMEM(dims, F32),
            pltpu.VMEM(dims, BF16),
            pltpu.VMEM((2 * units, half), BF16),
        ],
        in_specs=[IN_VMEM] * 2 + [IN_HBM] * 5,
        out_specs=[IN_VMEM] * 3,
        scratch_shapes=[pltpu.VMEM((3, half, units), BF16), pltpu.SemaphoreType.DMA((5,))],
        compiler_params=pltpu.CompilerParams(vmem_limit_bytes=16 * MIB),
    )(x, in_vmem(gate_own), *map(in_hbm, (w_up, w_down, *moved)))


def down_body(part_ref, arrived_ref, down_ref, out_ref):
    chips, tile, part = out_ref.shape
    size = 256
    groups = chips * tile // size
    order = slot_order(size, back=True)
    slots = size // 4
    units = down_ref.shape[0] // 2

    def act(at):
        gate, up = (
            part_ref[:, j : j + units] + arrived_ref[:, j : j + units].astype(F32)
            for j in (at, at + units)
        )
        return (gate / (1.0 + jnp.exp(-gate)) * up).astype(BF16)

    hidden = jnp.concatenate([act(0), act(2 * units)], axis=1)
    quarters = []
    for p in range(4):
        lanes = slice(p * part, (p + 1) * part)
        value = jnp.dot(hidden, down_ref[:, lanes], preferred_element_type=F32)
        quarters.append(value.astype(BF16))
    for g in range(groups):
        rows = jnp.concatenate([v[g * slots : (g + 1) * slots] for v in quarters])
        rows = jnp.dot(order, rows, preferred_element_type=F32).astype(BF16)
        out_ref[g * size // tile : (g + 1) * size // tile] = rows.reshape(size // tile, tile, part)


def down(part, arrived, weight, tile):
    slots = part.shape[0]
    width = weight.shape[1] // 4
    return kernel_call(
        down_body, pltpu.HBM((slots * 4 // tile, tile, width), BF16), [IN_VMEM] * 3, 8
    )(part, arrived, in_vmem(weight))


def combine_body(x_ref, mix_ref, own_ref, other_ref):
    x = x_ref[...].reshape(-1, x_ref.shape[2])
    rows = jnp.dot(mix_ref[...], x, preferred_element_type=F32)
    count = rows.shape[0] // 2
    rows = rows[:count] + rows[count:]
    own_ref[...] = rows[: count // 2].reshape(own_ref.shape)
    other_ref[...] = rows[count // 2 :].reshape(other_ref.shape)


def combine(x, mix):
    out = shape(2, x.shape[1], x.shape[2], dtype=F32)
    return kernel_call(combine_body, (out, out), [IN_VMEM] * 2, 4)(x, mix)


def finish_body(hidden_ref, own_ref, other_ref, out_ref, total):
    core = lax.axis_index(CORES)
    blocks, tile, half = hidden_ref.shape
    total[pl.ds(core * 2, 2)] = own_ref[...]
    total[pl.ds(2 - core * 2, 2)] = other_ref[...]
    for k in range(blocks):
        value = (hidden_ref[k] + total[k]).astype(BF16)
        for q in range(2):
            at = (2 * k + q) * half
            out_ref[:, at : at + half] = value[q * tile // 2 : (q + 1) * tile // 2]


def finish(hidden, own, other):
    blocks, tile, half = hidden.shape
    return kernel_call(
        finish_body, shape(tile // 2, 2 * blocks * half), [IN_VMEM] * 3, 2, [pltpu.VMEM(hidden.shape, F32)]
    )(hidden, own, other)


def on_device(
    queries,
    token_keys,
    token_values,
    stored_keys,
    stored_values,
    kv_len,
    residual,
    out_weight,
    norm_gain,
    expert_ids,
    route_weight,
    w_gate,
    w_up,
    w_down,
):
    chips = lax.axis_size(CHIPS)
    side = math.isqrt(chips)
    outgoing, *pieces = attend(
        queries, token_keys, token_values, kv_len, stored_keys, stored_values, out_weight
    )
    own = [pieces[0]] + [
        lax.ppermute(pieces[d], CHIPS, quad_step(side, d // 2, d % 2)) for d in (1, 2, 3)
    ]
    tokens = lax.all_to_all(outgoing, CHIPS, 0, 0, tiled=True)
    other = [swapped(piece) for piece in own]
    weight = stack(own, other)
    gate_own, *given_halves = halves(w_gate, w_up, w_down)
    moved = [swapped(x) for x in given_halves]
    pick, mix = route(expert_ids, route_weight, chips)

    sums = project(tokens, weight)
    came_back = lax.all_to_all(sums, CHIPS, 0, 0, tiled=True)
    hidden, normed, normed_given = settle(came_back, residual, norm_gain[None])
    outgoing = dispatch(normed, swapped(normed_given), pick)
    incoming = lax.all_to_all(outgoing, CHIPS, 0, 0, tiled=True)
    part, sent, down_weight = gate_up(incoming, gate_own, w_up, w_down, moved)
    expert_out = down(part, swapped(sent), down_weight, incoming.shape[1])
    returned = lax.all_to_all(expert_out, CHIPS, 0, 0, tiled=True)
    moe_own, moe_given = combine(returned, mix)
    return finish(hidden, moe_own, swapped(moe_given))


def solution(mesh):
    in_specs = (
        P(("groups", "expert", "replica"), None),
        P(("groups", "expert", "replica"), None),
        P(("groups", "expert", "replica"), None),
        P(("groups", "expert", "replica"), None, None),
        P(("groups", "expert", "replica"), None, None),
        P(("groups", "expert", "replica")),
        P(("groups", "expert", "replica"), None),
        P(("expert", "replica"), None),
        P(),
        P(("groups", "expert"), None),
        P(("groups", "expert"), None),
        P("expert", None, "replica"),
        P("expert", None, "replica"),
        P("expert", "replica", None),
    )
    out_specs = P(("groups", "expert", "replica"), None)
    return jax.shard_map(
        on_device, mesh=mesh, in_specs=in_specs, out_specs=out_specs, check_vma=False
    )
```

```python
import math

import jax
import jax.numpy as jnp
from jax import lax
from jax.experimental import pallas as pl
from jax.experimental.pallas import tpu as pltpu
from jax.sharding import PartitionSpec as P

HEAD_WIDTH = 128
CHIPS, CORES = "expert", "replica"
F32, BF16 = jnp.float32, jnp.bfloat16
IN_VMEM = pl.BlockSpec(memory_space=pltpu.VMEM)
IN_SMEM = pl.BlockSpec(memory_space=pltpu.SMEM)
IN_HBM = pl.BlockSpec(memory_space=pltpu.HBM)


def swapped(x):
    return lax.ppermute(x, CORES, [(0, 1), (1, 0)])


def quad_step(side, dx, dy):
    return [
        (x * side + y, (x ^ dx) * side + (y ^ dy)) for x in range(side) for y in range(side)
    ]


MIB = 1 << 20


def in_hbm(x):
    return pltpu.with_memory_space_constraint(x, pltpu.HBM)


def in_vmem(x):
    return pltpu.with_memory_space_constraint(x, pltpu.VMEM)


def kernel_call(body, outs, in_specs, limit, scratch=()):
    return pl.pallas_call(
        body,
        out_shape=outs,
        in_specs=in_specs,
        out_specs=jax.tree.map(lambda _: IN_VMEM, outs),
        scratch_shapes=list(scratch),
        compiler_params=pltpu.CompilerParams(vmem_limit_bytes=limit * MIB),
    )


def shape(*dims, dtype=BF16):
    return jax.ShapeDtypeStruct(dims, dtype)


def attend_body(
    q_hbm,
    tk_hbm,
    tv_hbm,
    len_hbm,
    keys_hbm,
    values_hbm,
    weight_hbm,
    out_ref,
    piece0,
    piece1,
    piece2,
    piece3,
    q_ref,
    tk_ref,
    tv_ref,
    len_ref,
    keys,
    values,
    pieces,
    rows,
    mixed,
    sems,
    few,
):
    core = lax.axis_index(CORES)
    seq_count, cache_len, kv_width = keys_hbm.shape
    kv_count = kv_width // HEAD_WIDTH
    head_count = q_hbm.shape[1] // HEAD_WIDTH
    group = head_count // kv_count
    side = group // 2
    small = [
        pltpu.make_async_copy(source, target, few.at[j])
        for j, (source, target) in enumerate(
            ((q_hbm, q_ref), (tk_hbm, tk_ref), (tv_hbm, tv_ref), (len_hbm, len_ref))
        )
    ]
    for copy in small:
        copy.start()
    copies = []
    for b in range(seq_count):
        pair = []
        for j, (source, target) in enumerate(((keys_hbm, keys), (values_hbm, values))):
            copy = pltpu.make_async_copy(source.at[b], target.at[b], sems.at[j, b])
            copy.start()
            pair.append(copy)
        copies.append(pair)
    chip = lax.axis_index(CHIPS)
    place = chip // side % 2 * 2 + chip % 2
    sliced, stored = [], []
    for d, piece in enumerate((piece0, piece1, piece2, piece3)):
        cols = piece.shape[1]
        at = pl.multiple_of((place ^ d) * cols, cols)
        source = weight_hbm.at[:, pl.ds(at, cols)]
        sliced.append(pltpu.make_async_copy(source, pieces.at[d], few.at[len(small) + d]))
        stored.append(pltpu.make_async_copy(pieces.at[d], piece, few.at[len(small) + 4 + d]))
        sliced[-1].start()
    for copy in small:
        copy.wait()
    for h in range(head_count):
        piece = q_ref[:, h * HEAD_WIDTH : (h + 1) * HEAD_WIDTH].astype(F32)
        rows[pl.ds(h, seq_count, stride=head_count), :] = piece
    inv_root = 1.0 / math.sqrt(HEAD_WIDTH)
    positions = lax.broadcasted_iota(jnp.int32, (head_count, cache_len), 1)
    lanes = [slice(g * HEAD_WIDTH, (g + 1) * HEAD_WIDTH) for g in range(kv_count)]
    for b in range(seq_count):
        query = rows[b * head_count : (b + 1) * head_count, :]
        latest = [tk_ref[b : b + 1, lanes[g]].astype(F32) for g in range(kv_count)]
        latest = jnp.concatenate([jnp.broadcast_to(v, (group, HEAD_WIDTH)) for v in latest])
        fresh = jnp.sum(query * latest, axis=1, keepdims=True) * inv_root
        query = query.astype(BF16)
        copies[b][0].wait()
        scores = [
            lax.dot_general(
                query[g * group : (g + 1) * group],
                keys[b, :, lanes[g]],
                (((1,), (1,)), ((), ())),
                preferred_element_type=F32,
            )
            for g in range(kv_count)
        ]
        scores = jnp.where(positions < len_ref[b], jnp.concatenate(scores) * inv_root, -jnp.inf)
        highest = jnp.maximum(jnp.max(scores, axis=1, keepdims=True), fresh)
        cached_exp = jnp.exp(scores - highest)
        fresh_exp = jnp.exp(fresh - highest)
        totals = jnp.sum(cached_exp, axis=1, keepdims=True) + fresh_exp
        prob = (cached_exp / totals).astype(BF16)
        fresh_prob = (fresh_exp / totals).astype(BF16).astype(F32)
        copies[b][1].wait()
        for g in range(kv_count):
            heads = slice(g * group, (g + 1) * group)
            out = jnp.dot(prob[heads], values[b, :, lanes[g]], preferred_element_type=F32)
            out = out + fresh_prob[heads] * tv_ref[b : b + 1, lanes[g]].astype(F32)
            out = pltpu.roll(out, core * (HEAD_WIDTH // 2), 1)
            for a in range(2):
                start = g * group * seq_count + a * seq_count + b
                mixed[pl.ds(start, side, stride=2 * seq_count), :] = out[a * side : (a + 1) * side]
        if b == seq_count // 2:
            for d in range(4):
                sliced[d].wait()
                stored[d].start()
    tile = 2 * seq_count
    for g in range(kv_count):
        for y in range(side):
            for part, source in enumerate((y, y ^ 1)):
                at = (g * side + source) * tile
                near = mixed[at : at + tile, :]
                far = pltpu.roll(near, seq_count, 0)
                out_ref[2 * g * side + y, :, lanes[part]] = near.astype(BF16)
                out_ref[(2 * g + 1) * side + y, :, lanes[part]] = far.astype(BF16)
    for copy in stored:
        copy.wait()


def attend(queries, token_keys, token_values, kv_len, stored_keys, stored_values, out_weight):
    seq_count, feature_total = queries.shape
    heads = feature_total // HEAD_WIDTH
    rows, cols = out_weight.shape
    return pl.pallas_call(
        attend_body,
        name="attend",
        out_shape=[pltpu.HBM((heads, 2 * seq_count, 2 * HEAD_WIDTH), BF16)]
        + [pltpu.HBM((rows, cols // 4), BF16)] * 4,
        in_specs=[IN_HBM] * 7,
        out_specs=[IN_VMEM] + [IN_HBM] * 4,
        scratch_shapes=[
            pltpu.VMEM(queries.shape, BF16),
            pltpu.VMEM(token_keys.shape, BF16),
            pltpu.VMEM(token_values.shape, BF16),
            pltpu.SMEM(kv_len.shape, jnp.int32),
            pltpu.VMEM(stored_keys.shape, BF16),
            pltpu.VMEM(stored_values.shape, BF16),
            pltpu.VMEM((4, rows, cols // 4), BF16),
            pltpu.VMEM((seq_count * heads, HEAD_WIDTH), F32),
            pltpu.VMEM((seq_count * heads, HEAD_WIDTH), F32),
            pltpu.SemaphoreType.DMA((2, seq_count)),
            pltpu.SemaphoreType.DMA((12,)),
        ],
        compiler_params=pltpu.CompilerParams(vmem_limit_bytes=8 * MIB),
    )(
        *map(
            in_hbm,
            (queries, token_keys, token_values, kv_len, stored_keys, stored_values, out_weight),
        )
    )


def copy_all(pairs, sems):
    copies = [pltpu.make_async_copy(*pair, sems.at[j]) for j, pair in enumerate(pairs)]
    for copy in copies:
        copy.start()
    for copy in copies:
        copy.wait()


def stack_body(*refs):
    own, other, out_ref, sems = refs[:4], refs[4:8], refs[8], refs[9]
    rows = own[0].shape[0]
    pairs = []
    for d in range(4):
        for half, source in enumerate((own[d], other[d])):
            at = (d % 2 * 2 + half) * rows
            pairs.append((source, out_ref.at[d // 2, at : at + rows]))
    copy_all(pairs, sems)


def stack(own, other):
    rows, cols = own[0].shape
    return pl.pallas_call(
        stack_body,
        name="stack",
        out_shape=pltpu.VMEM((2, 4 * rows, cols), BF16),
        in_specs=[IN_HBM] * 8,
        out_specs=IN_VMEM,
        scratch_shapes=[pltpu.SemaphoreType.DMA((8,))],
        compiler_params=pltpu.CompilerParams(vmem_limit_bytes=2 * MIB),
    )(*map(in_hbm, own), *map(in_hbm, other))


def halves_body(gate_hbm, up_hbm, down_hbm, kept_ref, *refs):
    outs, (tall, wide, sems) = refs[:3], refs[3:]
    core = lax.axis_index(CORES)
    half = kept_ref.shape[0]
    kept, given = (pl.ds(pl.multiple_of(j * half, half), half) for j in (core, 1 - core))
    held = (tall.at[0], tall.at[1], wide)
    sources = (gate_hbm.at[0, given, :], up_hbm.at[0, given, :], down_hbm.at[0, :, given])
    loads = [pltpu.make_async_copy(sources[j], held[j], sems.at[j]) for j in range(3)]
    stores = [pltpu.make_async_copy(held[j], outs[j], sems.at[3 + j]) for j in range(3)]
    own = pltpu.make_async_copy(gate_hbm.at[0, kept, :], kept_ref, sems.at[6])
    for load in loads:
        load.start()
    own.start()
    for load, store in zip(loads, stores, strict=True):
        load.wait()
        store.start()
    own.wait()
    for store in stores:
        store.wait()


def halves(w_gate, w_up, w_down):
    _, width, units = w_gate.shape
    tall, wide = (width // 2, units), (units, width // 2)
    return pl.pallas_call(
        halves_body,
        name="halves",
        out_shape=[pltpu.VMEM(tall, BF16)] + [pltpu.HBM(dims, BF16) for dims in (tall, tall, wide)],
        in_specs=[IN_HBM] * 3,
        out_specs=[IN_VMEM] + [IN_HBM] * 3,
        scratch_shapes=[
            pltpu.VMEM((2, *tall), BF16),
            pltpu.VMEM(wide, BF16),
            pltpu.SemaphoreType.DMA((7,)),
        ],
        compiler_params=pltpu.CompilerParams(vmem_limit_bytes=6 * MIB),
    )(*map(in_hbm, (w_gate, w_up, w_down)))


def project_body(x_ref, weight_ref, out_ref):
    chips, tile, width = x_ref.shape
    cols = weight_ref.shape[2]
    half = cols // 2
    step = 16
    low = lax.broadcasted_iota(jnp.int32, (step, tile, half), 1) < tile // 2
    for at in range(0, chips, step):
        x = x_ref[at : at + step].reshape(step * tile, width)
        near, far = (
            jnp.dot(x, weight_ref[j], preferred_element_type=F32).reshape(step, tile, cols)
            for j in range(2)
        )
        kept = jnp.where(low, near[:, :, :half], far[:, :, half:])
        moved = jnp.where(low, near[:, :, half:], far[:, :, :half])
        moved = pltpu.roll(moved, tile // 2, 1)
        out_ref[at : at + step] = (kept + moved).astype(BF16)


def project(x, weight):
    cols = weight.shape[2]
    return kernel_call(
        project_body, pltpu.HBM((x.shape[0], x.shape[1], cols // 2), BF16), [IN_VMEM] * 2, 12
    )(x, in_vmem(weight))


def settle_body(x_ref, residual_ref, gain_ref, hidden_ref, kept_ref, given_ref, normed):
    core = lax.axis_index(CORES)
    chips, tile, half = x_ref.shape
    side = math.isqrt(chips)
    blocks = 4
    seq_count = tile // 2
    width = residual_ref.shape[1]

    def rows_of(ref, k):
        low, high = (ref[:, (2 * k + q) * half : (2 * k + q + 1) * half].astype(F32) for q in (0, 1))
        low, high = (jnp.broadcast_to(v, (seq_count, half)) for v in (low, high))
        return jnp.concatenate([low, high])

    square = jnp.zeros((tile, 1), F32)
    for k in range(blocks):
        total = rows_of(residual_ref, k)
        for x in range(k // 2, side, 2):
            for y in range(k % 2, side, 2):
                total = total + x_ref[x * side + y].astype(F32)
        hidden_ref[k] = total
        square = square + jnp.sum(total * total, axis=1, keepdims=True)
    square = jnp.broadcast_to(square, (tile, HEAD_WIDTH))
    square = square + pltpu.roll(square, seq_count, 0)
    scale = lax.rsqrt(square[:, :1] / width + 1e-06)
    for k in range(blocks):
        normed[k] = (hidden_ref[k] * scale * rows_of(gain_ref, k)).astype(BF16)
    kept_ref[...] = normed[pl.ds(core * 2, 2)]
    given_ref[...] = normed[pl.ds(2 - core * 2, 2)]


def settle(x, residual, gain):
    tile, half = x.shape[1:]
    return kernel_call(
        settle_body,
        (shape(4, tile, half, dtype=F32), shape(2, tile, half), shape(2, tile, half)),
        [IN_VMEM] * 3,
        6,
        [pltpu.VMEM((4, tile, half), BF16)],
    )(x, residual, gain)


def route_body(ids_ref, weight_ref, pick_ref, mix_ref):
    core = lax.axis_index(CORES)
    tokens, topk = ids_ref.shape
    seq_count = tokens // 2
    lanes = pick_ref.shape[1]
    lane = lax.broadcasted_iota(jnp.int32, (tokens, lanes), 1)
    row = lax.broadcasted_iota(jnp.int32, (tokens, lanes), 0)
    weight = weight_ref[...]
    mixing = weight / jnp.sum(weight, axis=1, keepdims=True)
    ids = ids_ref[...]
    hit = jnp.zeros((tokens, lanes), F32)
    share = jnp.zeros((tokens, lanes), F32)
    for k in range(topk):
        same = ids[:, k : k + 1] == lane // 8
        hit = jnp.where(same, 1.0, hit)
        share = jnp.where(same, mixing[:, k : k + 1], share)
    rank = jnp.zeros((tokens, lanes), F32)
    for t in range(tokens - 1):
        rank = rank + jnp.where(row > t, jnp.broadcast_to(hit[t : t + 1], (tokens, lanes)), 0.0)
    taken = jnp.where(rank == (lane % 2).astype(F32), hit, 0.0)
    share = share * taken
    own_low = (row < seq_count) == (core == 0)
    quarter = lane // 2 % 4
    for src in range(2):
        low = own_low if src == 0 else jnp.logical_not(own_low)
        chosen = jnp.where(low, taken, pltpu.roll(taken, seq_count, 0))
        shares = jnp.where(low, share, pltpu.roll(share, seq_count, 0))
        for kk in range(2):
            at = (src * 2 + kk) * tokens
            mine = quarter == kk * 2 + row // seq_count
            pick_ref[at : at + tokens, :] = jnp.where(mine, chosen, 0.0).astype(BF16)
            value = jnp.where(mine, shares, 0.0)
            coarse = value.astype(BF16)
            mix_ref[at : at + tokens, :] = coarse
            mix_ref[4 * tokens + at : 5 * tokens + at, :] = (value - coarse.astype(F32)).astype(BF16)


def route(expert_ids, route_weight, chips):
    tokens = expert_ids.shape[0]
    return kernel_call(
        route_body, (shape(4 * tokens, 8 * chips), shape(8 * tokens, 8 * chips)), [IN_VMEM] * 2, 4
    )(expert_ids, route_weight)


def dispatch_body(kept_ref, other_ref, pick_ref, out_ref):
    pieces = [r[...].reshape(-1, r.shape[2]) for r in (kept_ref, other_ref)]
    rows = lax.dot_general(
        pick_ref[...],
        jnp.concatenate(pieces),
        (((0,), (0,)), ((), ())),
        preferred_element_type=F32,
    )
    out_ref[...] = rows.astype(BF16).reshape(out_ref.shape)


def dispatch(kept, other, pick):
    tile, half = kept.shape[1:]
    return kernel_call(
        dispatch_body, pltpu.HBM((pick.shape[1] // tile, tile, half), BF16), [IN_VMEM] * 3, 6
    )(kept, other, pick)


def slot_order(size, back=False):
    sorted_row = lax.broadcasted_iota(jnp.int32, (size, size), 1 if back else 0)
    row = lax.broadcasted_iota(jnp.int32, (size, size), 0 if back else 1)
    slot = sorted_row % (size // 4)
    quarter = sorted_row // (size // 4)
    return jnp.where(row == slot // 2 * 8 + quarter * 2 + slot % 2, 1.0, 0.0).astype(BF16)


def gate_body(
    x_ref,
    gate_ref,
    up_hbm,
    down_hbm,
    gate_moved,
    up_moved,
    down_moved,
    part_ref,
    sent_ref,
    down_ref,
    buffers,
    sems,
):
    core = lax.axis_index(CORES)
    chips, tile, part = x_ref.shape
    half, units = gate_ref.shape
    kept = pl.ds(pl.multiple_of(core * half, half), half)
    pairs = (
        (up_hbm.at[0, kept, :], buffers.at[0]),
        (gate_moved, buffers.at[1]),
        (up_moved, buffers.at[2]),
        (down_hbm.at[0, :, kept], down_ref.at[:units]),
        (down_moved, down_ref.at[units:]),
    )
    copies = [pltpu.make_async_copy(*pair, sems.at[j]) for j, pair in enumerate(pairs)]
    for copy in copies:
        copy.start()
    size = 256
    groups = chips * tile // size
    order = slot_order(size)
    slots = size // 4
    sorted_rows = []
    for g in range(groups):
        rows = x_ref[g * size // tile : (g + 1) * size // tile].reshape(size, part)
        sorted_rows.append(jnp.dot(order, rows, preferred_element_type=F32).astype(BF16))
    quarters = [
        jnp.concatenate([r[p * slots : (p + 1) * slots] for r in sorted_rows]) for p in range(4)
    ]
    x = jnp.concatenate(quarters, axis=1)
    for j in range(4):
        if j:
            copies[j - 1].wait()
        weight = buffers[j - 1] if j else gate_ref[...]
        value = jnp.dot(x, weight, preferred_element_type=F32)
        part_ref[:, j * units : (j + 1) * units] = value
        at = (j + 2) % 4 * units
        sent_ref[:, at : at + units] = value.astype(BF16)
    for copy in copies[3:]:
        copy.wait()


def gate_up(x, gate_own, w_up, w_down, moved):
    chips, tile, _ = x.shape
    half, units = gate_own.shape
    dims = chips * tile // 4, 4 * units
    return pl.pallas_call(
        gate_body,
        name="gate_up",
        out_shape=[
            pltpu.VMEM(dims, F32),
            pltpu.VMEM(dims, BF16),
            pltpu.VMEM((2 * units, half), BF16),
        ],
        in_specs=[IN_VMEM] * 2 + [IN_HBM] * 5,
        out_specs=[IN_VMEM] * 3,
        scratch_shapes=[pltpu.VMEM((3, half, units), BF16), pltpu.SemaphoreType.DMA((5,))],
        compiler_params=pltpu.CompilerParams(vmem_limit_bytes=16 * MIB),
    )(x, in_vmem(gate_own), *map(in_hbm, (w_up, w_down, *moved)))


def down_body(part_ref, arrived_ref, down_ref, out_ref):
    chips, tile, part = out_ref.shape
    size = 256
    groups = chips * tile // size
    order = slot_order(size, back=True)
    slots = size // 4
    units = down_ref.shape[0] // 2

    def act(at):
        gate, up = (
            part_ref[:, j : j + units] + arrived_ref[:, j : j + units].astype(F32)
            for j in (at, at + units)
        )
        return (gate / (1.0 + jnp.exp(-gate)) * up).astype(BF16)

    hidden = jnp.concatenate([act(0), act(2 * units)], axis=1)
    quarters = []
    for p in range(4):
        lanes = slice(p * part, (p + 1) * part)
        value = jnp.dot(hidden, down_ref[:, lanes], preferred_element_type=F32)
        quarters.append(value.astype(BF16))
    for g in range(groups):
        rows = jnp.concatenate([v[g * slots : (g + 1) * slots] for v in quarters])
        rows = jnp.dot(order, rows, preferred_element_type=F32).astype(BF16)
        out_ref[g * size // tile : (g + 1) * size // tile] = rows.reshape(size // tile, tile, part)


def down(part, arrived, weight, tile):
    slots = part.shape[0]
    width = weight.shape[1] // 4
    return kernel_call(
        down_body, pltpu.HBM((slots * 4 // tile, tile, width), BF16), [IN_VMEM] * 3, 8
    )(part, arrived, in_vmem(weight))


def combine_body(x_ref, mix_ref, own_ref, other_ref):
    x = x_ref[...].reshape(-1, x_ref.shape[2])
    rows = jnp.dot(mix_ref[...], x, preferred_element_type=F32)
    count = rows.shape[0] // 2
    rows = rows[:count] + rows[count:]
    own_ref[...] = rows[: count // 2].reshape(own_ref.shape)
    other_ref[...] = rows[count // 2 :].reshape(other_ref.shape)


def combine(x, mix):
    out = shape(2, x.shape[1], x.shape[2], dtype=F32)
    return kernel_call(combine_body, (out, out), [IN_VMEM] * 2, 4)(x, mix)


def finish_body(hidden_ref, own_ref, other_ref, out_ref, total):
    core = lax.axis_index(CORES)
    blocks, tile, half = hidden_ref.shape
    total[pl.ds(core * 2, 2)] = own_ref[...]
    total[pl.ds(2 - core * 2, 2)] = other_ref[...]
    for k in range(blocks):
        value = (hidden_ref[k] + total[k]).astype(BF16)
        for q in range(2):
            at = (2 * k + q) * half
            out_ref[:, at : at + half] = value[q * tile // 2 : (q + 1) * tile // 2]


def finish(hidden, own, other):
    blocks, tile, half = hidden.shape
    return kernel_call(
        finish_body, shape(tile // 2, 2 * blocks * half), [IN_VMEM] * 3, 2, [pltpu.VMEM(hidden.shape, F32)]
    )(hidden, own, other)


def on_device(
    queries,
    token_keys,
    token_values,
    stored_keys,
    stored_values,
    kv_len,
    residual,
    out_weight,
    norm_gain,
    expert_ids,
    route_weight,
    w_gate,
    w_up,
    w_down,
):
    chips = lax.axis_size(CHIPS)
    side = math.isqrt(chips)
    outgoing, *pieces = attend(
        queries, token_keys, token_values, kv_len, stored_keys, stored_values, out_weight
    )
    own = [pieces[0]] + [
        lax.ppermute(pieces[d], CHIPS, quad_step(side, d // 2, d % 2)) for d in (1, 2, 3)
    ]
    tokens = lax.all_to_all(outgoing, CHIPS, 0, 0, tiled=True)
    other = [swapped(piece) for piece in own]
    weight = stack(own, other)
    gate_own, *given_halves = halves(w_gate, w_up, w_down)
    moved = [swapped(x) for x in given_halves]
    pick, mix = route(expert_ids, route_weight, chips)

    sums = project(tokens, weight)
    came_back = lax.all_to_all(sums, CHIPS, 0, 0, tiled=True)
    hidden, normed, normed_given = settle(came_back, residual, norm_gain[None])
    outgoing = dispatch(normed, swapped(normed_given), pick)
    incoming = lax.all_to_all(outgoing, CHIPS, 0, 0, tiled=True)
    part, sent, down_weight = gate_up(incoming, gate_own, w_up, w_down, moved)
    expert_out = down(part, swapped(sent), down_weight, incoming.shape[1])
    returned = lax.all_to_all(expert_out, CHIPS, 0, 0, tiled=True)
    moe_own, moe_given = combine(returned, mix)
    return finish(hidden, moe_own, swapped(moe_given))


def solution(mesh):
    in_specs = (
        P(("groups", "expert", "replica"), None),
        P(("groups", "expert", "replica"), None),
        P(("groups", "expert", "replica"), None),
        P(("groups", "expert", "replica"), None, None),
        P(("groups", "expert", "replica"), None, None),
        P(("groups", "expert", "replica")),
        P(("groups", "expert", "replica"), None),
        P(("expert", "replica"), None),
        P(),
        P(("groups", "expert"), None),
        P(("groups", "expert"), None),
        P("expert", None, "replica"),
        P("expert", None, "replica"),
        P("expert", "replica", None),
    )
    out_specs = P(("groups", "expert", "replica"), None)
    return jax.shard_map(
        on_device, mesh=mesh, in_specs=in_specs, out_specs=out_specs, check_vma=False
    )
```

```python
import math

import jax
import jax.numpy as jnp
from jax import lax
from jax.experimental import pallas as pl
from jax.experimental.pallas import tpu as pltpu
from jax.sharding import PartitionSpec as P

HEAD_WIDTH = 128
CHIPS, CORES = "expert", "replica"
F32, BF16 = jnp.float32, jnp.bfloat16
IN_VMEM = pl.BlockSpec(memory_space=pltpu.VMEM)
IN_SMEM = pl.BlockSpec(memory_space=pltpu.SMEM)
IN_HBM = pl.BlockSpec(memory_space=pltpu.HBM)


def swapped(x):
    return lax.ppermute(x, CORES, [(0, 1), (1, 0)])


def quad_step(side, dx, dy):
    return [
        (x * side + y, (x ^ dx) * side + (y ^ dy)) for x in range(side) for y in range(side)
    ]


MIB = 1 << 20


def in_hbm(x):
    return pltpu.with_memory_space_constraint(x, pltpu.HBM)


def in_vmem(x):
    return pltpu.with_memory_space_constraint(x, pltpu.VMEM)


def kernel_call(body, outs, in_specs, limit, scratch=()):
    return pl.pallas_call(
        body,
        out_shape=outs,
        in_specs=in_specs,
        out_specs=jax.tree.map(lambda _: IN_VMEM, outs),
        scratch_shapes=list(scratch),
        compiler_params=pltpu.CompilerParams(vmem_limit_bytes=limit * MIB),
    )


def shape(*dims, dtype=BF16):
    return jax.ShapeDtypeStruct(dims, dtype)


def attend_body(
    q_hbm,
    tk_hbm,
    tv_hbm,
    len_hbm,
    keys_hbm,
    values_hbm,
    weight_hbm,
    out_hbm,
    piece0,
    piece1,
    piece2,
    piece3,
    q_ref,
    tk_ref,
    tv_ref,
    len_ref,
    keys,
    values,
    pieces,
    rows,
    mixed,
    scored,
    out_ref,
    sems,
    few,
):
    core = lax.axis_index(CORES)
    seq_count, cache_len, kv_width = keys_hbm.shape
    kv_count = kv_width // HEAD_WIDTH
    head_count = q_hbm.shape[1] // HEAD_WIDTH
    group = head_count // kv_count
    side = group // 2
    small = [
        pltpu.make_async_copy(source, target, few.at[j])
        for j, (source, target) in enumerate(
            ((q_hbm, q_ref), (tk_hbm, tk_ref), (tv_hbm, tv_ref), (len_hbm, len_ref))
        )
    ]
    for copy in small:
        copy.start()
    copies = [
        [pltpu.make_async_copy(source.at[b], target.at[b], sems.at[j, b]) for b in range(seq_count)]
        for j, (source, target) in enumerate(((keys_hbm, keys), (values_hbm, values)))
    ]
    for copy in copies[0] + copies[1]:
        copy.start()
    chip = lax.axis_index(CHIPS)
    place = chip // side % 2 * 2 + chip % 2
    sliced, stored = [], []
    for d, piece in enumerate((piece0, piece1, piece2, piece3)):
        cols = piece.shape[1]
        at = pl.multiple_of((place ^ d) * cols, cols)
        source = weight_hbm.at[:, pl.ds(at, cols)]
        sliced.append(pltpu.make_async_copy(source, pieces.at[d], few.at[len(small) + d]))
        stored.append(pltpu.make_async_copy(pieces.at[d], piece, few.at[len(small) + 4 + d]))
        sliced[-1].start()
    for copy in small:
        copy.wait()
    for h in range(head_count):
        piece = q_ref[:, h * HEAD_WIDTH : (h + 1) * HEAD_WIDTH].astype(F32)
        rows[pl.ds(h, seq_count, stride=head_count), :] = piece
    inv_root = 1.0 / math.sqrt(HEAD_WIDTH)
    positions = lax.broadcasted_iota(jnp.int32, (head_count, cache_len), 1)
    lanes = [slice(g * HEAD_WIDTH, (g + 1) * HEAD_WIDTH) for g in range(kv_count)]
    fresh = []
    for copy in copies[0]:
        copy.wait()
    for b in range(seq_count):
        query = rows[b * head_count : (b + 1) * head_count, :]
        latest = [tk_ref[b : b + 1, lanes[g]].astype(F32) for g in range(kv_count)]
        latest = jnp.concatenate([jnp.broadcast_to(v, (group, HEAD_WIDTH)) for v in latest])
        fresh.append(jnp.sum(query * latest, axis=1, keepdims=True) * inv_root)
        query = query.astype(BF16)
        for g in range(kv_count):
            at = b * head_count + g * group
            scored[at : at + group, :] = lax.dot_general(
                query[g * group : (g + 1) * group],
                keys[b, :, lanes[g]],
                (((1,), (1,)), ((), ())),
                preferred_element_type=F32,
            )
    for copy in copies[1] + sliced:
        copy.wait()
    for copy in stored:
        copy.start()
    probs, fresh_probs = [], []
    for b in range(seq_count):
        scores = scored[b * head_count : (b + 1) * head_count, :]
        scores = jnp.where(positions < len_ref[b], scores * inv_root, -jnp.inf)
        highest = jnp.maximum(jnp.max(scores, axis=1, keepdims=True), fresh[b])
        cached_exp = jnp.exp(scores - highest)
        fresh_exp = jnp.exp(fresh[b] - highest)
        share = 1.0 / (jnp.sum(cached_exp, axis=1, keepdims=True) + fresh_exp)
        probs.append((cached_exp * share).astype(BF16))
        fresh_probs.append((fresh_exp * share).astype(BF16).astype(F32))
    for b in range(seq_count):
        for g in range(kv_count):
            heads = slice(g * group, (g + 1) * group)
            out = jnp.dot(probs[b][heads], values[b, :, lanes[g]], preferred_element_type=F32)
            out = out + fresh_probs[b][heads] * tv_ref[b : b + 1, lanes[g]].astype(F32)
            out = pltpu.roll(out, core * (HEAD_WIDTH // 2), 1)
            for a in range(2):
                start = g * group * seq_count + a * seq_count + b
                mixed[pl.ds(start, side, stride=2 * seq_count), :] = out[a * side : (a + 1) * side]
    tile = 2 * seq_count
    for g in range(kv_count):
        for y in range(side):
            for part, source in enumerate((y, y ^ 1)):
                at = (g * side + source) * tile
                near = mixed[at : at + tile, :]
                far = pltpu.roll(near, seq_count, 0)
                out_ref[2 * g * side + y, :, lanes[part]] = near.astype(BF16)
                out_ref[(2 * g + 1) * side + y, :, lanes[part]] = far.astype(BF16)
        sent = pl.ds(2 * g * side, 2 * side)
        stored.append(
            pltpu.make_async_copy(out_ref.at[sent], out_hbm.at[sent], few.at[len(small) + 8 + g])
        )
        stored[-1].start()
    for copy in stored:
        copy.wait()


def attend(queries, token_keys, token_values, kv_len, stored_keys, stored_values, out_weight):
    seq_count, feature_total = queries.shape
    heads = feature_total // HEAD_WIDTH
    rows, cols = out_weight.shape
    return pl.pallas_call(
        attend_body,
        name="attend",
        out_shape=[pltpu.HBM((heads, 2 * seq_count, 2 * HEAD_WIDTH), BF16)]
        + [pltpu.HBM((rows, cols // 4), BF16)] * 4,
        in_specs=[IN_HBM] * 7,
        out_specs=[IN_HBM] * 5,
        scratch_shapes=[
            pltpu.VMEM(queries.shape, BF16),
            pltpu.VMEM(token_keys.shape, BF16),
            pltpu.VMEM(token_values.shape, BF16),
            pltpu.SMEM(kv_len.shape, jnp.int32),
            pltpu.VMEM(stored_keys.shape, BF16),
            pltpu.VMEM(stored_values.shape, BF16),
            pltpu.VMEM((4, rows, cols // 4), BF16),
            pltpu.VMEM((seq_count * heads, HEAD_WIDTH), F32),
            pltpu.VMEM((seq_count * heads, HEAD_WIDTH), F32),
            pltpu.VMEM((seq_count * heads, stored_keys.shape[1]), F32),
            pltpu.VMEM((heads, 2 * seq_count, 2 * HEAD_WIDTH), BF16),
            pltpu.SemaphoreType.DMA((2, seq_count)),
            pltpu.SemaphoreType.DMA((16,)),
        ],
        compiler_params=pltpu.CompilerParams(vmem_limit_bytes=8 * MIB),
    )(
        *map(
            in_hbm,
            (queries, token_keys, token_values, kv_len, stored_keys, stored_values, out_weight),
        )
    )


def copy_all(pairs, sems):
    copies = [pltpu.make_async_copy(*pair, sems.at[j]) for j, pair in enumerate(pairs)]
    for copy in copies:
        copy.start()
    for copy in copies:
        copy.wait()


def stack_body(*refs):
    own, other, out_ref, sems = refs[:4], refs[4:8], refs[8], refs[9]
    rows = own[0].shape[0]
    pairs = []
    for d in range(4):
        for half, source in enumerate((own[d], other[d])):
            at = (d % 2 * 2 + half) * rows
            pairs.append((source, out_ref.at[d // 2, at : at + rows]))
    copy_all(pairs, sems)


def stack(own, other):
    rows, cols = own[0].shape
    return pl.pallas_call(
        stack_body,
        name="stack",
        out_shape=pltpu.VMEM((2, 4 * rows, cols), BF16),
        in_specs=[IN_HBM] * 8,
        out_specs=IN_VMEM,
        scratch_shapes=[pltpu.SemaphoreType.DMA((8,))],
        compiler_params=pltpu.CompilerParams(vmem_limit_bytes=2 * MIB),
    )(*map(in_hbm, own), *map(in_hbm, other))


def halves_body(gate_hbm, up_hbm, down_hbm, kept_ref, *refs):
    outs, (tall, wide, sems) = refs[:2], refs[2:]
    core = lax.axis_index(CORES)
    count = kept_ref.shape[0]
    half, both = tall.shape
    units = both // 2
    given = pl.ds(pl.multiple_of((1 - core) * half, half), half)
    kept = pl.ds(pl.multiple_of(core * half, half), count)
    left, right = slice(0, units), slice(units, both)
    pairs = (
        (gate_hbm.at[0, given, :], tall.at[:, left]),
        (up_hbm.at[0, given, :], tall.at[:, right]),
        (down_hbm.at[0, :, given], wide),
        (gate_hbm.at[0, kept, :], kept_ref.at[:, left]),
        (up_hbm.at[0, kept, :], kept_ref.at[:, right]),
        (tall, outs[0]),
        (wide, outs[1]),
    )
    copies = [pltpu.make_async_copy(*pair, sems.at[j]) for j, pair in enumerate(pairs)]
    for copy in copies[:5]:
        copy.start()
    for copy in copies[:2]:
        copy.wait()
    copies[5].start()
    copies[2].wait()
    copies[6].start()
    for copy in copies[3:]:
        copy.wait()


def halves(w_gate, w_up, w_down, kept_share):
    _, width, units = w_gate.shape
    tall, wide = (width // 2, 2 * units), (units, width // 2)
    return pl.pallas_call(
        halves_body,
        name="halves",
        out_shape=[
            pltpu.VMEM((int(width // 2 * kept_share), 2 * units), BF16),
            pltpu.HBM(tall, BF16),
            pltpu.HBM(wide, BF16),
        ],
        in_specs=[IN_HBM] * 3,
        out_specs=[IN_VMEM] + [IN_HBM] * 2,
        scratch_shapes=[
            pltpu.VMEM(tall, BF16),
            pltpu.VMEM(wide, BF16),
            pltpu.SemaphoreType.DMA((7,)),
        ],
        compiler_params=pltpu.CompilerParams(vmem_limit_bytes=6 * MIB),
    )(*map(in_hbm, (w_gate, w_up, w_down)))


def project_body(x_ref, weight_ref, out_hbm, held, sems):
    chips, tile, width = x_ref.shape
    cols = weight_ref.shape[2]
    half = cols // 2
    step = 16
    low = lax.broadcasted_iota(jnp.int32, (step, tile, half), 1) < tile // 2
    copies = []
    for j, at in enumerate(range(0, chips, step)):
        rows = slice(at, at + step)
        x = x_ref[rows].reshape(step * tile, width)
        near, far = (
            jnp.dot(x, weight_ref[j], preferred_element_type=F32).reshape(step, tile, cols)
            for j in range(2)
        )
        kept = jnp.where(low, near[:, :, :half], far[:, :, half:])
        moved = jnp.where(low, near[:, :, half:], far[:, :, :half])
        moved = pltpu.roll(moved, tile // 2, 1)
        held[rows] = (kept + moved).astype(BF16)
        copies.append(pltpu.make_async_copy(held.at[rows], out_hbm.at[rows], sems.at[j]))
        copies[-1].start()
    for copy in copies:
        copy.wait()


def sending_call(body, dims, in_specs, limit, chunks):
    return pl.pallas_call(
        body,
        out_shape=pltpu.HBM(dims, BF16),
        in_specs=in_specs,
        out_specs=IN_HBM,
        scratch_shapes=[pltpu.VMEM(dims, BF16), pltpu.SemaphoreType.DMA((chunks,))],
        compiler_params=pltpu.CompilerParams(vmem_limit_bytes=limit * MIB),
    )


def project(x, weight):
    dims = x.shape[0], x.shape[1], weight.shape[2] // 2
    return sending_call(project_body, dims, [IN_VMEM] * 2, 12, x.shape[0] // 16)(
        x, in_vmem(weight)
    )


def project_body(x_ref, weight_ref, out_ref):
    chips, tile, width = x_ref.shape
    cols = weight_ref.shape[2]
    half = cols // 2
    step = 16
    low = lax.broadcasted_iota(jnp.int32, (step, tile, half), 1) < tile // 2
    for at in range(0, chips, step):
        x = x_ref[at : at + step].reshape(step * tile, width)
        near, far = (
            jnp.dot(x, weight_ref[j], preferred_element_type=F32).reshape(step, tile, cols)
            for j in range(2)
        )
        kept = jnp.where(low, near[:, :, :half], far[:, :, half:])
        moved = jnp.where(low, near[:, :, half:], far[:, :, :half])
        moved = pltpu.roll(moved, tile // 2, 1)
        out_ref[at : at + step] = (kept + moved).astype(BF16)


def project(x, weight):
    cols = weight.shape[2]
    return kernel_call(
        project_body, pltpu.HBM((x.shape[0], x.shape[1], cols // 2), BF16), [IN_VMEM] * 2, 12
    )(x, in_vmem(weight))


def settle_body(x_ref, residual_ref, gain_ref, hidden_ref, kept_ref, given_ref, normed):
    core = lax.axis_index(CORES)
    chips, tile, half = x_ref.shape
    side = math.isqrt(chips)
    blocks = 4
    seq_count = tile // 2
    width = residual_ref.shape[1]

    def rows_of(ref, k):
        low, high = (ref[:, (2 * k + q) * half : (2 * k + q + 1) * half].astype(F32) for q in (0, 1))
        low, high = (jnp.broadcast_to(v, (seq_count, half)) for v in (low, high))
        return jnp.concatenate([low, high])

    square = jnp.zeros((tile, 1), F32)
    for k in range(blocks):
        total = rows_of(residual_ref, k)
        for x in range(k // 2, side, 2):
            for y in range(k % 2, side, 2):
                total = total + x_ref[x * side + y].astype(F32)
        hidden_ref[k] = total
        square = square + jnp.sum(total * total, axis=1, keepdims=True)
    square = jnp.broadcast_to(square, (tile, HEAD_WIDTH))
    square = square + pltpu.roll(square, seq_count, 0)
    scale = lax.rsqrt(square[:, :1] / width + 1e-06)
    for k in range(blocks):
        normed[k] = (hidden_ref[k] * scale * rows_of(gain_ref, k)).astype(BF16)
    kept_ref[...] = normed[pl.ds(core * 2, 2)]
    given_ref[...] = normed[pl.ds(2 - core * 2, 2)]


def settle(x, residual, gain):
    tile, half = x.shape[1:]
    return kernel_call(
        settle_body,
        (shape(4, tile, half, dtype=F32), shape(2, tile, half), shape(2, tile, half)),
        [IN_VMEM] * 3,
        6,
        [pltpu.VMEM((4, tile, half), BF16)],
    )(x, residual, gain)


def route_body(ids_ref, weight_ref, pick_ref, mix_ref):
    core = lax.axis_index(CORES)
    tokens, topk = ids_ref.shape
    seq_count = tokens // 2
    lanes = pick_ref.shape[1]
    lane = lax.broadcasted_iota(jnp.int32, (tokens, lanes), 1)
    row = lax.broadcasted_iota(jnp.int32, (tokens, lanes), 0)
    weight = weight_ref[...]
    mixing = weight / jnp.sum(weight, axis=1, keepdims=True)
    ids = ids_ref[...]
    hit = jnp.zeros((tokens, lanes), F32)
    share = jnp.zeros((tokens, lanes), F32)
    for k in range(topk):
        same = ids[:, k : k + 1] == lane // 8
        hit = jnp.where(same, 1.0, hit)
        share = jnp.where(same, mixing[:, k : k + 1], share)
    rank = jnp.zeros((tokens, lanes), F32)
    for t in range(tokens - 1):
        rank = rank + jnp.where(row > t, jnp.broadcast_to(hit[t : t + 1], (tokens, lanes)), 0.0)
    taken = jnp.where(rank == (lane % 2).astype(F32), hit, 0.0)
    share = share * taken
    own_low = (row < seq_count) == (core == 0)
    quarter = lane // 2 % 4
    for src in range(2):
        low = own_low if src == 0 else jnp.logical_not(own_low)
        chosen = jnp.where(low, taken, pltpu.roll(taken, seq_count, 0))
        shares = jnp.where(low, share, pltpu.roll(share, seq_count, 0))
        for kk in range(2):
            at = (src * 2 + kk) * tokens
            mine = quarter == kk * 2 + row // seq_count
            pick_ref[at : at + tokens, :] = jnp.where(mine, chosen, 0.0).astype(BF16)
            value = jnp.where(mine, shares, 0.0)
            coarse = value.astype(BF16)
            mix_ref[at : at + tokens, :] = coarse
            mix_ref[4 * tokens + at : 5 * tokens + at, :] = (value - coarse.astype(F32)).astype(BF16)


def route(expert_ids, route_weight, chips):
    tokens = expert_ids.shape[0]
    return kernel_call(
        route_body, (shape(4 * tokens, 8 * chips), shape(8 * tokens, 8 * chips)), [IN_VMEM] * 2, 4
    )(expert_ids, route_weight)


def dispatch_body(kept_ref, other_ref, pick_ref, out_hbm, held, sems):
    pieces = [r[...].reshape(-1, r.shape[2]) for r in (kept_ref, other_ref)]
    tokens = jnp.concatenate(pieces)
    chips, tile, half = held.shape
    step = chips // 2
    copies = []
    for j in range(2):
        rows = lax.dot_general(
            pick_ref[:, j * step * tile : (j + 1) * step * tile],
            tokens,
            (((0,), (0,)), ((), ())),
            preferred_element_type=F32,
        )
        sent = slice(j * step, (j + 1) * step)
        held[sent] = rows.astype(BF16).reshape(step, tile, half)
        copies.append(pltpu.make_async_copy(held.at[sent], out_hbm.at[sent], sems.at[j]))
        copies[-1].start()
    for copy in copies:
        copy.wait()


def dispatch(kept, other, pick):
    tile, half = kept.shape[1:]
    dims = pick.shape[1] // tile, tile, half
    return sending_call(dispatch_body, dims, [IN_VMEM] * 3, 6, 2)(kept, other, pick)


def slot_order(size, back=False):
    sorted_row = lax.broadcasted_iota(jnp.int32, (size, size), 1 if back else 0)
    row = lax.broadcasted_iota(jnp.int32, (size, size), 0 if back else 1)
    slot = sorted_row % (size // 4)
    quarter = sorted_row // (size // 4)
    return jnp.where(row == slot // 2 * 8 + quarter * 2 + slot % 2, 1.0, 0.0).astype(BF16)


def gate_body(x_ref, kept_ref, gate_hbm, up_hbm, moved_hbm, part_ref, sent_ref, rest, moved, sems):
    core = lax.axis_index(CORES)
    chips, tile, part = x_ref.shape
    half, both = moved.shape
    units = both // 2
    count = kept_ref.shape[0]
    late = pl.ds(pl.multiple_of(core * half + count, part), half - count)
    pairs = [(gate_hbm.at[0, late, :], rest.at[:, :units]), (up_hbm.at[0, late, :], rest.at[:, units:])]
    step = half // 2
    for j in range(2):
        rows = slice(j * step, (j + 1) * step)
        pairs.append((moved_hbm.at[rows], moved.at[rows]))
    copies = [pltpu.make_async_copy(*pair, sems.at[j]) for j, pair in enumerate(pairs)]
    for copy in copies:
        copy.start()
    size = 256
    groups = chips * tile // size
    order = slot_order(size)
    slots = size // 4
    sorted_rows = []
    for g in range(groups):
        rows = x_ref[g * size // tile : (g + 1) * size // tile].reshape(size, part)
        sorted_rows.append(jnp.dot(order, rows, preferred_element_type=F32).astype(BF16))
    quarters = [
        jnp.concatenate([r[p * slots : (p + 1) * slots] for r in sorted_rows]) for p in range(4)
    ]
    x = jnp.concatenate(quarters, axis=1)
    own = jnp.dot(x[:, :count], kept_ref[...], preferred_element_type=F32)
    for copy in copies[:2]:
        copy.wait()
    own = own + jnp.dot(x[:, count:], rest[...], preferred_element_type=F32)
    part_ref[:, :both] = own
    sent_ref[:, both:] = own.astype(BF16)
    copies[2].wait()
    other = jnp.dot(x[:, :step], moved[:step], preferred_element_type=F32)
    copies[3].wait()
    other = other + jnp.dot(x[:, step:], moved[step:], preferred_element_type=F32)
    part_ref[:, both:] = other
    sent_ref[:, :both] = other.astype(BF16)


def gate_up(x, kept, w_gate, w_up, moved):
    chips, tile, _ = x.shape
    half, both = moved.shape
    dims = chips * tile // 4, 2 * both
    return pl.pallas_call(
        gate_body,
        name="gate_up",
        out_shape=[pltpu.VMEM(dims, F32), pltpu.VMEM(dims, BF16)],
        in_specs=[IN_VMEM] * 2 + [IN_HBM] * 3,
        out_specs=[IN_VMEM] * 2,
        scratch_shapes=[
            pltpu.VMEM((half - kept.shape[0], both), BF16),
            pltpu.VMEM((half, both), BF16),
            pltpu.SemaphoreType.DMA((4,)),
        ],
        compiler_params=pltpu.CompilerParams(vmem_limit_bytes=14 * MIB),
    )(x, in_vmem(kept), *map(in_hbm, (w_gate, w_up, moved)))


def fetch_body(down_hbm, moved_hbm, after_ref, out_ref, sems):
    del after_ref
    core = lax.axis_index(CORES)
    units, half = moved_hbm.shape
    kept = pl.ds(pl.multiple_of(core * half, half), half)
    copies = [
        pltpu.make_async_copy(down_hbm.at[0, :, kept], out_ref.at[:units], sems.at[0]),
        pltpu.make_async_copy(moved_hbm, out_ref.at[units:], sems.at[1]),
    ]
    for copy in copies:
        copy.start()
    for copy in copies:
        copy.wait()


def fetch_down(w_down, moved, after):
    units, half = moved.shape
    return pl.pallas_call(
        fetch_body,
        name="fetch_down",
        out_shape=pltpu.VMEM((2 * units, half), BF16),
        in_specs=[IN_HBM] * 3,
        out_specs=IN_VMEM,
        scratch_shapes=[pltpu.SemaphoreType.DMA((2,))],
        compiler_params=pltpu.CompilerParams(vmem_limit_bytes=MIB),
    )(in_hbm(w_down), in_hbm(moved), after)


def down_body(part_ref, arrived_ref, down_ref, out_hbm, held, sems):
    chips, tile, part = held.shape
    size = 256
    groups = chips * tile // size
    order = slot_order(size, back=True)
    slots = size // 4
    units = down_ref.shape[0] // 2

    def act(at):
        gate, up = (
            part_ref[:, j : j + units] + arrived_ref[:, j : j + units].astype(F32)
            for j in (at, at + units)
        )
        return (gate / (1.0 + jnp.exp(-gate)) * up).astype(BF16)

    hidden = jnp.concatenate([act(0), act(2 * units)], axis=1)
    quarters = []
    for p in range(4):
        lanes = slice(p * part, (p + 1) * part)
        value = jnp.dot(hidden, down_ref[:, lanes], preferred_element_type=F32)
        quarters.append(value.astype(BF16))
    copies = []
    for g in range(groups):
        rows = jnp.concatenate([v[g * slots : (g + 1) * slots] for v in quarters])
        rows = jnp.dot(order, rows, preferred_element_type=F32).astype(BF16)
        sent = slice(g * size // tile, (g + 1) * size // tile)
        held[sent] = rows.reshape(size // tile, tile, part)
        copies.append(pltpu.make_async_copy(held.at[sent], out_hbm.at[sent], sems.at[g]))
        copies[-1].start()
    for copy in copies:
        copy.wait()


def down(part, arrived, weight, tile):
    dims = part.shape[0] * 4 // tile, tile, weight.shape[1] // 4
    return sending_call(down_body, dims, [IN_VMEM] * 3, 8, 2)(
        part, arrived, in_vmem(weight)
    )


def combine_body(x_ref, mix_ref, own_ref, other_ref):
    x = x_ref[...].reshape(-1, x_ref.shape[2])
    rows = jnp.dot(mix_ref[...], x, preferred_element_type=F32)
    count = rows.shape[0] // 2
    rows = rows[:count] + rows[count:]
    own_ref[...] = rows[: count // 2].reshape(own_ref.shape)
    other_ref[...] = rows[count // 2 :].reshape(other_ref.shape)


def combine(x, mix):
    out = shape(2, x.shape[1], x.shape[2], dtype=F32)
    return kernel_call(combine_body, (out, out), [IN_VMEM] * 2, 4)(x, mix)


def finish_body(hidden_ref, own_ref, other_ref, out_ref, total):
    core = lax.axis_index(CORES)
    blocks, tile, half = hidden_ref.shape
    total[pl.ds(core * 2, 2)] = own_ref[...]
    total[pl.ds(2 - core * 2, 2)] = other_ref[...]
    for k in range(blocks):
        value = (hidden_ref[k] + total[k]).astype(BF16)
        for q in range(2):
            at = (2 * k + q) * half
            out_ref[:, at : at + half] = value[q * tile // 2 : (q + 1) * tile // 2]


def finish(hidden, own, other):
    blocks, tile, half = hidden.shape
    return kernel_call(
        finish_body, shape(tile // 2, 2 * blocks * half), [IN_VMEM] * 3, 2, [pltpu.VMEM(hidden.shape, F32)]
    )(hidden, own, other)


def on_device(
    queries,
    token_keys,
    token_values,
    stored_keys,
    stored_values,
    kv_len,
    residual,
    out_weight,
    norm_gain,
    expert_ids,
    route_weight,
    w_gate,
    w_up,
    w_down,
):
    chips = lax.axis_size(CHIPS)
    side = math.isqrt(chips)
    outgoing, *pieces = attend(
        queries, token_keys, token_values, kv_len, stored_keys, stored_values, out_weight
    )
    own = [pieces[0]] + [
        lax.ppermute(pieces[d], CHIPS, quad_step(side, d // 2, d % 2)) for d in (1, 2, 3)
    ]
    tokens = lax.all_to_all(outgoing, CHIPS, 0, 0, tiled=True)
    other = [swapped(piece) for piece in own]
    weight = stack(own, other)
    kept, *given_halves = halves(w_gate, w_up, w_down, 0.75)
    gate_moved, down_moved = (swapped(x) for x in given_halves)
    pick, mix = route(expert_ids, route_weight, chips)

    sums = project(tokens, weight)
    came_back = lax.all_to_all(sums, CHIPS, 0, 0, tiled=True)
    hidden, normed, normed_given = settle(came_back, residual, norm_gain[None])
    outgoing = dispatch(normed, swapped(normed_given), pick)
    incoming = lax.all_to_all(outgoing, CHIPS, 0, 0, tiled=True)
    part, sent = gate_up(incoming, kept, w_gate, w_up, gate_moved)
    down_weight = fetch_down(w_down, down_moved, part)
    expert_out = down(part, swapped(sent), down_weight, incoming.shape[1])
    returned = lax.all_to_all(expert_out, CHIPS, 0, 0, tiled=True)
    moe_own, moe_given = combine(returned, mix)
    return finish(hidden, moe_own, swapped(moe_given))


def solution(mesh):
    in_specs = (
        P(("groups", "expert", "replica"), None),
        P(("groups", "expert", "replica"), None),
        P(("groups", "expert", "replica"), None),
        P(("groups", "expert", "replica"), None, None),
        P(("groups", "expert", "replica"), None, None),
        P(("groups", "expert", "replica")),
        P(("groups", "expert", "replica"), None),
        P(("expert", "replica"), None),
        P(),
        P(("groups", "expert"), None),
        P(("groups", "expert"), None),
        P("expert", None, "replica"),
        P("expert", None, "replica"),
        P("expert", "replica", None),
    )
    out_specs = P(("groups", "expert", "replica"), None)
    return jax.shard_map(
        on_device, mesh=mesh, in_specs=in_specs, out_specs=out_specs, check_vma=False
    )
```

```python
import math

import jax
import jax.numpy as jnp
from jax import lax
from jax.experimental import pallas as pl
from jax.experimental.pallas import tpu as pltpu
from jax.sharding import PartitionSpec as P

HEAD_WIDTH = 128
CHIPS, CORES = "expert", "replica"
F32, BF16 = jnp.float32, jnp.bfloat16
IN_VMEM = pl.BlockSpec(memory_space=pltpu.VMEM)
IN_SMEM = pl.BlockSpec(memory_space=pltpu.SMEM)
IN_HBM = pl.BlockSpec(memory_space=pltpu.HBM)


def swapped(x):
    return lax.ppermute(x, CORES, [(0, 1), (1, 0)])


def quad_step(side, dx, dy):
    return [
        (x * side + y, (x ^ dx) * side + (y ^ dy)) for x in range(side) for y in range(side)
    ]


MIB = 1 << 20


def in_hbm(x):
    return pltpu.with_memory_space_constraint(x, pltpu.HBM)


def in_vmem(x):
    return pltpu.with_memory_space_constraint(x, pltpu.VMEM)


def kernel_call(body, outs, in_specs, limit, scratch=()):
    return pl.pallas_call(
        body,
        out_shape=outs,
        in_specs=in_specs,
        out_specs=jax.tree.map(lambda _: IN_VMEM, outs),
        scratch_shapes=list(scratch),
        compiler_params=pltpu.CompilerParams(vmem_limit_bytes=limit * MIB),
    )


def shape(*dims, dtype=BF16):
    return jax.ShapeDtypeStruct(dims, dtype)


def attend_body(
    q_hbm,
    tk_hbm,
    tv_hbm,
    len_hbm,
    keys_hbm,
    values_hbm,
    weight_hbm,
    out_hbm,
    piece0,
    piece1,
    piece2,
    piece3,
    q_ref,
    tk_ref,
    tv_ref,
    len_ref,
    keys,
    values,
    pieces,
    rows,
    mixed,
    scored,
    out_ref,
    sems,
    few,
):
    core = lax.axis_index(CORES)
    seq_count, cache_len, kv_width = keys_hbm.shape
    kv_count = kv_width // HEAD_WIDTH
    head_count = q_hbm.shape[1] // HEAD_WIDTH
    group = head_count // kv_count
    side = group // 2
    small = [
        pltpu.make_async_copy(source, target, few.at[j])
        for j, (source, target) in enumerate(
            ((q_hbm, q_ref), (tk_hbm, tk_ref), (tv_hbm, tv_ref), (len_hbm, len_ref))
        )
    ]
    for copy in small:
        copy.start()
    copies = [
        [pltpu.make_async_copy(source.at[b], target.at[b], sems.at[j, b]) for b in range(seq_count)]
        for j, (source, target) in enumerate(((keys_hbm, keys), (values_hbm, values)))
    ]
    for copy in copies[0] + copies[1]:
        copy.start()
    chip = lax.axis_index(CHIPS)
    place = chip // side % 2 * 2 + chip % 2
    sliced, stored = [], []
    for d, piece in enumerate((piece0, piece1, piece2, piece3)):
        cols = piece.shape[1]
        at = pl.multiple_of((place ^ d) * cols, cols)
        source = weight_hbm.at[:, pl.ds(at, cols)]
        sliced.append(pltpu.make_async_copy(source, pieces.at[d], few.at[len(small) + d]))
        stored.append(pltpu.make_async_copy(pieces.at[d], piece, few.at[len(small) + 4 + d]))
        sliced[-1].start()
    for copy in small:
        copy.wait()
    for h in range(head_count):
        piece = q_ref[:, h * HEAD_WIDTH : (h + 1) * HEAD_WIDTH].astype(F32)
        rows[pl.ds(h, seq_count, stride=head_count), :] = piece
    inv_root = 1.0 / math.sqrt(HEAD_WIDTH)
    positions = lax.broadcasted_iota(jnp.int32, (head_count, cache_len), 1)
    lanes = [slice(g * HEAD_WIDTH, (g + 1) * HEAD_WIDTH) for g in range(kv_count)]
    fresh = []
    for copy in copies[0]:
        copy.wait()
    for b in range(seq_count):
        query = rows[b * head_count : (b + 1) * head_count, :]
        latest = [tk_ref[b : b + 1, lanes[g]].astype(F32) for g in range(kv_count)]
        latest = jnp.concatenate([jnp.broadcast_to(v, (group, HEAD_WIDTH)) for v in latest])
        fresh.append(jnp.sum(query * latest, axis=1, keepdims=True) * inv_root)
        query = query.astype(BF16)
        for g in range(kv_count):
            at = b * head_count + g * group
            scored[at : at + group, :] = lax.dot_general(
                query[g * group : (g + 1) * group],
                keys[b, :, lanes[g]],
                (((1,), (1,)), ((), ())),
                preferred_element_type=F32,
            )
    for copy in copies[1] + sliced:
        copy.wait()
    for copy in stored:
        copy.start()
    probs, fresh_probs = [], []
    for b in range(seq_count):
        scores = scored[b * head_count : (b + 1) * head_count, :]
        scores = jnp.where(positions < len_ref[b], scores * inv_root, -jnp.inf)
        highest = jnp.maximum(jnp.max(scores, axis=1, keepdims=True), fresh[b])
        cached_exp = jnp.exp(scores - highest)
        fresh_exp = jnp.exp(fresh[b] - highest)
        share = 1.0 / (jnp.sum(cached_exp, axis=1, keepdims=True) + fresh_exp)
        probs.append((cached_exp * share).astype(BF16))
        fresh_probs.append((fresh_exp * share).astype(BF16).astype(F32))
    for b in range(seq_count):
        for g in range(kv_count):
            heads = slice(g * group, (g + 1) * group)
            out = jnp.dot(probs[b][heads], values[b, :, lanes[g]], preferred_element_type=F32)
            out = out + fresh_probs[b][heads] * tv_ref[b : b + 1, lanes[g]].astype(F32)
            out = pltpu.roll(out, core * (HEAD_WIDTH // 2), 1)
            for a in range(2):
                start = g * group * seq_count + a * seq_count + b
                mixed[pl.ds(start, side, stride=2 * seq_count), :] = out[a * side : (a + 1) * side]
    tile = 2 * seq_count
    for g in range(kv_count):
        for y in range(side):
            for part, source in enumerate((y, y ^ 1)):
                at = (g * side + source) * tile
                near = mixed[at : at + tile, :]
                far = pltpu.roll(near, seq_count, 0)
                out_ref[2 * g * side + y, :, lanes[part]] = near.astype(BF16)
                out_ref[(2 * g + 1) * side + y, :, lanes[part]] = far.astype(BF16)
        sent = pl.ds(2 * g * side, 2 * side)
        stored.append(
            pltpu.make_async_copy(out_ref.at[sent], out_hbm.at[sent], few.at[len(small) + 8 + g])
        )
        stored[-1].start()
    for copy in stored:
        copy.wait()


def attend(queries, token_keys, token_values, kv_len, stored_keys, stored_values, out_weight):
    seq_count, feature_total = queries.shape
    heads = feature_total // HEAD_WIDTH
    rows, cols = out_weight.shape
    return pl.pallas_call(
        attend_body,
        name="attend",
        out_shape=[pltpu.HBM((heads, 2 * seq_count, 2 * HEAD_WIDTH), BF16)]
        + [pltpu.HBM((rows, cols // 4), BF16)] * 4,
        in_specs=[IN_HBM] * 7,
        out_specs=[IN_HBM] * 5,
        scratch_shapes=[
            pltpu.VMEM(queries.shape, BF16),
            pltpu.VMEM(token_keys.shape, BF16),
            pltpu.VMEM(token_values.shape, BF16),
            pltpu.SMEM(kv_len.shape, jnp.int32),
            pltpu.VMEM(stored_keys.shape, BF16),
            pltpu.VMEM(stored_values.shape, BF16),
            pltpu.VMEM((4, rows, cols // 4), BF16),
            pltpu.VMEM((seq_count * heads, HEAD_WIDTH), F32),
            pltpu.VMEM((seq_count * heads, HEAD_WIDTH), F32),
            pltpu.VMEM((seq_count * heads, stored_keys.shape[1]), F32),
            pltpu.VMEM((heads, 2 * seq_count, 2 * HEAD_WIDTH), BF16),
            pltpu.SemaphoreType.DMA((2, seq_count)),
            pltpu.SemaphoreType.DMA((16,)),
        ],
        compiler_params=pltpu.CompilerParams(vmem_limit_bytes=8 * MIB),
    )(
        *map(
            in_hbm,
            (queries, token_keys, token_values, kv_len, stored_keys, stored_values, out_weight),
        )
    )


def copy_all(pairs, sems):
    copies = [pltpu.make_async_copy(*pair, sems.at[j]) for j, pair in enumerate(pairs)]
    for copy in copies:
        copy.start()
    for copy in copies:
        copy.wait()


def stack_body(*refs):
    own, other, out_ref, sems = refs[:4], refs[4:8], refs[8], refs[9]
    rows = own[0].shape[0]
    pairs = []
    for d in range(4):
        for half, source in enumerate((own[d], other[d])):
            at = (d % 2 * 2 + half) * rows
            pairs.append((source, out_ref.at[d // 2, at : at + rows]))
    copy_all(pairs, sems)


def stack(own, other):
    rows, cols = own[0].shape
    return pl.pallas_call(
        stack_body,
        name="stack",
        out_shape=pltpu.VMEM((2, 4 * rows, cols), BF16),
        in_specs=[IN_HBM] * 8,
        out_specs=IN_VMEM,
        scratch_shapes=[pltpu.SemaphoreType.DMA((8,))],
        compiler_params=pltpu.CompilerParams(vmem_limit_bytes=2 * MIB),
    )(*map(in_hbm, own), *map(in_hbm, other))


def halves_body(gate_hbm, up_hbm, down_hbm, kept_ref, *refs):
    outs, (tall, wide, sems) = refs[:2], refs[2:]
    core = lax.axis_index(CORES)
    count = kept_ref.shape[0]
    half, both = tall.shape
    units = both // 2
    given = pl.ds(pl.multiple_of((1 - core) * half, half), half)
    kept = pl.ds(pl.multiple_of(core * half, half), count)
    left, right = slice(0, units), slice(units, both)
    pairs = (
        (gate_hbm.at[0, given, :], tall.at[:, left]),
        (up_hbm.at[0, given, :], tall.at[:, right]),
        (down_hbm.at[0, :, given], wide),
        (gate_hbm.at[0, kept, :], kept_ref.at[:, left]),
        (up_hbm.at[0, kept, :], kept_ref.at[:, right]),
        (tall, outs[0]),
        (wide, outs[1]),
    )
    copies = [pltpu.make_async_copy(*pair, sems.at[j]) for j, pair in enumerate(pairs)]
    for copy in copies[:5]:
        copy.start()
    for copy in copies[:2]:
        copy.wait()
    copies[5].start()
    copies[2].wait()
    copies[6].start()
    for copy in copies[3:]:
        copy.wait()


def halves(w_gate, w_up, w_down, kept_share):
    _, width, units = w_gate.shape
    tall, wide = (width // 2, 2 * units), (units, width // 2)
    return pl.pallas_call(
        halves_body,
        name="halves",
        out_shape=[
            pltpu.VMEM((int(width // 2 * kept_share), 2 * units), BF16),
            pltpu.HBM(tall, BF16),
            pltpu.HBM(wide, BF16),
        ],
        in_specs=[IN_HBM] * 3,
        out_specs=[IN_VMEM] + [IN_HBM] * 2,
        scratch_shapes=[
            pltpu.VMEM(tall, BF16),
            pltpu.VMEM(wide, BF16),
            pltpu.SemaphoreType.DMA((7,)),
        ],
        compiler_params=pltpu.CompilerParams(vmem_limit_bytes=6 * MIB),
    )(*map(in_hbm, (w_gate, w_up, w_down)))


def project_body(x_ref, weight_ref, out_hbm, held, sems):
    chips, tile, width = x_ref.shape
    cols = weight_ref.shape[2]
    half = cols // 2
    step = 16
    low = lax.broadcasted_iota(jnp.int32, (step, tile, half), 1) < tile // 2
    copies = []
    for j, at in enumerate(range(0, chips, step)):
        rows = slice(at, at + step)
        x = x_ref[rows].reshape(step * tile, width)
        near, far = (
            jnp.dot(x, weight_ref[j], preferred_element_type=F32).reshape(step, tile, cols)
            for j in range(2)
        )
        kept = jnp.where(low, near[:, :, :half], far[:, :, half:])
        moved = jnp.where(low, near[:, :, half:], far[:, :, :half])
        moved = pltpu.roll(moved, tile // 2, 1)
        held[rows] = (kept + moved).astype(BF16)
        copies.append(pltpu.make_async_copy(held.at[rows], out_hbm.at[rows], sems.at[j]))
        copies[-1].start()
    for copy in copies:
        copy.wait()


def sending_call(body, dims, in_specs, limit, chunks):
    return pl.pallas_call(
        body,
        out_shape=pltpu.HBM(dims, BF16),
        in_specs=in_specs,
        out_specs=IN_HBM,
        scratch_shapes=[pltpu.VMEM(dims, BF16), pltpu.SemaphoreType.DMA((chunks,))],
        compiler_params=pltpu.CompilerParams(vmem_limit_bytes=limit * MIB),
    )


def project(x, weight):
    dims = x.shape[0], x.shape[1], weight.shape[2] // 2
    return sending_call(project_body, dims, [IN_VMEM] * 2, 12, x.shape[0] // 16)(
        x, in_vmem(weight)
    )


def project_body(x_ref, weight_ref, out_ref):
    chips, tile, width = x_ref.shape
    cols = weight_ref.shape[2]
    half = cols // 2
    step = 16
    low = lax.broadcasted_iota(jnp.int32, (step, tile, half), 1) < tile // 2
    for at in range(0, chips, step):
        x = x_ref[at : at + step].reshape(step * tile, width)
        near, far = (
            jnp.dot(x, weight_ref[j], preferred_element_type=F32).reshape(step, tile, cols)
            for j in range(2)
        )
        kept = jnp.where(low, near[:, :, :half], far[:, :, half:])
        moved = jnp.where(low, near[:, :, half:], far[:, :, :half])
        moved = pltpu.roll(moved, tile // 2, 1)
        out_ref[at : at + step] = (kept + moved).astype(BF16)


def project(x, weight):
    cols = weight.shape[2]
    return kernel_call(
        project_body, pltpu.HBM((x.shape[0], x.shape[1], cols // 2), BF16), [IN_VMEM] * 2, 12
    )(x, in_vmem(weight))


def settle_body(x_ref, residual_ref, gain_ref, hidden_ref, kept_ref, given_ref, normed):
    core = lax.axis_index(CORES)
    chips, tile, half = x_ref.shape
    side = math.isqrt(chips)
    blocks = 4
    seq_count = tile // 2
    width = residual_ref.shape[1]

    def rows_of(ref, k):
        low, high = (ref[:, (2 * k + q) * half : (2 * k + q + 1) * half].astype(F32) for q in (0, 1))
        low, high = (jnp.broadcast_to(v, (seq_count, half)) for v in (low, high))
        return jnp.concatenate([low, high])

    square = jnp.zeros((tile, 1), F32)
    for k in range(blocks):
        total = rows_of(residual_ref, k)
        for x in range(k // 2, side, 2):
            for y in range(k % 2, side, 2):
                total = total + x_ref[x * side + y].astype(F32)
        hidden_ref[k] = total
        square = square + jnp.sum(total * total, axis=1, keepdims=True)
    square = jnp.broadcast_to(square, (tile, HEAD_WIDTH))
    square = square + pltpu.roll(square, seq_count, 0)
    scale = lax.rsqrt(square[:, :1] / width + 1e-06)
    for k in range(blocks):
        normed[k] = (hidden_ref[k] * scale * rows_of(gain_ref, k)).astype(BF16)
    kept_ref[...] = normed[pl.ds(core * 2, 2)]
    given_ref[...] = normed[pl.ds(2 - core * 2, 2)]


def settle(x, residual, gain):
    tile, half = x.shape[1:]
    return kernel_call(
        settle_body,
        (shape(4, tile, half, dtype=F32), shape(2, tile, half), shape(2, tile, half)),
        [IN_VMEM] * 3,
        6,
        [pltpu.VMEM((4, tile, half), BF16)],
    )(x, residual, gain)


def route_body(ids_ref, weight_ref, pick_ref, mix_ref):
    core = lax.axis_index(CORES)
    tokens, topk = ids_ref.shape
    seq_count = tokens // 2
    lanes = pick_ref.shape[1]
    lane = lax.broadcasted_iota(jnp.int32, (tokens, lanes), 1)
    row = lax.broadcasted_iota(jnp.int32, (tokens, lanes), 0)
    weight = weight_ref[...]
    mixing = weight / jnp.sum(weight, axis=1, keepdims=True)
    ids = ids_ref[...]
    hit = jnp.zeros((tokens, lanes), F32)
    share = jnp.zeros((tokens, lanes), F32)
    for k in range(topk):
        same = ids[:, k : k + 1] == lane // 8
        hit = jnp.where(same, 1.0, hit)
        share = jnp.where(same, mixing[:, k : k + 1], share)
    rank = jnp.zeros((tokens, lanes), F32)
    for t in range(tokens - 1):
        rank = rank + jnp.where(row > t, jnp.broadcast_to(hit[t : t + 1], (tokens, lanes)), 0.0)
    taken = jnp.where(rank == (lane % 2).astype(F32), hit, 0.0)
    share = share * taken
    own_low = (row < seq_count) == (core == 0)
    quarter = lane // 2 % 4
    for src in range(2):
        low = own_low if src == 0 else jnp.logical_not(own_low)
        chosen = jnp.where(low, taken, pltpu.roll(taken, seq_count, 0))
        shares = jnp.where(low, share, pltpu.roll(share, seq_count, 0))
        for kk in range(2):
            at = (src * 2 + kk) * tokens
            mine = quarter == kk * 2 + row // seq_count
            pick_ref[at : at + tokens, :] = jnp.where(mine, chosen, 0.0).astype(BF16)
            value = jnp.where(mine, shares, 0.0)
            coarse = value.astype(BF16)
            mix_ref[at : at + tokens, :] = coarse
            mix_ref[4 * tokens + at : 5 * tokens + at, :] = (value - coarse.astype(F32)).astype(BF16)


def route(expert_ids, route_weight, chips):
    tokens = expert_ids.shape[0]
    return kernel_call(
        route_body, (shape(4 * tokens, 8 * chips), shape(8 * tokens, 8 * chips)), [IN_VMEM] * 2, 4
    )(expert_ids, route_weight)


def dispatch_body(kept_ref, other_ref, pick_ref, out_hbm, held, sems):
    pieces = [r[...].reshape(-1, r.shape[2]) for r in (kept_ref, other_ref)]
    tokens = jnp.concatenate(pieces)
    chips, tile, half = held.shape
    step = chips // 2
    copies = []
    for j in range(2):
        rows = lax.dot_general(
            pick_ref[:, j * step * tile : (j + 1) * step * tile],
            tokens,
            (((0,), (0,)), ((), ())),
            preferred_element_type=F32,
        )
        sent = slice(j * step, (j + 1) * step)
        held[sent] = rows.astype(BF16).reshape(step, tile, half)
        copies.append(pltpu.make_async_copy(held.at[sent], out_hbm.at[sent], sems.at[j]))
        copies[-1].start()
    for copy in copies:
        copy.wait()


def dispatch(kept, other, pick):
    tile, half = kept.shape[1:]
    dims = pick.shape[1] // tile, tile, half
    return sending_call(dispatch_body, dims, [IN_VMEM] * 3, 6, 2)(kept, other, pick)


def slot_order(size, back=False):
    sorted_row = lax.broadcasted_iota(jnp.int32, (size, size), 1 if back else 0)
    row = lax.broadcasted_iota(jnp.int32, (size, size), 0 if back else 1)
    slot = sorted_row % (size // 4)
    quarter = sorted_row // (size // 4)
    return jnp.where(row == slot // 2 * 8 + quarter * 2 + slot % 2, 1.0, 0.0).astype(BF16)


def gate_body(x_ref, kept_ref, gate_hbm, up_hbm, moved_hbm, part_ref, sent_ref, rest, moved, sems):
    core = lax.axis_index(CORES)
    chips, tile, part = x_ref.shape
    half, both = moved.shape
    units = both // 2
    count = kept_ref.shape[0]
    late = pl.ds(pl.multiple_of(core * half + count, part), half - count)
    pairs = [(gate_hbm.at[0, late, :], rest.at[:, :units]), (up_hbm.at[0, late, :], rest.at[:, units:])]
    step = half // 2
    for j in range(2):
        rows = slice(j * step, (j + 1) * step)
        pairs.append((moved_hbm.at[rows], moved.at[rows]))
    copies = [pltpu.make_async_copy(*pair, sems.at[j]) for j, pair in enumerate(pairs)]
    for copy in copies:
        copy.start()
    size = 256
    groups = chips * tile // size
    order = slot_order(size)
    slots = size // 4
    sorted_rows = []
    for g in range(groups):
        rows = x_ref[g * size // tile : (g + 1) * size // tile].reshape(size, part)
        sorted_rows.append(jnp.dot(order, rows, preferred_element_type=F32).astype(BF16))
    quarters = [
        jnp.concatenate([r[p * slots : (p + 1) * slots] for r in sorted_rows]) for p in range(4)
    ]
    x = jnp.concatenate(quarters, axis=1)
    own = jnp.dot(x[:, :count], kept_ref[...], preferred_element_type=F32)
    for copy in copies[:2]:
        copy.wait()
    own = own + jnp.dot(x[:, count:], rest[...], preferred_element_type=F32)
    part_ref[:, :both] = own
    sent_ref[:, both:] = own.astype(BF16)
    copies[2].wait()
    other = jnp.dot(x[:, :step], moved[:step], preferred_element_type=F32)
    copies[3].wait()
    other = other + jnp.dot(x[:, step:], moved[step:], preferred_element_type=F32)
    part_ref[:, both:] = other
    sent_ref[:, :both] = other.astype(BF16)


def gate_up(x, kept, w_gate, w_up, moved):
    chips, tile, _ = x.shape
    half, both = moved.shape
    dims = chips * tile // 4, 2 * both
    return pl.pallas_call(
        gate_body,
        name="gate_up",
        out_shape=[pltpu.VMEM(dims, F32), pltpu.VMEM(dims, BF16)],
        in_specs=[IN_VMEM] * 2 + [IN_HBM] * 3,
        out_specs=[IN_VMEM] * 2,
        scratch_shapes=[
            pltpu.VMEM((half - kept.shape[0], both), BF16),
            pltpu.VMEM((half, both), BF16),
            pltpu.SemaphoreType.DMA((4,)),
        ],
        compiler_params=pltpu.CompilerParams(vmem_limit_bytes=14 * MIB),
    )(x, in_vmem(kept), *map(in_hbm, (w_gate, w_up, moved)))


def fetch_body(down_hbm, moved_hbm, after_ref, out_ref, sems):
    del after_ref
    core = lax.axis_index(CORES)
    units, half = moved_hbm.shape
    kept = pl.ds(pl.multiple_of(core * half, half), half)
    copies = [
        pltpu.make_async_copy(down_hbm.at[0, :, kept], out_ref.at[:units], sems.at[0]),
        pltpu.make_async_copy(moved_hbm, out_ref.at[units:], sems.at[1]),
    ]
    for copy in copies:
        copy.start()
    for copy in copies:
        copy.wait()


def fetch_down(w_down, moved, after):
    units, half = moved.shape
    return pl.pallas_call(
        fetch_body,
        name="fetch_down",
        out_shape=pltpu.VMEM((2 * units, half), BF16),
        in_specs=[IN_HBM] * 3,
        out_specs=IN_VMEM,
        scratch_shapes=[pltpu.SemaphoreType.DMA((2,))],
        compiler_params=pltpu.CompilerParams(vmem_limit_bytes=MIB),
    )(in_hbm(w_down), in_hbm(moved), after)


def down_body(part_ref, arrived_ref, down_ref, out_hbm, held, sems):
    chips, tile, part = held.shape
    size = 256
    groups = chips * tile // size
    order = slot_order(size, back=True)
    slots = size // 4
    units = down_ref.shape[0] // 2

    def act(at):
        gate, up = (
            part_ref[:, j : j + units] + arrived_ref[:, j : j + units].astype(F32)
            for j in (at, at + units)
        )
        return (gate / (1.0 + jnp.exp(-gate)) * up).astype(BF16)

    hidden = jnp.concatenate([act(0), act(2 * units)], axis=1)
    quarters = []
    for p in range(4):
        lanes = slice(p * part, (p + 1) * part)
        value = jnp.dot(hidden, down_ref[:, lanes], preferred_element_type=F32)
        quarters.append(value.astype(BF16))
    copies = []
    for g in range(groups):
        rows = jnp.concatenate([v[g * slots : (g + 1) * slots] for v in quarters])
        rows = jnp.dot(order, rows, preferred_element_type=F32).astype(BF16)
        sent = slice(g * size // tile, (g + 1) * size // tile)
        held[sent] = rows.reshape(size // tile, tile, part)
        copies.append(pltpu.make_async_copy(held.at[sent], out_hbm.at[sent], sems.at[g]))
        copies[-1].start()
    for copy in copies:
        copy.wait()


def down(part, arrived, weight, tile):
    dims = part.shape[0] * 4 // tile, tile, weight.shape[1] // 4
    return sending_call(down_body, dims, [IN_VMEM] * 3, 8, 2)(
        part, arrived, in_vmem(weight)
    )


def combine_body(x_ref, mix_ref, own_ref, other_ref):
    x = x_ref[...].reshape(-1, x_ref.shape[2])
    rows = jnp.dot(mix_ref[...], x, preferred_element_type=F32)
    count = rows.shape[0] // 2
    rows = rows[:count] + rows[count:]
    own_ref[...] = rows[: count // 2].reshape(own_ref.shape)
    other_ref[...] = rows[count // 2 :].reshape(other_ref.shape)


def combine(x, mix):
    out = shape(2, x.shape[1], x.shape[2], dtype=F32)
    return kernel_call(combine_body, (out, out), [IN_VMEM] * 2, 4)(x, mix)


def finish_body(hidden_ref, own_ref, other_ref, out_ref, total):
    core = lax.axis_index(CORES)
    blocks, tile, half = hidden_ref.shape
    total[pl.ds(core * 2, 2)] = own_ref[...]
    total[pl.ds(2 - core * 2, 2)] = other_ref[...]
    for k in range(blocks):
        value = (hidden_ref[k] + total[k]).astype(BF16)
        for q in range(2):
            at = (2 * k + q) * half
            out_ref[:, at : at + half] = value[q * tile // 2 : (q + 1) * tile // 2]


def finish(hidden, own, other):
    blocks, tile, half = hidden.shape
    return kernel_call(
        finish_body, shape(tile // 2, 2 * blocks * half), [IN_VMEM] * 3, 2, [pltpu.VMEM(hidden.shape, F32)]
    )(hidden, own, other)


def on_device(
    queries,
    token_keys,
    token_values,
    stored_keys,
    stored_values,
    kv_len,
    residual,
    out_weight,
    norm_gain,
    expert_ids,
    route_weight,
    w_gate,
    w_up,
    w_down,
):
    chips = lax.axis_size(CHIPS)
    side = math.isqrt(chips)
    outgoing, *pieces = attend(
        queries, token_keys, token_values, kv_len, stored_keys, stored_values, out_weight
    )
    own = [pieces[0]]
    for d in (1, 2, 3):
        own.append(lax.ppermute(pieces[d], CHIPS, quad_step(side, d // 2, d % 2)))
    tokens = lax.all_to_all(outgoing, CHIPS, 0, 0, tiled=True)
    other = [swapped(piece) for piece in own]
    weight = stack(own, other)
    kept, *given_halves = halves(w_gate, w_up, w_down, 0.75)
    gate_moved, down_moved = (swapped(x) for x in given_halves)
    pick, mix = route(expert_ids, route_weight, chips)

    sums = project(tokens, weight)
    came_back = lax.all_to_all(sums, CHIPS, 0, 0, tiled=True)
    hidden, normed, normed_given = settle(came_back, residual, norm_gain[None])
    outgoing = dispatch(normed, swapped(normed_given), pick)
    incoming = lax.all_to_all(outgoing, CHIPS, 0, 0, tiled=True)
    part, sent = gate_up(incoming, kept, w_gate, w_up, gate_moved)
    down_weight = fetch_down(w_down, down_moved, part)
    expert_out = down(part, swapped(sent), down_weight, incoming.shape[1])
    returned = lax.all_to_all(expert_out, CHIPS, 0, 0, tiled=True)
    moe_own, moe_given = combine(returned, mix)
    return finish(hidden, moe_own, swapped(moe_given))


def solution(mesh):
    in_specs = (
        P(("groups", "expert", "replica"), None),
        P(("groups", "expert", "replica"), None),
        P(("groups", "expert", "replica"), None),
        P(("groups", "expert", "replica"), None, None),
        P(("groups", "expert", "replica"), None, None),
        P(("groups", "expert", "replica")),
        P(("groups", "expert", "replica"), None),
        P(("expert", "replica"), None),
        P(),
        P(("groups", "expert"), None),
        P(("groups", "expert"), None),
        P("expert", None, "replica"),
        P("expert", None, "replica"),
        P("expert", "replica", None),
    )
    out_specs = P(("groups", "expert", "replica"), None)
    return jax.shard_map(
        on_device, mesh=mesh, in_specs=in_specs, out_specs=out_specs, check_vma=False
    )
```

```python
import math

import jax
import jax.numpy as jnp
from jax import lax
from jax.experimental import pallas as pl
from jax.experimental.pallas import tpu as pltpu
from jax.sharding import PartitionSpec as P

HEAD_WIDTH = 128
CHIPS, CORES = "expert", "replica"
F32, BF16 = jnp.float32, jnp.bfloat16
IN_VMEM = pl.BlockSpec(memory_space=pltpu.VMEM)
IN_SMEM = pl.BlockSpec(memory_space=pltpu.SMEM)
IN_HBM = pl.BlockSpec(memory_space=pltpu.HBM)


def swapped(x):
    return lax.ppermute(x, CORES, [(0, 1), (1, 0)])


def quad_step(side, dx, dy):
    return [
        (x * side + y, (x ^ dx) * side + (y ^ dy)) for x in range(side) for y in range(side)
    ]


MIB = 1 << 20


def in_hbm(x):
    return pltpu.with_memory_space_constraint(x, pltpu.HBM)


def in_vmem(x):
    return pltpu.with_memory_space_constraint(x, pltpu.VMEM)


def kernel_call(body, outs, in_specs, limit, scratch=()):
    return pl.pallas_call(
        body,
        out_shape=outs,
        in_specs=in_specs,
        out_specs=jax.tree.map(lambda _: IN_VMEM, outs),
        scratch_shapes=list(scratch),
        compiler_params=pltpu.CompilerParams(vmem_limit_bytes=limit * MIB),
    )


def shape(*dims, dtype=BF16):
    return jax.ShapeDtypeStruct(dims, dtype)


def attend_body(
    q_hbm,
    tk_hbm,
    tv_hbm,
    len_hbm,
    keys_hbm,
    values_hbm,
    weight_hbm,
    out_hbm,
    piece_own,
    piece_near,
    piece_diagonal,
    q_ref,
    tk_ref,
    tv_ref,
    len_ref,
    keys,
    values,
    pieces,
    rows,
    mixed,
    scored,
    out_ref,
    sems,
    few,
):
    core = lax.axis_index(CORES)
    seq_count, cache_len, kv_width = keys_hbm.shape
    kv_count = kv_width // HEAD_WIDTH
    head_count = q_hbm.shape[1] // HEAD_WIDTH
    group = head_count // kv_count
    side = group // 2
    small = [
        pltpu.make_async_copy(source, target, few.at[j])
        for j, (source, target) in enumerate(
            ((q_hbm, q_ref), (tk_hbm, tk_ref), (tv_hbm, tv_ref), (len_hbm, len_ref))
        )
    ]
    for copy in small:
        copy.start()
    copies = [
        [pltpu.make_async_copy(source.at[b], target.at[b], sems.at[j, b]) for b in range(seq_count)]
        for j, (source, target) in enumerate(((keys_hbm, keys), (values_hbm, values)))
    ]
    for copy in copies[0] + copies[1]:
        copy.start()
    chip = lax.axis_index(CHIPS)
    place = chip // side % 2 * 2 + chip % 2
    sliced, stored = [], []
    for j, (d, piece) in enumerate(
        ((0, piece_own), (1 + core, piece_near), (3, piece_diagonal))
    ):
        cols = piece.shape[1]
        at = pl.multiple_of((place ^ d) * cols, cols)
        source = weight_hbm.at[:, pl.ds(at, cols)]
        sliced.append(pltpu.make_async_copy(source, pieces.at[j], few.at[len(small) + j]))
        stored.append(pltpu.make_async_copy(pieces.at[j], piece, few.at[len(small) + 3 + j]))
        sliced[-1].start()
    for copy in small:
        copy.wait()
    for h in range(head_count):
        piece = q_ref[:, h * HEAD_WIDTH : (h + 1) * HEAD_WIDTH].astype(F32)
        rows[pl.ds(h, seq_count, stride=head_count), :] = piece
    inv_root = 1.0 / math.sqrt(HEAD_WIDTH)
    positions = lax.broadcasted_iota(jnp.int32, (head_count, cache_len), 1)
    lanes = [slice(g * HEAD_WIDTH, (g + 1) * HEAD_WIDTH) for g in range(kv_count)]
    fresh = []
    for copy in copies[0]:
        copy.wait()
    for b in range(seq_count):
        query = rows[b * head_count : (b + 1) * head_count, :]
        latest = [tk_ref[b : b + 1, lanes[g]].astype(F32) for g in range(kv_count)]
        latest = jnp.concatenate([jnp.broadcast_to(v, (group, HEAD_WIDTH)) for v in latest])
        fresh.append(jnp.sum(query * latest, axis=1, keepdims=True) * inv_root)
        query = query.astype(BF16)
        for g in range(kv_count):
            at = b * head_count + g * group
            scored[at : at + group, :] = lax.dot_general(
                query[g * group : (g + 1) * group],
                keys[b, :, lanes[g]],
                (((1,), (1,)), ((), ())),
                preferred_element_type=F32,
            )
    for copy in copies[1] + sliced:
        copy.wait()
    for copy in stored:
        copy.start()
    probs, fresh_probs = [], []
    for b in range(seq_count):
        scores = scored[b * head_count : (b + 1) * head_count, :]
        scores = jnp.where(positions < len_ref[b], scores * inv_root, -jnp.inf)
        highest = jnp.maximum(jnp.max(scores, axis=1, keepdims=True), fresh[b])
        cached_exp = jnp.exp(scores - highest)
        fresh_exp = jnp.exp(fresh[b] - highest)
        share = 1.0 / (jnp.sum(cached_exp, axis=1, keepdims=True) + fresh_exp)
        probs.append((cached_exp * share).astype(BF16))
        fresh_probs.append((fresh_exp * share).astype(BF16).astype(F32))
    for b in range(seq_count):
        for g in range(kv_count):
            heads = slice(g * group, (g + 1) * group)
            out = jnp.dot(probs[b][heads], values[b, :, lanes[g]], preferred_element_type=F32)
            out = out + fresh_probs[b][heads] * tv_ref[b : b + 1, lanes[g]].astype(F32)
            out = pltpu.roll(out, core * (HEAD_WIDTH // 2), 1)
            for a in range(2):
                start = g * group * seq_count + a * seq_count + b
                mixed[pl.ds(start, side, stride=2 * seq_count), :] = out[a * side : (a + 1) * side]
    tile = 2 * seq_count
    for g in range(kv_count):
        for y in range(side):
            for part, source in enumerate((y, y ^ 1)):
                at = (g * side + source) * tile
                near = mixed[at : at + tile, :]
                far = pltpu.roll(near, seq_count, 0)
                out_ref[2 * g * side + y, :, lanes[part]] = near.astype(BF16)
                out_ref[(2 * g + 1) * side + y, :, lanes[part]] = far.astype(BF16)
        sent = pl.ds(2 * g * side, 2 * side)
        stored.append(
            pltpu.make_async_copy(out_ref.at[sent], out_hbm.at[sent], few.at[len(small) + 6 + g])
        )
        stored[-1].start()
    for copy in stored:
        copy.wait()


def attend(queries, token_keys, token_values, kv_len, stored_keys, stored_values, out_weight):
    seq_count, feature_total = queries.shape
    heads = feature_total // HEAD_WIDTH
    rows, cols = out_weight.shape
    return pl.pallas_call(
        attend_body,
        name="attend",
        out_shape=[pltpu.HBM((heads, 2 * seq_count, 2 * HEAD_WIDTH), BF16)]
        + [pltpu.HBM((rows, cols // 4), BF16)] * 3,
        in_specs=[IN_HBM] * 7,
        out_specs=[IN_HBM] * 4,
        scratch_shapes=[
            pltpu.VMEM(queries.shape, BF16),
            pltpu.VMEM(token_keys.shape, BF16),
            pltpu.VMEM(token_values.shape, BF16),
            pltpu.SMEM(kv_len.shape, jnp.int32),
            pltpu.VMEM(stored_keys.shape, BF16),
            pltpu.VMEM(stored_values.shape, BF16),
            pltpu.VMEM((3, rows, cols // 4), BF16),
            pltpu.VMEM((seq_count * heads, HEAD_WIDTH), F32),
            pltpu.VMEM((seq_count * heads, HEAD_WIDTH), F32),
            pltpu.VMEM((seq_count * heads, stored_keys.shape[1]), F32),
            pltpu.VMEM((heads, 2 * seq_count, 2 * HEAD_WIDTH), BF16),
            pltpu.SemaphoreType.DMA((2, seq_count)),
            pltpu.SemaphoreType.DMA((14,)),
        ],
        compiler_params=pltpu.CompilerParams(vmem_limit_bytes=8 * MIB),
    )(
        *map(
            in_hbm,
            (queries, token_keys, token_values, kv_len, stored_keys, stored_values, out_weight),
        )
    )


def copy_all(pairs, sems):
    copies = [pltpu.make_async_copy(*pair, sems.at[j]) for j, pair in enumerate(pairs)]
    for copy in copies:
        copy.start()
    for copy in copies:
        copy.wait()


def stack_body(own, own_raw, near, near_raw, far, far_raw, diagonal, diagonal_far, out_ref, sems):
    core = lax.axis_index(CORES)
    chip = lax.axis_index(CHIPS)
    rows, cols = own.shape
    side = math.isqrt(lax.axis_size(CHIPS))
    place = chip // side % 2 * 2 + chip % 2
    block = pl.ds(pl.multiple_of(place * cols, cols), cols)
    pairs = []
    for d, sources in (
        (0, (own, own_raw.at[:, block])),
        (1 + core, (near, near_raw.at[:, block])),
        (2 - core, (far_raw.at[:, block], far)),
        (3, (diagonal, diagonal_far)),
    ):
        for half, source in enumerate(sources):
            at = pl.multiple_of((2 * d + half) * rows, rows)
            pairs.append((source, out_ref.at[pl.ds(at, rows)]))
    copy_all(pairs, sems)


def stack(*pieces):
    rows, cols = pieces[0].shape
    return pl.pallas_call(
        stack_body,
        name="stack",
        out_shape=pltpu.VMEM((8 * rows, cols), BF16),
        in_specs=[IN_HBM] * 8,
        out_specs=IN_VMEM,
        scratch_shapes=[pltpu.SemaphoreType.DMA((8,))],
        compiler_params=pltpu.CompilerParams(vmem_limit_bytes=2 * MIB),
    )(*map(in_hbm, pieces))


def halves_body(gate_hbm, up_hbm, down_hbm, kept_ref, *refs):
    outs, (tall, wide, sems) = refs[:2], refs[2:]
    core = lax.axis_index(CORES)
    count = kept_ref.shape[0]
    half, both = tall.shape
    units = both // 2
    given = pl.ds(pl.multiple_of((1 - core) * half, half), half)
    kept = pl.ds(pl.multiple_of(core * half, half), count)
    left, right = slice(0, units), slice(units, both)
    pairs = (
        (gate_hbm.at[0, given, :], tall.at[:, left]),
        (up_hbm.at[0, given, :], tall.at[:, right]),
        (down_hbm.at[0, :, given], wide),
        (gate_hbm.at[0, kept, :], kept_ref.at[:, left]),
        (up_hbm.at[0, kept, :], kept_ref.at[:, right]),
        (tall, outs[0]),
        (wide, outs[1]),
    )
    copies = [pltpu.make_async_copy(*pair, sems.at[j]) for j, pair in enumerate(pairs)]
    for copy in copies[:5]:
        copy.start()
    for copy in copies[:2]:
        copy.wait()
    copies[5].start()
    copies[2].wait()
    copies[6].start()
    for copy in copies[3:]:
        copy.wait()


def halves(w_gate, w_up, w_down, kept_share):
    _, width, units = w_gate.shape
    tall, wide = (width // 2, 2 * units), (units, width // 2)
    return pl.pallas_call(
        halves_body,
        name="halves",
        out_shape=[
            pltpu.VMEM((int(width // 2 * kept_share), 2 * units), BF16),
            pltpu.HBM(tall, BF16),
            pltpu.HBM(wide, BF16),
        ],
        in_specs=[IN_HBM] * 3,
        out_specs=[IN_VMEM] + [IN_HBM] * 2,
        scratch_shapes=[
            pltpu.VMEM(tall, BF16),
            pltpu.VMEM(wide, BF16),
            pltpu.SemaphoreType.DMA((7,)),
        ],
        compiler_params=pltpu.CompilerParams(vmem_limit_bytes=6 * MIB),
    )(*map(in_hbm, (w_gate, w_up, w_down)))


def project_body(x_ref, weight_ref, out_hbm, held, sems):
    chips, tile, width = x_ref.shape
    cols = weight_ref.shape[1]
    half = cols // 2
    step = chips // 2

    def paired(first, second):
        low = lax.broadcasted_iota(jnp.int32, first.shape, 1) < tile // 2
        return (
            jnp.where(low, first, pltpu.roll(second, tile // 2, 1)),
            jnp.where(low, pltpu.roll(first, tile // 2, 1), second),
        )

    copies = []
    for j in range(2):
        sent = slice(j * step, (j + 1) * step)
        x = x_ref[sent].astype(F32).reshape(step // 2, 2, tile, width)
        x = jnp.concatenate(paired(x[:, 0], x[:, 1]), axis=2)
        x = x.reshape(step // 2 * tile, 2 * width).astype(BF16)
        sums = jnp.dot(x, weight_ref[...], preferred_element_type=F32)
        sums = sums.reshape(step // 2, tile, cols)
        sums = jnp.stack(paired(sums[:, :, :half], sums[:, :, half:]), axis=1)
        held[sent] = sums.reshape(step, tile, half).astype(BF16)
        copies.append(pltpu.make_async_copy(held.at[sent], out_hbm.at[sent], sems.at[j]))
        copies[-1].start()
    for copy in copies:
        copy.wait()


def sending_call(body, dims, in_specs, limit, chunks):
    return pl.pallas_call(
        body,
        out_shape=pltpu.HBM(dims, BF16),
        in_specs=in_specs,
        out_specs=IN_HBM,
        scratch_shapes=[pltpu.VMEM(dims, BF16), pltpu.SemaphoreType.DMA((chunks,))],
        compiler_params=pltpu.CompilerParams(vmem_limit_bytes=limit * MIB),
    )


def project(x, weight):
    dims = x.shape[0], x.shape[1], weight.shape[1] // 2
    return sending_call(project_body, dims, [IN_VMEM] * 2, 12, 2)(
        x, in_vmem(weight)
    )


def settle_body(x_ref, residual_ref, gain_ref, hidden_ref, kept_ref, given_ref, normed):
    core = lax.axis_index(CORES)
    chips, tile, half = x_ref.shape
    side = math.isqrt(chips)
    blocks = 4
    seq_count = tile // 2
    width = residual_ref.shape[1]

    def rows_of(ref, k):
        low, high = (ref[:, (2 * k + q) * half : (2 * k + q + 1) * half].astype(F32) for q in (0, 1))
        low, high = (jnp.broadcast_to(v, (seq_count, half)) for v in (low, high))
        return jnp.concatenate([low, high])

    square = jnp.zeros((tile, 1), F32)
    for k in range(blocks):
        total = rows_of(residual_ref, k)
        for x in range(k // 2, side, 2):
            for y in range(k % 2, side, 2):
                total = total + x_ref[x * side + y].astype(F32)
        hidden_ref[k] = total
        square = square + jnp.sum(total * total, axis=1, keepdims=True)
    square = jnp.broadcast_to(square, (tile, HEAD_WIDTH))
    square = square + pltpu.roll(square, seq_count, 0)
    scale = lax.rsqrt(square[:, :1] / width + 1e-06)
    for k in range(blocks):
        normed[k] = (hidden_ref[k] * scale * rows_of(gain_ref, k)).astype(BF16)
    kept_ref[...] = normed[pl.ds(core * 2, 2)]
    given_ref[...] = normed[pl.ds(2 - core * 2, 2)]


def settle(x, residual, gain):
    tile, half = x.shape[1:]
    return kernel_call(
        settle_body,
        (shape(4, tile, half, dtype=F32), shape(2, tile, half), shape(2, tile, half)),
        [IN_VMEM] * 3,
        6,
        [pltpu.VMEM((4, tile, half), BF16)],
    )(x, residual, gain)


def route_body(ids_ref, weight_ref, pick_ref, mix_ref):
    core = lax.axis_index(CORES)
    tokens, topk = ids_ref.shape
    seq_count = tokens // 2
    lanes = pick_ref.shape[1]
    lane = lax.broadcasted_iota(jnp.int32, (tokens, lanes), 1)
    row = lax.broadcasted_iota(jnp.int32, (tokens, lanes), 0)
    weight = weight_ref[...]
    mixing = weight / jnp.sum(weight, axis=1, keepdims=True)
    ids = ids_ref[...]
    hit = jnp.zeros((tokens, lanes), F32)
    share = jnp.zeros((tokens, lanes), F32)
    for k in range(topk):
        same = ids[:, k : k + 1] == lane // 8
        hit = jnp.where(same, 1.0, hit)
        share = jnp.where(same, mixing[:, k : k + 1], share)
    rank = jnp.zeros((tokens, lanes), F32)
    for t in range(tokens - 1):
        rank = rank + jnp.where(row > t, jnp.broadcast_to(hit[t : t + 1], (tokens, lanes)), 0.0)
    taken = jnp.where(rank == (lane % 2).astype(F32), hit, 0.0)
    share = share * taken
    own_low = (row < seq_count) == (core == 0)
    quarter = lane // 2 % 4
    for src in range(2):
        low = own_low if src == 0 else jnp.logical_not(own_low)
        chosen = jnp.where(low, taken, pltpu.roll(taken, seq_count, 0))
        shares = jnp.where(low, share, pltpu.roll(share, seq_count, 0))
        for kk in range(2):
            at = (src * 2 + kk) * tokens
            mine = quarter == kk * 2 + row // seq_count
            pick_ref[at : at + tokens, :] = jnp.where(mine, chosen, 0.0).astype(BF16)
            value = jnp.where(mine, shares, 0.0)
            coarse = value.astype(BF16)
            mix_ref[at : at + tokens, :] = coarse
            mix_ref[4 * tokens + at : 5 * tokens + at, :] = (value - coarse.astype(F32)).astype(BF16)


def route(expert_ids, route_weight, chips):
    tokens = expert_ids.shape[0]
    return kernel_call(
        route_body, (shape(4 * tokens, 8 * chips), shape(8 * tokens, 8 * chips)), [IN_VMEM] * 2, 4
    )(expert_ids, route_weight)


def dispatch_body(kept_ref, other_ref, pick_ref, out_hbm, held, sems):
    pieces = [r[...].reshape(-1, r.shape[2]) for r in (kept_ref, other_ref)]
    tokens = jnp.concatenate(pieces)
    chips, tile, half = held.shape
    step = chips // 2
    copies = []
    for j in range(2):
        rows = lax.dot_general(
            pick_ref[:, j * step * tile : (j + 1) * step * tile],
            tokens,
            (((0,), (0,)), ((), ())),
            preferred_element_type=F32,
        )
        sent = slice(j * step, (j + 1) * step)
        held[sent] = rows.astype(BF16).reshape(step, tile, half)
        copies.append(pltpu.make_async_copy(held.at[sent], out_hbm.at[sent], sems.at[j]))
        copies[-1].start()
    for copy in copies:
        copy.wait()


def dispatch(kept, other, pick):
    tile, half = kept.shape[1:]
    dims = pick.shape[1] // tile, tile, half
    return sending_call(dispatch_body, dims, [IN_VMEM] * 3, 6, 2)(kept, other, pick)


def slot_order(size, back=False):
    sorted_row = lax.broadcasted_iota(jnp.int32, (size, size), 1 if back else 0)
    row = lax.broadcasted_iota(jnp.int32, (size, size), 0 if back else 1)
    slot = sorted_row % (size // 4)
    quarter = sorted_row // (size // 4)
    return jnp.where(row == slot // 2 * 8 + quarter * 2 + slot % 2, 1.0, 0.0).astype(BF16)


def gate_body(
    x_ref, kept_ref, gate_hbm, up_hbm, moved_hbm, down_hbm, part_ref, sent_ref, down_ref, rest, moved, sems
):
    core = lax.axis_index(CORES)
    chips, tile, part = x_ref.shape
    half, both = moved.shape
    units = both // 2
    count = kept_ref.shape[0]
    late = pl.ds(pl.multiple_of(core * half + count, part), half - count)
    pairs = [(gate_hbm.at[0, late, :], rest.at[:, :units]), (up_hbm.at[0, late, :], rest.at[:, units:])]
    step = half // 2
    for j in range(2):
        rows = slice(j * step, (j + 1) * step)
        pairs.append((moved_hbm.at[rows], moved.at[rows]))
    mine = pl.ds(pl.multiple_of(core * half, half), half)
    pairs.append((down_hbm.at[0, : down_ref.shape[0], mine], down_ref))
    copies = [pltpu.make_async_copy(*pair, sems.at[j]) for j, pair in enumerate(pairs)]
    for copy in copies:
        copy.start()
    size = 256
    groups = chips * tile // size
    order = slot_order(size)
    slots = size // 4
    sorted_rows = []
    for g in range(groups):
        rows = x_ref[g * size // tile : (g + 1) * size // tile].reshape(size, part)
        sorted_rows.append(jnp.dot(order, rows, preferred_element_type=F32).astype(BF16))
    quarters = [
        jnp.concatenate([r[p * slots : (p + 1) * slots] for r in sorted_rows]) for p in range(4)
    ]
    x = jnp.concatenate(quarters, axis=1)
    own = jnp.dot(x[:, :count], kept_ref[...], preferred_element_type=F32)
    for copy in copies[:2]:
        copy.wait()
    own = own + jnp.dot(x[:, count:], rest[...], preferred_element_type=F32)
    part_ref[:, :both] = own
    sent_ref[:, both:] = own.astype(BF16)
    copies[2].wait()
    other = jnp.dot(x[:, :step], moved[:step], preferred_element_type=F32)
    copies[3].wait()
    other = other + jnp.dot(x[:, step:], moved[step:], preferred_element_type=F32)
    part_ref[:, both:] = other
    sent_ref[:, :both] = other.astype(BF16)
    copies[4].wait()


def gate_up(x, kept, w_gate, w_up, moved, w_down, ahead):
    chips, tile, _ = x.shape
    half, both = moved.shape
    dims = chips * tile // 4, 2 * both
    return pl.pallas_call(
        gate_body,
        name="gate_up",
        out_shape=[pltpu.VMEM(dims, F32), pltpu.VMEM(dims, BF16), pltpu.VMEM((ahead, half), BF16)],
        in_specs=[IN_VMEM] * 2 + [IN_HBM] * 4,
        out_specs=[IN_VMEM] * 3,
        scratch_shapes=[
            pltpu.VMEM((half - kept.shape[0], both), BF16),
            pltpu.VMEM((half, both), BF16),
            pltpu.SemaphoreType.DMA((5,)),
        ],
        compiler_params=pltpu.CompilerParams(vmem_limit_bytes=14 * MIB),
    )(x, in_vmem(kept), *map(in_hbm, (w_gate, w_up, moved, w_down)))


def fetch_body(down_hbm, moved_hbm, after_ref, out_ref, sems):
    core = lax.axis_index(CORES)
    ahead = after_ref.shape[0]
    units, half = moved_hbm.shape
    kept = pl.ds(pl.multiple_of(core * half, half), half)
    copies = [
        pltpu.make_async_copy(
            down_hbm.at[0, ahead:, kept], out_ref.at[: units - ahead], sems.at[0]
        ),
        pltpu.make_async_copy(moved_hbm, out_ref.at[units - ahead :], sems.at[1]),
    ]
    for copy in copies:
        copy.start()
    for copy in copies:
        copy.wait()


def fetch_down(w_down, moved, after):
    units, half = moved.shape
    return pl.pallas_call(
        fetch_body,
        name="fetch_down",
        out_shape=pltpu.VMEM((2 * units - after.shape[0], half), BF16),
        in_specs=[IN_HBM] * 3,
        out_specs=IN_VMEM,
        scratch_shapes=[pltpu.SemaphoreType.DMA((2,))],
        compiler_params=pltpu.CompilerParams(vmem_limit_bytes=MIB),
    )(in_hbm(w_down), in_hbm(moved), after)


def down_body(part_ref, arrived_ref, first_ref, rest_ref, out_hbm, held, sems):
    chips, tile, part = held.shape
    size = 256
    groups = chips * tile // size
    order = slot_order(size, back=True)
    slots = size // 4
    ahead = first_ref.shape[0]
    units = (ahead + rest_ref.shape[0]) // 2

    def act(at):
        gate, up = (
            part_ref[:, j : j + units] + arrived_ref[:, j : j + units].astype(F32)
            for j in (at, at + units)
        )
        return (gate / (1.0 + jnp.exp(-gate)) * up).astype(BF16)

    hidden = jnp.concatenate([act(0), act(2 * units)], axis=1)
    quarters = []
    for p in range(4):
        lanes = slice(p * part, (p + 1) * part)
        value = jnp.dot(hidden[:, :ahead], first_ref[:, lanes], preferred_element_type=F32)
        value = value + jnp.dot(hidden[:, ahead:], rest_ref[:, lanes], preferred_element_type=F32)
        quarters.append(value.astype(BF16))
    copies = []
    for g in range(groups):
        rows = jnp.concatenate([v[g * slots : (g + 1) * slots] for v in quarters])
        rows = jnp.dot(order, rows, preferred_element_type=F32).astype(BF16)
        sent = slice(g * size // tile, (g + 1) * size // tile)
        held[sent] = rows.reshape(size // tile, tile, part)
        copies.append(pltpu.make_async_copy(held.at[sent], out_hbm.at[sent], sems.at[g]))
        copies[-1].start()
    for copy in copies:
        copy.wait()


def down(part, arrived, first, rest, tile):
    dims = part.shape[0] * 4 // tile, tile, first.shape[1] // 4
    return sending_call(down_body, dims, [IN_VMEM] * 4, 8, 2)(
        part, arrived, in_vmem(first), in_vmem(rest)
    )


def combine_body(x_ref, mix_ref, own_ref, other_ref):
    x = x_ref[...].reshape(-1, x_ref.shape[2])
    rows = jnp.dot(mix_ref[...], x, preferred_element_type=F32)
    count = rows.shape[0] // 2
    rows = rows[:count] + rows[count:]
    own_ref[...] = rows[: count // 2].reshape(own_ref.shape)
    other_ref[...] = rows[count // 2 :].reshape(other_ref.shape)


def combine(x, mix):
    out = shape(2, x.shape[1], x.shape[2], dtype=F32)
    return kernel_call(combine_body, (out, out), [IN_VMEM] * 2, 4)(x, mix)


def finish_body(hidden_ref, own_ref, other_ref, out_ref, total):
    core = lax.axis_index(CORES)
    blocks, tile, half = hidden_ref.shape
    total[pl.ds(core * 2, 2)] = own_ref[...]
    total[pl.ds(2 - core * 2, 2)] = other_ref[...]
    for k in range(blocks):
        value = (hidden_ref[k] + total[k]).astype(BF16)
        for q in range(2):
            at = (2 * k + q) * half
            out_ref[:, at : at + half] = value[q * tile // 2 : (q + 1) * tile // 2]


def finish(hidden, own, other):
    blocks, tile, half = hidden.shape
    return kernel_call(
        finish_body, shape(tile // 2, 2 * blocks * half), [IN_VMEM] * 3, 2, [pltpu.VMEM(hidden.shape, F32)]
    )(hidden, own, other)


def on_device(
    queries,
    token_keys,
    token_values,
    stored_keys,
    stored_values,
    kv_len,
    residual,
    out_weight,
    norm_gain,
    expert_ids,
    route_weight,
    w_gate,
    w_up,
    w_down,
):
    chips = lax.axis_size(CHIPS)
    side = math.isqrt(chips)
    own_raw = swapped(out_weight)
    outgoing, own, near, diagonal = attend(
        queries, token_keys, token_values, kv_len, stored_keys, stored_values, out_weight
    )
    step = [
        (2 * source + j, 2 * target + j)
        for j, way in enumerate((quad_step(side, 0, 1), quad_step(side, 1, 0)))
        for source, target in way
    ]
    near = lax.ppermute(near, (CHIPS, CORES), step)
    near_raw = lax.ppermute(own_raw, (CHIPS, CORES), step)
    diagonal = lax.ppermute(diagonal, CHIPS, quad_step(side, 1, 1))
    tokens = lax.all_to_all(outgoing, CHIPS, 0, 0, tiled=True)
    far, far_raw, diagonal_far = (swapped(x) for x in (near, near_raw, diagonal))
    weight = stack(own, own_raw, near, near_raw, far, far_raw, diagonal, diagonal_far)
    kept, *given_halves = halves(w_gate, w_up, w_down, 0.75)
    gate_moved, down_moved = (swapped(x) for x in given_halves)
    pick, mix = route(expert_ids, route_weight, chips)

    sums = project(tokens, weight)
    came_back = lax.all_to_all(sums, CHIPS, 0, 0, tiled=True)
    hidden, normed, normed_given = settle(came_back, residual, norm_gain[None])
    outgoing = dispatch(normed, swapped(normed_given), pick)
    incoming = lax.all_to_all(outgoing, CHIPS, 0, 0, tiled=True)
    part, sent, down_first = gate_up(incoming, kept, w_gate, w_up, gate_moved, w_down, 256)
    down_rest = fetch_down(w_down, down_moved, down_first)
    expert_out = down(part, swapped(sent), down_first, down_rest, incoming.shape[1])
    returned = lax.all_to_all(expert_out, CHIPS, 0, 0, tiled=True)
    moe_own, moe_given = combine(returned, mix)
    return finish(hidden, moe_own, swapped(moe_given))


def solution(mesh):
    in_specs = (
        P(("groups", "expert", "replica"), None),
        P(("groups", "expert", "replica"), None),
        P(("groups", "expert", "replica"), None),
        P(("groups", "expert", "replica"), None, None),
        P(("groups", "expert", "replica"), None, None),
        P(("groups", "expert", "replica")),
        P(("groups", "expert", "replica"), None),
        P(("expert", "replica"), None),
        P(),
        P(("groups", "expert"), None),
        P(("groups", "expert"), None),
        P("expert", None, "replica"),
        P("expert", None, "replica"),
        P("expert", "replica", None),
    )
    out_specs = P(("groups", "expert", "replica"), None)
    return jax.shard_map(
        on_device, mesh=mesh, in_specs=in_specs, out_specs=out_specs, check_vma=False
    )
```

```python
import math

import jax
import jax.numpy as jnp
from jax import lax
from jax.experimental import pallas as pl
from jax.experimental.pallas import tpu as pltpu
from jax.sharding import PartitionSpec as P

HEAD_WIDTH = 128
CHIPS, CORES = "expert", "replica"
F32, BF16 = jnp.float32, jnp.bfloat16
IN_VMEM = pl.BlockSpec(memory_space=pltpu.VMEM)
IN_SMEM = pl.BlockSpec(memory_space=pltpu.SMEM)
IN_HBM = pl.BlockSpec(memory_space=pltpu.HBM)


def swapped(x):
    return lax.ppermute(x, CORES, [(0, 1), (1, 0)])


def square_place(chip, side):
    x, y = chip // side % 2, chip % 2
    return x * 2 + y, 1 + (x ^ y)


def square_step(side, way):
    steps = []
    for x in range(side):
        for y in range(side):
            along_y = {1: (x ^ y) & 1 == 0, -1: (x ^ y) & 1 == 1}.get(way)
            dx, dy = (1, 1) if way == 0 else ((0, 1) if along_y else (1, 0))
            steps.append((x * side + y, (x ^ dx) * side + (y ^ dy)))
    return steps


MIB = 1 << 20


def in_hbm(x):
    return pltpu.with_memory_space_constraint(x, pltpu.HBM)


def in_vmem(x):
    return pltpu.with_memory_space_constraint(x, pltpu.VMEM)


def kernel_call(body, outs, in_specs, limit, scratch=()):
    return pl.pallas_call(
        body,
        out_shape=outs,
        in_specs=in_specs,
        out_specs=jax.tree.map(lambda _: IN_VMEM, outs),
        scratch_shapes=list(scratch),
        compiler_params=pltpu.CompilerParams(vmem_limit_bytes=limit * MIB),
    )


def shape(*dims, dtype=BF16):
    return jax.ShapeDtypeStruct(dims, dtype)


def attend_body(
    q_hbm,
    tk_hbm,
    tv_hbm,
    len_hbm,
    keys_hbm,
    values_hbm,
    weight_hbm,
    out_hbm,
    piece_own,
    piece_next,
    piece_last,
    piece_diagonal,
    q_ref,
    tk_ref,
    tv_ref,
    len_ref,
    keys,
    values,
    pieces,
    rows,
    mixed,
    scored,
    out_ref,
    sems,
    few,
):
    core = lax.axis_index(CORES)
    seq_count, cache_len, kv_width = keys_hbm.shape
    kv_count = kv_width // HEAD_WIDTH
    head_count = q_hbm.shape[1] // HEAD_WIDTH
    group = head_count // kv_count
    side = group // 2
    small = [
        pltpu.make_async_copy(source, target, few.at[j])
        for j, (source, target) in enumerate(
            ((q_hbm, q_ref), (tk_hbm, tk_ref), (tv_hbm, tv_ref), (len_hbm, len_ref))
        )
    ]
    for copy in small:
        copy.start()
    copies = [
        [pltpu.make_async_copy(source.at[b], target.at[b], sems.at[j, b]) for b in range(seq_count)]
        for j, (source, target) in enumerate(((keys_hbm, keys), (values_hbm, values)))
    ]
    for copy in copies[0] + copies[1]:
        copy.start()
    chip = lax.axis_index(CHIPS)
    place, ahead = square_place(chip, side)
    sliced, stored = [], []
    for j, (d, piece) in enumerate(
        ((0, piece_own), (ahead, piece_next), (3 - ahead, piece_last), (3, piece_diagonal))
    ):
        cols = piece.shape[1]
        at = pl.multiple_of((place ^ d) * cols, cols)
        source = weight_hbm.at[:, pl.ds(at, cols)]
        sliced.append(pltpu.make_async_copy(source, pieces.at[j], few.at[len(small) + j]))
        stored.append(pltpu.make_async_copy(pieces.at[j], piece, few.at[len(small) + 4 + j]))
        sliced[-1].start()
    for copy in small:
        copy.wait()
    for h in range(head_count):
        piece = q_ref[:, h * HEAD_WIDTH : (h + 1) * HEAD_WIDTH].astype(F32)
        rows[pl.ds(h, seq_count, stride=head_count), :] = piece
    inv_root = 1.0 / math.sqrt(HEAD_WIDTH)
    positions = lax.broadcasted_iota(jnp.int32, (head_count, cache_len), 1)
    lanes = [slice(g * HEAD_WIDTH, (g + 1) * HEAD_WIDTH) for g in range(kv_count)]
    fresh = []
    for copy in copies[0]:
        copy.wait()
    for b in range(seq_count):
        query = rows[b * head_count : (b + 1) * head_count, :]
        latest = [tk_ref[b : b + 1, lanes[g]].astype(F32) for g in range(kv_count)]
        latest = jnp.concatenate([jnp.broadcast_to(v, (group, HEAD_WIDTH)) for v in latest])
        fresh.append(jnp.sum(query * latest, axis=1, keepdims=True) * inv_root)
        query = query.astype(BF16)
        for g in range(kv_count):
            at = b * head_count + g * group
            scored[at : at + group, :] = lax.dot_general(
                query[g * group : (g + 1) * group],
                keys[b, :, lanes[g]],
                (((1,), (1,)), ((), ())),
                preferred_element_type=F32,
            )
    for copy in copies[1] + sliced:
        copy.wait()
    for copy in stored:
        copy.start()
    probs, fresh_probs = [], []
    for b in range(seq_count):
        scores = scored[b * head_count : (b + 1) * head_count, :]
        scores = jnp.where(positions < len_ref[b], scores * inv_root, -jnp.inf)
        highest = jnp.maximum(jnp.max(scores, axis=1, keepdims=True), fresh[b])
        cached_exp = jnp.exp(scores - highest)
        fresh_exp = jnp.exp(fresh[b] - highest)
        share = 1.0 / (jnp.sum(cached_exp, axis=1, keepdims=True) + fresh_exp)
        probs.append((cached_exp * share).astype(BF16))
        fresh_probs.append((fresh_exp * share).astype(BF16).astype(F32))
    for b in range(seq_count):
        for g in range(kv_count):
            heads = slice(g * group, (g + 1) * group)
            out = jnp.dot(probs[b][heads], values[b, :, lanes[g]], preferred_element_type=F32)
            out = out + fresh_probs[b][heads] * tv_ref[b : b + 1, lanes[g]].astype(F32)
            out = pltpu.roll(out, core * (HEAD_WIDTH // 2), 1)
            for a in range(2):
                start = g * group * seq_count + a * seq_count + b
                mixed[pl.ds(start, side, stride=2 * seq_count), :] = out[a * side : (a + 1) * side]
    tile = 2 * seq_count
    for g in range(kv_count):
        for y in range(side):
            for part, source in enumerate((y, y ^ 1)):
                at = (g * side + source) * tile
                near = mixed[at : at + tile, :]
                far = pltpu.roll(near, seq_count, 0)
                out_ref[2 * g * side + y, :, lanes[part]] = near.astype(BF16)
                out_ref[(2 * g + 1) * side + y, :, lanes[part]] = far.astype(BF16)
        sent = pl.ds(2 * g * side, 2 * side)
        stored.append(
            pltpu.make_async_copy(out_ref.at[sent], out_hbm.at[sent], few.at[len(small) + 8 + g])
        )
        stored[-1].start()
    for copy in stored:
        copy.wait()


def attend(queries, token_keys, token_values, kv_len, stored_keys, stored_values, out_weight):
    seq_count, feature_total = queries.shape
    heads = feature_total // HEAD_WIDTH
    rows, cols = out_weight.shape
    return pl.pallas_call(
        attend_body,
        name="attend",
        out_shape=[pltpu.HBM((heads, 2 * seq_count, 2 * HEAD_WIDTH), BF16)]
        + [pltpu.HBM((rows, cols // 4), BF16)] * 4,
        in_specs=[IN_HBM] * 7,
        out_specs=[IN_HBM] * 5,
        scratch_shapes=[
            pltpu.VMEM(queries.shape, BF16),
            pltpu.VMEM(token_keys.shape, BF16),
            pltpu.VMEM(token_values.shape, BF16),
            pltpu.SMEM(kv_len.shape, jnp.int32),
            pltpu.VMEM(stored_keys.shape, BF16),
            pltpu.VMEM(stored_values.shape, BF16),
            pltpu.VMEM((4, rows, cols // 4), BF16),
            pltpu.VMEM((seq_count * heads, HEAD_WIDTH), F32),
            pltpu.VMEM((seq_count * heads, HEAD_WIDTH), F32),
            pltpu.VMEM((seq_count * heads, stored_keys.shape[1]), F32),
            pltpu.VMEM((heads, 2 * seq_count, 2 * HEAD_WIDTH), BF16),
            pltpu.SemaphoreType.DMA((2, seq_count)),
            pltpu.SemaphoreType.DMA((16,)),
        ],
        compiler_params=pltpu.CompilerParams(vmem_limit_bytes=8 * MIB),
    )(
        *map(
            in_hbm,
            (queries, token_keys, token_values, kv_len, stored_keys, stored_values, out_weight),
        )
    )


def copy_all(pairs, sems):
    copies = [pltpu.make_async_copy(*pair, sems.at[j]) for j, pair in enumerate(pairs)]
    for copy in copies:
        copy.start()
    for copy in copies:
        copy.wait()


def stack_body(*refs):
    own, other, out_ref, sems = refs[:4], refs[4:8], refs[8], refs[9]
    rows = own[0].shape[0]
    side = math.isqrt(lax.axis_size(CHIPS))
    _, ahead = square_place(lax.axis_index(CHIPS), side)
    pairs = []
    for j, d in enumerate((0, 3 - ahead, ahead, 3)):
        for half, source in enumerate((own[j], other[j])):
            at = pl.multiple_of((2 * d + half) * rows, rows)
            pairs.append((source, out_ref.at[pl.ds(at, rows)]))
    copy_all(pairs, sems)


def stack(own, other):
    rows, cols = own[0].shape
    return pl.pallas_call(
        stack_body,
        name="stack",
        out_shape=pltpu.VMEM((8 * rows, cols), BF16),
        in_specs=[IN_HBM] * 8,
        out_specs=IN_VMEM,
        scratch_shapes=[pltpu.SemaphoreType.DMA((8,))],
        compiler_params=pltpu.CompilerParams(vmem_limit_bytes=2 * MIB),
    )(*map(in_hbm, own), *map(in_hbm, other))


def halves_body(gate_hbm, up_hbm, down_hbm, kept_ref, *refs):
    outs, (tall, wide, sems) = refs[:2], refs[2:]
    core = lax.axis_index(CORES)
    count = kept_ref.shape[0]
    half, both = tall.shape
    units = both // 2
    given = pl.ds(pl.multiple_of((1 - core) * half, half), half)
    kept = pl.ds(pl.multiple_of(core * half, half), count)
    left, right = slice(0, units), slice(units, both)
    pairs = (
        (gate_hbm.at[0, given, :], tall.at[:, left]),
        (up_hbm.at[0, given, :], tall.at[:, right]),
        (down_hbm.at[0, :, given], wide),
        (gate_hbm.at[0, kept, :], kept_ref.at[:, left]),
        (up_hbm.at[0, kept, :], kept_ref.at[:, right]),
        (tall, outs[0]),
        (wide, outs[1]),
    )
    copies = [pltpu.make_async_copy(*pair, sems.at[j]) for j, pair in enumerate(pairs)]
    for copy in copies[:5]:
        copy.start()
    for copy in copies[:2]:
        copy.wait()
    copies[5].start()
    copies[2].wait()
    copies[6].start()
    for copy in copies[3:]:
        copy.wait()


def halves(w_gate, w_up, w_down, kept_share):
    _, width, units = w_gate.shape
    tall, wide = (width // 2, 2 * units), (units, width // 2)
    return pl.pallas_call(
        halves_body,
        name="halves",
        out_shape=[
            pltpu.VMEM((int(width // 2 * kept_share), 2 * units), BF16),
            pltpu.HBM(tall, BF16),
            pltpu.HBM(wide, BF16),
        ],
        in_specs=[IN_HBM] * 3,
        out_specs=[IN_VMEM] + [IN_HBM] * 2,
        scratch_shapes=[
            pltpu.VMEM(tall, BF16),
            pltpu.VMEM(wide, BF16),
            pltpu.SemaphoreType.DMA((7,)),
        ],
        compiler_params=pltpu.CompilerParams(vmem_limit_bytes=6 * MIB),
    )(*map(in_hbm, (w_gate, w_up, w_down)))


def project_body(x_ref, weight_ref, out_hbm, held, sems):
    chips, tile, width = x_ref.shape
    cols = weight_ref.shape[1]
    half = cols // 2
    step = chips // 2

    def paired(first, second):
        low = lax.broadcasted_iota(jnp.int32, first.shape, 1) < tile // 2
        return (
            jnp.where(low, first, pltpu.roll(second, tile // 2, 1)),
            jnp.where(low, pltpu.roll(first, tile // 2, 1), second),
        )

    copies = []
    for j in range(2):
        sent = slice(j * step, (j + 1) * step)
        x = x_ref[sent].astype(F32).reshape(step // 2, 2, tile, width)
        x = jnp.concatenate(paired(x[:, 0], x[:, 1]), axis=2)
        x = x.reshape(step // 2 * tile, 2 * width).astype(BF16)
        sums = jnp.dot(x, weight_ref[...], preferred_element_type=F32)
        sums = sums.reshape(step // 2, tile, cols)
        sums = jnp.stack(paired(sums[:, :, :half], sums[:, :, half:]), axis=1)
        held[sent] = sums.reshape(step, tile, half).astype(BF16)
        copies.append(pltpu.make_async_copy(held.at[sent], out_hbm.at[sent], sems.at[j]))
        copies[-1].start()
    for copy in copies:
        copy.wait()


def sending_call(body, dims, in_specs, limit, chunks):
    return pl.pallas_call(
        body,
        out_shape=pltpu.HBM(dims, BF16),
        in_specs=in_specs,
        out_specs=IN_HBM,
        scratch_shapes=[pltpu.VMEM(dims, BF16), pltpu.SemaphoreType.DMA((chunks,))],
        compiler_params=pltpu.CompilerParams(vmem_limit_bytes=limit * MIB),
    )


def project(x, weight):
    dims = x.shape[0], x.shape[1], weight.shape[1] // 2
    return sending_call(project_body, dims, [IN_VMEM] * 2, 12, 2)(
        x, in_vmem(weight)
    )


def settle_body(x_ref, residual_ref, gain_ref, hidden_ref, kept_ref, given_ref, normed):
    core = lax.axis_index(CORES)
    chips, tile, half = x_ref.shape
    side = math.isqrt(chips)
    blocks = 4
    seq_count = tile // 2
    width = residual_ref.shape[1]

    def rows_of(ref, k):
        low, high = (ref[:, (2 * k + q) * half : (2 * k + q + 1) * half].astype(F32) for q in (0, 1))
        low, high = (jnp.broadcast_to(v, (seq_count, half)) for v in (low, high))
        return jnp.concatenate([low, high])

    square = jnp.zeros((tile, 1), F32)
    for k in range(blocks):
        total = rows_of(residual_ref, k)
        for x in range(k // 2, side, 2):
            for y in range(k % 2, side, 2):
                total = total + x_ref[x * side + y].astype(F32)
        hidden_ref[k] = total
        square = square + jnp.sum(total * total, axis=1, keepdims=True)
    square = jnp.broadcast_to(square, (tile, HEAD_WIDTH))
    square = square + pltpu.roll(square, seq_count, 0)
    scale = lax.rsqrt(square[:, :1] / width + 1e-06)
    for k in range(blocks):
        normed[k] = (hidden_ref[k] * scale * rows_of(gain_ref, k)).astype(BF16)
    kept_ref[...] = normed[pl.ds(core * 2, 2)]
    given_ref[...] = normed[pl.ds(2 - core * 2, 2)]


def settle(x, residual, gain):
    tile, half = x.shape[1:]
    return kernel_call(
        settle_body,
        (shape(4, tile, half, dtype=F32), shape(2, tile, half), shape(2, tile, half)),
        [IN_VMEM] * 3,
        6,
        [pltpu.VMEM((4, tile, half), BF16)],
    )(x, residual, gain)


def route_body(ids_ref, weight_ref, pick_ref, mix_ref):
    core = lax.axis_index(CORES)
    tokens, topk = ids_ref.shape
    seq_count = tokens // 2
    lanes = pick_ref.shape[1]
    lane = lax.broadcasted_iota(jnp.int32, (tokens, lanes), 1)
    row = lax.broadcasted_iota(jnp.int32, (tokens, lanes), 0)
    weight = weight_ref[...]
    mixing = weight / jnp.sum(weight, axis=1, keepdims=True)
    ids = ids_ref[...]
    hit = jnp.zeros((tokens, lanes), F32)
    share = jnp.zeros((tokens, lanes), F32)
    for k in range(topk):
        same = ids[:, k : k + 1] == lane // 8
        hit = jnp.where(same, 1.0, hit)
        share = jnp.where(same, mixing[:, k : k + 1], share)
    rank = jnp.zeros((tokens, lanes), F32)
    for t in range(tokens - 1):
        rank = rank + jnp.where(row > t, jnp.broadcast_to(hit[t : t + 1], (tokens, lanes)), 0.0)
    taken = jnp.where(rank == (lane % 2).astype(F32), hit, 0.0)
    share = share * taken
    own_low = (row < seq_count) == (core == 0)
    quarter = lane // 2 % 4
    for src in range(2):
        low = own_low if src == 0 else jnp.logical_not(own_low)
        chosen = jnp.where(low, taken, pltpu.roll(taken, seq_count, 0))
        shares = jnp.where(low, share, pltpu.roll(share, seq_count, 0))
        for kk in range(2):
            at = (src * 2 + kk) * tokens
            mine = quarter == kk * 2 + row // seq_count
            pick_ref[at : at + tokens, :] = jnp.where(mine, chosen, 0.0).astype(BF16)
            value = jnp.where(mine, shares, 0.0)
            coarse = value.astype(BF16)
            mix_ref[at : at + tokens, :] = coarse
            mix_ref[4 * tokens + at : 5 * tokens + at, :] = (value - coarse.astype(F32)).astype(BF16)


def route(expert_ids, route_weight, chips):
    tokens = expert_ids.shape[0]
    return kernel_call(
        route_body, (shape(4 * tokens, 8 * chips), shape(8 * tokens, 8 * chips)), [IN_VMEM] * 2, 4
    )(expert_ids, route_weight)


def dispatch_body(kept_ref, other_ref, pick_ref, out_hbm, held, sems):
    pieces = [r[...].reshape(-1, r.shape[2]) for r in (kept_ref, other_ref)]
    tokens = jnp.concatenate(pieces)
    chips, tile, half = held.shape
    step = chips // 2
    copies = []
    for j in range(2):
        rows = lax.dot_general(
            pick_ref[:, j * step * tile : (j + 1) * step * tile],
            tokens,
            (((0,), (0,)), ((), ())),
            preferred_element_type=F32,
        )
        sent = slice(j * step, (j + 1) * step)
        held[sent] = rows.astype(BF16).reshape(step, tile, half)
        copies.append(pltpu.make_async_copy(held.at[sent], out_hbm.at[sent], sems.at[j]))
        copies[-1].start()
    for copy in copies:
        copy.wait()


def dispatch(kept, other, pick):
    tile, half = kept.shape[1:]
    dims = pick.shape[1] // tile, tile, half
    return sending_call(dispatch_body, dims, [IN_VMEM] * 3, 6, 2)(kept, other, pick)


def slot_order(size, back=False):
    sorted_row = lax.broadcasted_iota(jnp.int32, (size, size), 1 if back else 0)
    row = lax.broadcasted_iota(jnp.int32, (size, size), 0 if back else 1)
    slot = sorted_row % (size // 4)
    quarter = sorted_row // (size // 4)
    return jnp.where(row == slot // 2 * 8 + quarter * 2 + slot % 2, 1.0, 0.0).astype(BF16)


def gate_body(
    x_ref, kept_ref, gate_hbm, up_hbm, moved_hbm, down_hbm, part_ref, sent_ref, down_ref, rest, moved, sems
):
    core = lax.axis_index(CORES)
    chips, tile, part = x_ref.shape
    half, both = moved.shape
    units = both // 2
    count = kept_ref.shape[0]
    late = pl.ds(pl.multiple_of(core * half + count, part), half - count)
    pairs = [(gate_hbm.at[0, late, :], rest.at[:, :units]), (up_hbm.at[0, late, :], rest.at[:, units:])]
    step = half // 2
    for j in range(2):
        rows = slice(j * step, (j + 1) * step)
        pairs.append((moved_hbm.at[rows], moved.at[rows]))
    mine = pl.ds(pl.multiple_of(core * half, half), half)
    pairs.append((down_hbm.at[0, : down_ref.shape[0], mine], down_ref))
    copies = [pltpu.make_async_copy(*pair, sems.at[j]) for j, pair in enumerate(pairs)]
    for copy in copies:
        copy.start()
    size = 256
    groups = chips * tile // size
    order = slot_order(size)
    slots = size // 4
    sorted_rows = []
    for g in range(groups):
        rows = x_ref[g * size // tile : (g + 1) * size // tile].reshape(size, part)
        sorted_rows.append(jnp.dot(order, rows, preferred_element_type=F32).astype(BF16))
    quarters = [
        jnp.concatenate([r[p * slots : (p + 1) * slots] for r in sorted_rows]) for p in range(4)
    ]
    x = jnp.concatenate(quarters, axis=1)
    own = jnp.dot(x[:, :count], kept_ref[...], preferred_element_type=F32)
    for copy in copies[:2]:
        copy.wait()
    own = own + jnp.dot(x[:, count:], rest[...], preferred_element_type=F32)
    part_ref[:, :both] = own
    sent_ref[:, both:] = own.astype(BF16)
    copies[2].wait()
    other = jnp.dot(x[:, :step], moved[:step], preferred_element_type=F32)
    copies[3].wait()
    other = other + jnp.dot(x[:, step:], moved[step:], preferred_element_type=F32)
    part_ref[:, both:] = other
    sent_ref[:, :both] = other.astype(BF16)
    copies[4].wait()


def gate_up(x, kept, w_gate, w_up, moved, w_down, ahead):
    chips, tile, _ = x.shape
    half, both = moved.shape
    dims = chips * tile // 4, 2 * both
    return pl.pallas_call(
        gate_body,
        name="gate_up",
        out_shape=[pltpu.VMEM(dims, F32), pltpu.VMEM(dims, BF16), pltpu.VMEM((ahead, half), BF16)],
        in_specs=[IN_VMEM] * 2 + [IN_HBM] * 4,
        out_specs=[IN_VMEM] * 3,
        scratch_shapes=[
            pltpu.VMEM((half - kept.shape[0], both), BF16),
            pltpu.VMEM((half, both), BF16),
            pltpu.SemaphoreType.DMA((5,)),
        ],
        compiler_params=pltpu.CompilerParams(vmem_limit_bytes=14 * MIB),
    )(x, in_vmem(kept), *map(in_hbm, (w_gate, w_up, moved, w_down)))


def fetch_body(down_hbm, moved_hbm, after_ref, out_ref, sems):
    core = lax.axis_index(CORES)
    ahead = after_ref.shape[0]
    units, half = moved_hbm.shape
    kept = pl.ds(pl.multiple_of(core * half, half), half)
    copies = [
        pltpu.make_async_copy(
            down_hbm.at[0, ahead:, kept], out_ref.at[: units - ahead], sems.at[0]
        ),
        pltpu.make_async_copy(moved_hbm, out_ref.at[units - ahead :], sems.at[1]),
    ]
    for copy in copies:
        copy.start()
    for copy in copies:
        copy.wait()


def fetch_down(w_down, moved, after):
    units, half = moved.shape
    return pl.pallas_call(
        fetch_body,
        name="fetch_down",
        out_shape=pltpu.VMEM((2 * units - after.shape[0], half), BF16),
        in_specs=[IN_HBM] * 3,
        out_specs=IN_VMEM,
        scratch_shapes=[pltpu.SemaphoreType.DMA((2,))],
        compiler_params=pltpu.CompilerParams(vmem_limit_bytes=MIB),
    )(in_hbm(w_down), in_hbm(moved), after)


def down_body(part_ref, arrived_ref, first_ref, rest_ref, out_hbm, held, sems):
    chips, tile, part = held.shape
    size = 256
    groups = chips * tile // size
    order = slot_order(size, back=True)
    slots = size // 4
    ahead = first_ref.shape[0]
    units = (ahead + rest_ref.shape[0]) // 2

    def act(at):
        gate, up = (
            part_ref[:, j : j + units] + arrived_ref[:, j : j + units].astype(F32)
            for j in (at, at + units)
        )
        return (gate / (1.0 + jnp.exp(-gate)) * up).astype(BF16)

    hidden = jnp.concatenate([act(0), act(2 * units)], axis=1)
    quarters = []
    for p in range(4):
        lanes = slice(p * part, (p + 1) * part)
        value = jnp.dot(hidden[:, :ahead], first_ref[:, lanes], preferred_element_type=F32)
        value = value + jnp.dot(hidden[:, ahead:], rest_ref[:, lanes], preferred_element_type=F32)
        quarters.append(value.astype(BF16))
    copies = []
    for g in range(groups):
        rows = jnp.concatenate([v[g * slots : (g + 1) * slots] for v in quarters])
        rows = jnp.dot(order, rows, preferred_element_type=F32).astype(BF16)
        sent = slice(g * size // tile, (g + 1) * size // tile)
        held[sent] = rows.reshape(size // tile, tile, part)
        copies.append(pltpu.make_async_copy(held.at[sent], out_hbm.at[sent], sems.at[g]))
        copies[-1].start()
    for copy in copies:
        copy.wait()


def down(part, arrived, first, rest, tile):
    dims = part.shape[0] * 4 // tile, tile, first.shape[1] // 4
    return sending_call(down_body, dims, [IN_VMEM] * 4, 8, 2)(
        part, arrived, in_vmem(first), in_vmem(rest)
    )


def combine_body(x_ref, mix_ref, own_ref, other_ref):
    x = x_ref[...].reshape(-1, x_ref.shape[2])
    rows = jnp.dot(mix_ref[...], x, preferred_element_type=F32)
    count = rows.shape[0] // 2
    rows = rows[:count] + rows[count:]
    own_ref[...] = rows[: count // 2].reshape(own_ref.shape)
    other_ref[...] = rows[count // 2 :].reshape(other_ref.shape)


def combine(x, mix):
    out = shape(2, x.shape[1], x.shape[2], dtype=F32)
    return kernel_call(combine_body, (out, out), [IN_VMEM] * 2, 4)(x, mix)


def finish_body(hidden_ref, own_ref, other_ref, out_ref, total):
    core = lax.axis_index(CORES)
    blocks, tile, half = hidden_ref.shape
    total[pl.ds(core * 2, 2)] = own_ref[...]
    total[pl.ds(2 - core * 2, 2)] = other_ref[...]
    for k in range(blocks):
        value = (hidden_ref[k] + total[k]).astype(BF16)
        for q in range(2):
            at = (2 * k + q) * half
            out_ref[:, at : at + half] = value[q * tile // 2 : (q + 1) * tile // 2]


def finish(hidden, own, other):
    blocks, tile, half = hidden.shape
    return kernel_call(
        finish_body, shape(tile // 2, 2 * blocks * half), [IN_VMEM] * 3, 2, [pltpu.VMEM(hidden.shape, F32)]
    )(hidden, own, other)


def on_device(
    queries,
    token_keys,
    token_values,
    stored_keys,
    stored_values,
    kv_len,
    residual,
    out_weight,
    norm_gain,
    expert_ids,
    route_weight,
    w_gate,
    w_up,
    w_down,
):
    chips = lax.axis_size(CHIPS)
    side = math.isqrt(chips)
    outgoing, *pieces = attend(
        queries, token_keys, token_values, kv_len, stored_keys, stored_values, out_weight
    )
    own = pieces[:1] + [
        lax.ppermute(piece, CHIPS, square_step(side, way))
        for piece, way in zip(pieces[1:], (1, -1, 0), strict=True)
    ]
    tokens = lax.all_to_all(outgoing, CHIPS, 0, 0, tiled=True)
    other = [swapped(piece) for piece in own]
    weight = stack(own, other)
    kept, *given_halves = halves(w_gate, w_up, w_down, 0.75)
    gate_moved, down_moved = (swapped(x) for x in given_halves)
    pick, mix = route(expert_ids, route_weight, chips)

    sums = project(tokens, weight)
    came_back = lax.all_to_all(sums, CHIPS, 0, 0, tiled=True)
    hidden, normed, normed_given = settle(came_back, residual, norm_gain[None])
    outgoing = dispatch(normed, swapped(normed_given), pick)
    incoming = lax.all_to_all(outgoing, CHIPS, 0, 0, tiled=True)
    part, sent, down_first = gate_up(incoming, kept, w_gate, w_up, gate_moved, w_down, 256)
    down_rest = fetch_down(w_down, down_moved, down_first)
    expert_out = down(part, swapped(sent), down_first, down_rest, incoming.shape[1])
    returned = lax.all_to_all(expert_out, CHIPS, 0, 0, tiled=True)
    moe_own, moe_given = combine(returned, mix)
    return finish(hidden, moe_own, swapped(moe_given))


def solution(mesh):
    in_specs = (
        P(("groups", "expert", "replica"), None),
        P(("groups", "expert", "replica"), None),
        P(("groups", "expert", "replica"), None),
        P(("groups", "expert", "replica"), None, None),
        P(("groups", "expert", "replica"), None, None),
        P(("groups", "expert", "replica")),
        P(("groups", "expert", "replica"), None),
        P(("expert", "replica"), None),
        P(),
        P(("groups", "expert"), None),
        P(("groups", "expert"), None),
        P("expert", None, "replica"),
        P("expert", None, "replica"),
        P("expert", "replica", None),
    )
    out_specs = P(("groups", "expert", "replica"), None)
    return jax.shard_map(
        on_device, mesh=mesh, in_specs=in_specs, out_specs=out_specs, check_vma=False
    )
```

```python
import math

import jax
import jax.numpy as jnp
from jax import lax
from jax.experimental import pallas as pl
from jax.experimental.pallas import tpu as pltpu
from jax.sharding import PartitionSpec as P

HEAD_WIDTH = 128
CHIPS, CORES = "expert", "replica"
F32, BF16 = jnp.float32, jnp.bfloat16
IN_VMEM = pl.BlockSpec(memory_space=pltpu.VMEM)
IN_SMEM = pl.BlockSpec(memory_space=pltpu.SMEM)
IN_HBM = pl.BlockSpec(memory_space=pltpu.HBM)


def swapped(x):
    return lax.ppermute(x, CORES, [(0, 1), (1, 0)])


def square_place(chip, side):
    x, y = chip // side % 2, chip % 2
    return x * 2 + y, 1 + (x ^ y)


def square_step(side, way):
    steps = []
    for x in range(side):
        for y in range(side):
            along_y = {1: (x ^ y) & 1 == 0, -1: (x ^ y) & 1 == 1}.get(way)
            dx, dy = (1, 1) if way == 0 else ((0, 1) if along_y else (1, 0))
            steps.append((x * side + y, (x ^ dx) * side + (y ^ dy)))
    return steps


MIB = 1 << 20


def in_hbm(x):
    return pltpu.with_memory_space_constraint(x, pltpu.HBM)


def in_vmem(x):
    return pltpu.with_memory_space_constraint(x, pltpu.VMEM)


def kernel_call(body, outs, in_specs, limit, scratch=()):
    return pl.pallas_call(
        body,
        out_shape=outs,
        in_specs=in_specs,
        out_specs=jax.tree.map(lambda _: IN_VMEM, outs),
        scratch_shapes=list(scratch),
        compiler_params=pltpu.CompilerParams(vmem_limit_bytes=limit * MIB),
    )


def shape(*dims, dtype=BF16):
    return jax.ShapeDtypeStruct(dims, dtype)


def attend_body(
    q_hbm,
    tk_hbm,
    tv_hbm,
    len_hbm,
    keys_hbm,
    values_hbm,
    weight_hbm,
    out_hbm,
    piece_own,
    piece_next,
    piece_last,
    piece_diagonal,
    q_ref,
    tk_ref,
    tv_ref,
    len_ref,
    keys,
    values,
    pieces,
    rows,
    mixed,
    scored,
    out_ref,
    sems,
    few,
):
    core = lax.axis_index(CORES)
    seq_count, cache_len, kv_width = keys_hbm.shape
    kv_count = kv_width // HEAD_WIDTH
    head_count = q_hbm.shape[1] // HEAD_WIDTH
    group = head_count // kv_count
    side = group // 2
    small = [
        pltpu.make_async_copy(source, target, few.at[j])
        for j, (source, target) in enumerate(
            ((q_hbm, q_ref), (tk_hbm, tk_ref), (tv_hbm, tv_ref), (len_hbm, len_ref))
        )
    ]
    for copy in small:
        copy.start()
    copies = [
        [pltpu.make_async_copy(source.at[b], target.at[b], sems.at[j, b]) for b in range(seq_count)]
        for j, (source, target) in enumerate(((keys_hbm, keys), (values_hbm, values)))
    ]
    for copy in copies[0] + copies[1]:
        copy.start()
    chip = lax.axis_index(CHIPS)
    place, ahead = square_place(chip, side)
    sliced, stored = [], []
    for j, (d, piece) in enumerate(
        ((0, piece_own), (ahead, piece_next), (3 - ahead, piece_last), (3, piece_diagonal))
    ):
        cols = piece.shape[1]
        at = pl.multiple_of((place ^ d) * cols, cols)
        source = weight_hbm.at[:, pl.ds(at, cols)]
        sliced.append(pltpu.make_async_copy(source, pieces.at[j], few.at[len(small) + j]))
        stored.append(pltpu.make_async_copy(pieces.at[j], piece, few.at[len(small) + 4 + j]))
        sliced[-1].start()
    for copy in small:
        copy.wait()
    for h in range(head_count):
        piece = q_ref[:, h * HEAD_WIDTH : (h + 1) * HEAD_WIDTH].astype(F32)
        rows[pl.ds(h, seq_count, stride=head_count), :] = piece
    inv_root = 1.0 / math.sqrt(HEAD_WIDTH)
    positions = lax.broadcasted_iota(jnp.int32, (head_count, cache_len), 1)
    lanes = [slice(g * HEAD_WIDTH, (g + 1) * HEAD_WIDTH) for g in range(kv_count)]
    fresh = []
    for copy in copies[0]:
        copy.wait()
    for b in range(seq_count):
        query = rows[b * head_count : (b + 1) * head_count, :]
        latest = [tk_ref[b : b + 1, lanes[g]].astype(F32) for g in range(kv_count)]
        latest = jnp.concatenate([jnp.broadcast_to(v, (group, HEAD_WIDTH)) for v in latest])
        fresh.append(jnp.sum(query * latest, axis=1, keepdims=True) * inv_root)
        query = query.astype(BF16)
        for g in range(kv_count):
            at = b * head_count + g * group
            scored[at : at + group, :] = lax.dot_general(
                query[g * group : (g + 1) * group],
                keys[b, :, lanes[g]],
                (((1,), (1,)), ((), ())),
                preferred_element_type=F32,
            )
    for copy in copies[1] + sliced:
        copy.wait()
    for copy in stored:
        copy.start()
    probs, fresh_probs = [], []
    for b in range(seq_count):
        scores = scored[b * head_count : (b + 1) * head_count, :]
        scores = jnp.where(positions < len_ref[b], scores * inv_root, -jnp.inf)
        highest = jnp.maximum(jnp.max(scores, axis=1, keepdims=True), fresh[b])
        cached_exp = jnp.exp(scores - highest)
        fresh_exp = jnp.exp(fresh[b] - highest)
        share = 1.0 / (jnp.sum(cached_exp, axis=1, keepdims=True) + fresh_exp)
        probs.append((cached_exp * share).astype(BF16))
        fresh_probs.append((fresh_exp * share).astype(BF16).astype(F32))
    for b in range(seq_count):
        for g in range(kv_count):
            heads = slice(g * group, (g + 1) * group)
            out = jnp.dot(probs[b][heads], values[b, :, lanes[g]], preferred_element_type=F32)
            out = out + fresh_probs[b][heads] * tv_ref[b : b + 1, lanes[g]].astype(F32)
            out = pltpu.roll(out, core * (HEAD_WIDTH // 2), 1)
            for a in range(2):
                start = g * group * seq_count + a * seq_count + b
                mixed[pl.ds(start, side, stride=2 * seq_count), :] = out[a * side : (a + 1) * side]
    tile = 2 * seq_count
    for g in range(kv_count):
        for y in range(side):
            for part, source in enumerate((y, y ^ 1)):
                at = (g * side + source) * tile
                near = mixed[at : at + tile, :]
                far = pltpu.roll(near, seq_count, 0)
                out_ref[2 * g * side + y, :, lanes[part]] = near.astype(BF16)
                out_ref[(2 * g + 1) * side + y, :, lanes[part]] = far.astype(BF16)
        sent = pl.ds(2 * g * side, 2 * side)
        stored.append(
            pltpu.make_async_copy(out_ref.at[sent], out_hbm.at[sent], few.at[len(small) + 8 + g])
        )
        stored[-1].start()
    for copy in stored:
        copy.wait()


def attend(queries, token_keys, token_values, kv_len, stored_keys, stored_values, out_weight):
    seq_count, feature_total = queries.shape
    heads = feature_total // HEAD_WIDTH
    rows, cols = out_weight.shape
    return pl.pallas_call(
        attend_body,
        name="attend",
        out_shape=[pltpu.HBM((heads, 2 * seq_count, 2 * HEAD_WIDTH), BF16)]
        + [pltpu.HBM((rows, cols // 4), BF16)] * 4,
        in_specs=[IN_HBM] * 7,
        out_specs=[IN_HBM] * 5,
        scratch_shapes=[
            pltpu.VMEM(queries.shape, BF16),
            pltpu.VMEM(token_keys.shape, BF16),
            pltpu.VMEM(token_values.shape, BF16),
            pltpu.SMEM(kv_len.shape, jnp.int32),
            pltpu.VMEM(stored_keys.shape, BF16),
            pltpu.VMEM(stored_values.shape, BF16),
            pltpu.VMEM((4, rows, cols // 4), BF16),
            pltpu.VMEM((seq_count * heads, HEAD_WIDTH), F32),
            pltpu.VMEM((seq_count * heads, HEAD_WIDTH), F32),
            pltpu.VMEM((seq_count * heads, stored_keys.shape[1]), F32),
            pltpu.VMEM((heads, 2 * seq_count, 2 * HEAD_WIDTH), BF16),
            pltpu.SemaphoreType.DMA((2, seq_count)),
            pltpu.SemaphoreType.DMA((16,)),
        ],
        compiler_params=pltpu.CompilerParams(vmem_limit_bytes=8 * MIB),
    )(
        *map(
            in_hbm,
            (queries, token_keys, token_values, kv_len, stored_keys, stored_values, out_weight),
        )
    )


def copy_all(pairs, sems):
    copies = [pltpu.make_async_copy(*pair, sems.at[j]) for j, pair in enumerate(pairs)]
    for copy in copies:
        copy.start()
    for copy in copies:
        copy.wait()


def stack_body(*refs):
    own, other, out_ref, sems = refs[:4], refs[4:8], refs[8], refs[9]
    rows = own[0].shape[0]
    side = math.isqrt(lax.axis_size(CHIPS))
    _, ahead = square_place(lax.axis_index(CHIPS), side)
    pairs = []
    for j, d in enumerate((0, 3 - ahead, ahead, 3)):
        for half, source in enumerate((own[j], other[j])):
            at = pl.multiple_of((2 * d + half) * rows, rows)
            pairs.append((source, out_ref.at[pl.ds(at, rows)]))
    copy_all(pairs, sems)


def stack(own, other):
    rows, cols = own[0].shape
    return pl.pallas_call(
        stack_body,
        name="stack",
        out_shape=pltpu.VMEM((8 * rows, cols), BF16),
        in_specs=[IN_HBM] * 8,
        out_specs=IN_VMEM,
        scratch_shapes=[pltpu.SemaphoreType.DMA((8,))],
        compiler_params=pltpu.CompilerParams(vmem_limit_bytes=2 * MIB),
    )(*map(in_hbm, own), *map(in_hbm, other))


def halves_body(gate_hbm, up_hbm, down_hbm, kept_ref, *refs):
    outs, (tall, wide, sems) = refs[:2], refs[2:]
    core = lax.axis_index(CORES)
    count = kept_ref.shape[0]
    half, both = tall.shape
    units = both // 2
    given = pl.ds(pl.multiple_of((1 - core) * half, half), half)
    kept = pl.ds(pl.multiple_of(core * half, half), count)
    left, right = slice(0, units), slice(units, both)
    pairs = (
        (gate_hbm.at[0, given, :], tall.at[:, left]),
        (up_hbm.at[0, given, :], tall.at[:, right]),
        (down_hbm.at[0, :, given], wide),
        (gate_hbm.at[0, kept, :], kept_ref.at[:, left]),
        (up_hbm.at[0, kept, :], kept_ref.at[:, right]),
        (tall, outs[0]),
        (wide, outs[1]),
    )
    copies = [pltpu.make_async_copy(*pair, sems.at[j]) for j, pair in enumerate(pairs)]
    for copy in copies[:5]:
        copy.start()
    for copy in copies[:2]:
        copy.wait()
    copies[5].start()
    copies[2].wait()
    copies[6].start()
    for copy in copies[3:]:
        copy.wait()


def halves(w_gate, w_up, w_down, kept_share):
    _, width, units = w_gate.shape
    tall, wide = (width // 2, 2 * units), (units, width // 2)
    return pl.pallas_call(
        halves_body,
        name="halves",
        out_shape=[
            pltpu.VMEM((int(width // 2 * kept_share), 2 * units), BF16),
            pltpu.HBM(tall, BF16),
            pltpu.HBM(wide, BF16),
        ],
        in_specs=[IN_HBM] * 3,
        out_specs=[IN_VMEM] + [IN_HBM] * 2,
        scratch_shapes=[
            pltpu.VMEM(tall, BF16),
            pltpu.VMEM(wide, BF16),
            pltpu.SemaphoreType.DMA((7,)),
        ],
        compiler_params=pltpu.CompilerParams(vmem_limit_bytes=6 * MIB),
    )(*map(in_hbm, (w_gate, w_up, w_down)))


def project_body(x_ref, weight_ref, out_hbm, held, sems):
    chips, tile, width = x_ref.shape
    cols = weight_ref.shape[1]
    half = cols // 2
    step = chips // 2

    def paired(first, second):
        low = lax.broadcasted_iota(jnp.int32, first.shape, 1) < tile // 2
        return (
            jnp.where(low, first, pltpu.roll(second, tile // 2, 1)),
            jnp.where(low, pltpu.roll(first, tile // 2, 1), second),
        )

    copies = []
    for j in range(2):
        sent = slice(j * step, (j + 1) * step)
        x = x_ref[sent].astype(F32).reshape(step // 2, 2, tile, width)
        x = jnp.concatenate(paired(x[:, 0], x[:, 1]), axis=2)
        x = x.reshape(step // 2 * tile, 2 * width).astype(BF16)
        sums = jnp.dot(x, weight_ref[...], preferred_element_type=F32)
        sums = sums.reshape(step // 2, tile, cols)
        sums = jnp.stack(paired(sums[:, :, :half], sums[:, :, half:]), axis=1)
        held[sent] = sums.reshape(step, tile, half).astype(BF16)
        copies.append(pltpu.make_async_copy(held.at[sent], out_hbm.at[sent], sems.at[j]))
        copies[-1].start()
    for copy in copies:
        copy.wait()


def sending_call(body, dims, in_specs, limit, chunks):
    return pl.pallas_call(
        body,
        out_shape=pltpu.HBM(dims, BF16),
        in_specs=in_specs,
        out_specs=IN_HBM,
        scratch_shapes=[pltpu.VMEM(dims, BF16), pltpu.SemaphoreType.DMA((chunks,))],
        compiler_params=pltpu.CompilerParams(vmem_limit_bytes=limit * MIB),
    )


def project(x, weight):
    dims = x.shape[0], x.shape[1], weight.shape[1] // 2
    return sending_call(project_body, dims, [IN_VMEM] * 2, 12, 2)(
        x, in_vmem(weight)
    )


def settle_body(x_ref, residual_ref, gain_ref, hidden_ref, kept_ref, given_ref, normed):
    core = lax.axis_index(CORES)
    chips, tile, half = x_ref.shape
    side = math.isqrt(chips)
    blocks = 4
    seq_count = tile // 2
    width = residual_ref.shape[1]

    def rows_of(ref, k):
        low, high = (ref[:, (2 * k + q) * half : (2 * k + q + 1) * half].astype(F32) for q in (0, 1))
        low, high = (jnp.broadcast_to(v, (seq_count, half)) for v in (low, high))
        return jnp.concatenate([low, high])

    square = jnp.zeros((tile, 1), F32)
    for k in range(blocks):
        total = rows_of(residual_ref, k)
        for x in range(k // 2, side, 2):
            for y in range(k % 2, side, 2):
                total = total + x_ref[x * side + y].astype(F32)
        hidden_ref[k] = total
        square = square + jnp.sum(total * total, axis=1, keepdims=True)
    square = jnp.broadcast_to(square, (tile, HEAD_WIDTH))
    square = square + pltpu.roll(square, seq_count, 0)
    scale = lax.rsqrt(square[:, :1] / width + 1e-06)
    for k in range(blocks):
        normed[k] = (hidden_ref[k] * scale * rows_of(gain_ref, k)).astype(BF16)
    kept_ref[...] = normed[pl.ds(core * 2, 2)]
    given_ref[...] = normed[pl.ds(2 - core * 2, 2)]


def settle(x, residual, gain):
    tile, half = x.shape[1:]
    return kernel_call(
        settle_body,
        (shape(4, tile, half, dtype=F32), shape(2, tile, half), shape(2, tile, half)),
        [IN_VMEM] * 3,
        6,
        [pltpu.VMEM((4, tile, half), BF16)],
    )(x, residual, gain)


def route_body(ids_ref, weight_ref, pick_ref, mix_ref):
    core = lax.axis_index(CORES)
    tokens, topk = ids_ref.shape
    seq_count = tokens // 2
    lanes = pick_ref.shape[1]
    lane = lax.broadcasted_iota(jnp.int32, (tokens, lanes), 1)
    row = lax.broadcasted_iota(jnp.int32, (tokens, lanes), 0)
    weight = weight_ref[...]
    mixing = weight / jnp.sum(weight, axis=1, keepdims=True)
    ids = ids_ref[...]
    hit = jnp.zeros((tokens, lanes), F32)
    share = jnp.zeros((tokens, lanes), F32)
    for k in range(topk):
        same = ids[:, k : k + 1] == lane // 8
        hit = jnp.where(same, 1.0, hit)
        share = jnp.where(same, mixing[:, k : k + 1], share)
    rank = jnp.zeros((tokens, lanes), F32)
    for t in range(tokens - 1):
        rank = rank + jnp.where(row > t, jnp.broadcast_to(hit[t : t + 1], (tokens, lanes)), 0.0)
    taken = jnp.where(rank == (lane % 2).astype(F32), hit, 0.0)
    share = share * taken
    own_low = (row < seq_count) == (core == 0)
    quarter = lane // 2 % 4
    for src in range(2):
        low = own_low if src == 0 else jnp.logical_not(own_low)
        chosen = jnp.where(low, taken, pltpu.roll(taken, seq_count, 0))
        shares = jnp.where(low, share, pltpu.roll(share, seq_count, 0))
        for kk in range(2):
            at = (src * 2 + kk) * tokens
            mine = quarter == kk * 2 + row // seq_count
            pick_ref[at : at + tokens, :] = jnp.where(mine, chosen, 0.0).astype(BF16)
            value = jnp.where(mine, shares, 0.0)
            coarse = value.astype(BF16)
            mix_ref[at : at + tokens, :] = coarse
            mix_ref[4 * tokens + at : 5 * tokens + at, :] = (value - coarse.astype(F32)).astype(BF16)


def route(expert_ids, route_weight, chips):
    tokens = expert_ids.shape[0]
    return kernel_call(
        route_body, (shape(4 * tokens, 8 * chips), shape(8 * tokens, 8 * chips)), [IN_VMEM] * 2, 4
    )(expert_ids, route_weight)


def dispatch_body(kept_ref, other_ref, pick_ref, out_hbm, held, sems):
    pieces = [r[...].reshape(-1, r.shape[2]) for r in (kept_ref, other_ref)]
    tokens = jnp.concatenate(pieces)
    chips, tile, half = held.shape
    step = chips // 2
    copies = []
    for j in range(2):
        rows = lax.dot_general(
            pick_ref[:, j * step * tile : (j + 1) * step * tile],
            tokens,
            (((0,), (0,)), ((), ())),
            preferred_element_type=F32,
        )
        sent = slice(j * step, (j + 1) * step)
        held[sent] = rows.astype(BF16).reshape(step, tile, half)
        copies.append(pltpu.make_async_copy(held.at[sent], out_hbm.at[sent], sems.at[j]))
        copies[-1].start()
    for copy in copies:
        copy.wait()


def dispatch(kept, other, pick):
    tile, half = kept.shape[1:]
    dims = pick.shape[1] // tile, tile, half
    return sending_call(dispatch_body, dims, [IN_VMEM] * 3, 6, 2)(kept, other, pick)


def slot_order(size, back=False):
    sorted_row = lax.broadcasted_iota(jnp.int32, (size, size), 1 if back else 0)
    row = lax.broadcasted_iota(jnp.int32, (size, size), 0 if back else 1)
    slot = sorted_row % (size // 4)
    quarter = sorted_row // (size // 4)
    return jnp.where(row == slot // 2 * 8 + quarter * 2 + slot % 2, 1.0, 0.0).astype(BF16)


def gate_body(x_ref, kept_ref, moved_ref, gate_hbm, up_hbm, part_ref, sent_ref, rest, sems):
    core = lax.axis_index(CORES)
    chips, tile, part = x_ref.shape
    half, both = moved_ref.shape
    units = both // 2
    count = kept_ref.shape[0]
    late = pl.ds(pl.multiple_of(core * half + count, part), half - count)
    pairs = (
        (gate_hbm.at[0, late, :], rest.at[:, :units]),
        (up_hbm.at[0, late, :], rest.at[:, units:]),
    )
    copies = [pltpu.make_async_copy(*pair, sems.at[j]) for j, pair in enumerate(pairs)]
    for copy in copies:
        copy.start()
    size = 256
    groups = chips * tile // size
    order = slot_order(size)
    slots = size // 4
    sorted_rows = []
    for g in range(groups):
        rows = x_ref[g * size // tile : (g + 1) * size // tile].reshape(size, part)
        sorted_rows.append(jnp.dot(order, rows, preferred_element_type=F32).astype(BF16))
    quarters = [
        jnp.concatenate([r[p * slots : (p + 1) * slots] for r in sorted_rows]) for p in range(4)
    ]
    x = jnp.concatenate(quarters, axis=1)
    other = jnp.dot(x, moved_ref[...], preferred_element_type=F32)
    part_ref[:, both:] = other
    sent_ref[:, :both] = other.astype(BF16)
    own = jnp.dot(x[:, :count], kept_ref[...], preferred_element_type=F32)
    for copy in copies:
        copy.wait()
    own = own + jnp.dot(x[:, count:], rest[...], preferred_element_type=F32)
    part_ref[:, :both] = own
    sent_ref[:, both:] = own.astype(BF16)


def gate_up(x, kept, moved, w_gate, w_up):
    chips, tile, _ = x.shape
    half, both = moved.shape
    dims = chips * tile // 4, 2 * both
    return pl.pallas_call(
        gate_body,
        name="gate_up",
        out_shape=[pltpu.VMEM(dims, F32), pltpu.VMEM(dims, BF16)],
        in_specs=[IN_VMEM] * 3 + [IN_HBM] * 2,
        out_specs=[IN_VMEM] * 2,
        scratch_shapes=[
            pltpu.VMEM((half - kept.shape[0], both), BF16),
            pltpu.SemaphoreType.DMA((2,)),
        ],
        compiler_params=pltpu.CompilerParams(vmem_limit_bytes=8 * MIB),
    )(x, in_vmem(kept), in_vmem(moved), in_hbm(w_gate), in_hbm(w_up))


def fetch_body(down_hbm, after_ref, out_ref, sem):
    del after_ref
    half = out_ref.shape[1]
    kept = pl.ds(pl.multiple_of(lax.axis_index(CORES) * half, half), half)
    copy = pltpu.make_async_copy(down_hbm.at[0, :, kept], out_ref, sem)
    copy.start()
    copy.wait()


def fetch_down(w_down, after):
    _, units, width = w_down.shape
    return pl.pallas_call(
        fetch_body,
        name="fetch_down",
        out_shape=pltpu.VMEM((units, width // 2), BF16),
        in_specs=[IN_HBM] * 2,
        out_specs=IN_VMEM,
        scratch_shapes=[pltpu.SemaphoreType.DMA],
        compiler_params=pltpu.CompilerParams(vmem_limit_bytes=MIB),
    )(in_hbm(w_down), after)


def down_body(part_ref, arrived_ref, first_ref, rest_ref, out_hbm, held, sems):
    chips, tile, part = held.shape
    size = 256
    groups = chips * tile // size
    order = slot_order(size, back=True)
    slots = size // 4
    units = first_ref.shape[0]

    def act(at):
        gate, up = (
            part_ref[:, j : j + units] + arrived_ref[:, j : j + units].astype(F32)
            for j in (at, at + units)
        )
        return (gate / (1.0 + jnp.exp(-gate)) * up).astype(BF16)

    hidden = act(0), act(2 * units)
    quarters = []
    for p in range(4):
        lanes = slice(p * part, (p + 1) * part)
        value = jnp.dot(hidden[0], first_ref[:, lanes], preferred_element_type=F32)
        value = value + jnp.dot(hidden[1], rest_ref[:, lanes], preferred_element_type=F32)
        quarters.append(value.astype(BF16))
    copies = []
    for g in range(groups):
        rows = jnp.concatenate([v[g * slots : (g + 1) * slots] for v in quarters])
        rows = jnp.dot(order, rows, preferred_element_type=F32).astype(BF16)
        sent = slice(g * size // tile, (g + 1) * size // tile)
        held[sent] = rows.reshape(size // tile, tile, part)
        copies.append(pltpu.make_async_copy(held.at[sent], out_hbm.at[sent], sems.at[g]))
        copies[-1].start()
    for copy in copies:
        copy.wait()


def down(part, arrived, first, rest, tile):
    dims = part.shape[0] * 4 // tile, tile, first.shape[1] // 4
    return sending_call(down_body, dims, [IN_VMEM] * 4, 8, 2)(
        part, arrived, in_vmem(first), in_vmem(rest)
    )


def combine_body(x_ref, mix_ref, own_ref, other_ref):
    x = x_ref[...].reshape(-1, x_ref.shape[2])
    rows = jnp.dot(mix_ref[...], x, preferred_element_type=F32)
    count = rows.shape[0] // 2
    rows = rows[:count] + rows[count:]
    own_ref[...] = rows[: count // 2].reshape(own_ref.shape)
    other_ref[...] = rows[count // 2 :].reshape(other_ref.shape)


def combine(x, mix):
    out = shape(2, x.shape[1], x.shape[2], dtype=F32)
    return kernel_call(combine_body, (out, out), [IN_VMEM] * 2, 4)(x, mix)


def finish_body(hidden_ref, own_ref, other_ref, out_ref, total):
    core = lax.axis_index(CORES)
    blocks, tile, half = hidden_ref.shape
    total[pl.ds(core * 2, 2)] = own_ref[...]
    total[pl.ds(2 - core * 2, 2)] = other_ref[...]
    for k in range(blocks):
        value = (hidden_ref[k] + total[k]).astype(BF16)
        for q in range(2):
            at = (2 * k + q) * half
            out_ref[:, at : at + half] = value[q * tile // 2 : (q + 1) * tile // 2]


def finish(hidden, own, other):
    blocks, tile, half = hidden.shape
    return kernel_call(
        finish_body, shape(tile // 2, 2 * blocks * half), [IN_VMEM] * 3, 2, [pltpu.VMEM(hidden.shape, F32)]
    )(hidden, own, other)


def on_device(
    queries,
    token_keys,
    token_values,
    stored_keys,
    stored_values,
    kv_len,
    residual,
    out_weight,
    norm_gain,
    expert_ids,
    route_weight,
    w_gate,
    w_up,
    w_down,
):
    chips = lax.axis_size(CHIPS)
    side = math.isqrt(chips)
    outgoing, *pieces = attend(
        queries, token_keys, token_values, kv_len, stored_keys, stored_values, out_weight
    )
    own = pieces[:1] + [
        lax.ppermute(piece, CHIPS, square_step(side, way))
        for piece, way in zip(pieces[1:], (1, -1, 0), strict=True)
    ]
    tokens = lax.all_to_all(outgoing, CHIPS, 0, 0, tiled=True)
    other = [swapped(piece) for piece in own]
    weight = stack(own, other)
    kept, gate_given, down_given = halves(w_gate, w_up, w_down, 0.75)
    gate_moved, down_moved = swapped(gate_given), swapped(down_given)
    pick, mix = route(expert_ids, route_weight, chips)

    sums = project(tokens, weight)
    came_back = lax.all_to_all(sums, CHIPS, 0, 0, tiled=True)
    hidden, normed, normed_given = settle(came_back, residual, norm_gain[None])
    normed_other = swapped(normed_given)
    outgoing = dispatch(normed, normed_other, pick)
    incoming = lax.all_to_all(outgoing, CHIPS, 0, 0, tiled=True)
    part, sent = gate_up(incoming, kept, gate_moved, w_gate, w_up)
    down_kept = fetch_down(w_down, part)
    expert_out = down(part, swapped(sent), down_kept, down_moved, incoming.shape[1])
    returned = lax.all_to_all(expert_out, CHIPS, 0, 0, tiled=True)
    moe_own, moe_given = combine(returned, mix)
    return finish(hidden, moe_own, swapped(moe_given))


def solution(mesh):
    in_specs = (
        P(("groups", "expert", "replica"), None),
        P(("groups", "expert", "replica"), None),
        P(("groups", "expert", "replica"), None),
        P(("groups", "expert", "replica"), None, None),
        P(("groups", "expert", "replica"), None, None),
        P(("groups", "expert", "replica")),
        P(("groups", "expert", "replica"), None),
        P(("expert", "replica"), None),
        P(),
        P(("groups", "expert"), None),
        P(("groups", "expert"), None),
        P("expert", None, "replica"),
        P("expert", None, "replica"),
        P("expert", "replica", None),
    )
    out_specs = P(("groups", "expert", "replica"), None)
    return jax.shard_map(
        on_device, mesh=mesh, in_specs=in_specs, out_specs=out_specs, check_vma=False
    )
```

```python
import math

import jax
import jax.numpy as jnp
from jax import lax
from jax.experimental import pallas as pl
from jax.experimental.pallas import tpu as pltpu
from jax.sharding import PartitionSpec as P

HEAD_WIDTH = 128
CHIPS, CORES = "expert", "replica"
F32, BF16 = jnp.float32, jnp.bfloat16
IN_VMEM = pl.BlockSpec(memory_space=pltpu.VMEM)
IN_SMEM = pl.BlockSpec(memory_space=pltpu.SMEM)
IN_HBM = pl.BlockSpec(memory_space=pltpu.HBM)


def swapped(x):
    return lax.ppermute(x, CORES, [(0, 1), (1, 0)])


def square_place(chip, side):
    x, y = chip // side % 2, chip % 2
    return x * 2 + y, 1 + (x ^ y)


def square_step(side, way):
    steps = []
    for x in range(side):
        for y in range(side):
            along_y = {1: (x ^ y) & 1 == 0, -1: (x ^ y) & 1 == 1}.get(way)
            dx, dy = (1, 1) if way == 0 else ((0, 1) if along_y else (1, 0))
            steps.append((x * side + y, (x ^ dx) * side + (y ^ dy)))
    return steps


MIB = 1 << 20


def in_hbm(x):
    return pltpu.with_memory_space_constraint(x, pltpu.HBM)


def in_vmem(x):
    return pltpu.with_memory_space_constraint(x, pltpu.VMEM)


def kernel_call(body, outs, in_specs, limit, scratch=()):
    return pl.pallas_call(
        body,
        out_shape=outs,
        in_specs=in_specs,
        out_specs=jax.tree.map(lambda _: IN_VMEM, outs),
        scratch_shapes=list(scratch),
        compiler_params=pltpu.CompilerParams(vmem_limit_bytes=limit * MIB),
    )


def shape(*dims, dtype=BF16):
    return jax.ShapeDtypeStruct(dims, dtype)


def attend_body(
    q_hbm,
    tk_hbm,
    tv_hbm,
    len_hbm,
    keys_hbm,
    values_hbm,
    weight_hbm,
    out_hbm,
    piece_own,
    piece_next,
    piece_last,
    piece_diagonal,
    q_ref,
    tk_ref,
    tv_ref,
    len_ref,
    keys,
    values,
    pieces,
    rows,
    mixed,
    scored,
    out_ref,
    sems,
    few,
):
    core = lax.axis_index(CORES)
    seq_count, cache_len, kv_width = keys_hbm.shape
    kv_count = kv_width // HEAD_WIDTH
    head_count = q_hbm.shape[1] // HEAD_WIDTH
    group = head_count // kv_count
    side = group // 2
    small = [
        pltpu.make_async_copy(source, target, few.at[j])
        for j, (source, target) in enumerate(
            ((q_hbm, q_ref), (tk_hbm, tk_ref), (tv_hbm, tv_ref), (len_hbm, len_ref))
        )
    ]
    for copy in small:
        copy.start()
    copies = [
        [pltpu.make_async_copy(source.at[b], target.at[b], sems.at[j, b]) for b in range(seq_count)]
        for j, (source, target) in enumerate(((keys_hbm, keys), (values_hbm, values)))
    ]
    for copy in copies[0] + copies[1]:
        copy.start()
    chip = lax.axis_index(CHIPS)
    place, ahead = square_place(chip, side)
    sliced, stored = [], []
    for j, (d, piece) in enumerate(
        ((0, piece_own), (ahead, piece_next), (3 - ahead, piece_last), (3, piece_diagonal))
    ):
        cols = piece.shape[1]
        at = pl.multiple_of((place ^ d) * cols, cols)
        source = weight_hbm.at[:, pl.ds(at, cols)]
        sliced.append(pltpu.make_async_copy(source, pieces.at[j], few.at[len(small) + j]))
        stored.append(pltpu.make_async_copy(pieces.at[j], piece, few.at[len(small) + 4 + j]))
        sliced[-1].start()
    for copy in small:
        copy.wait()
    for h in range(head_count):
        piece = q_ref[:, h * HEAD_WIDTH : (h + 1) * HEAD_WIDTH].astype(F32)
        rows[pl.ds(h, seq_count, stride=head_count), :] = piece
    inv_root = 1.0 / math.sqrt(HEAD_WIDTH)
    positions = lax.broadcasted_iota(jnp.int32, (head_count, cache_len), 1)
    lanes = [slice(g * HEAD_WIDTH, (g + 1) * HEAD_WIDTH) for g in range(kv_count)]
    fresh = []
    for copy in copies[0]:
        copy.wait()
    for b in range(seq_count):
        query = rows[b * head_count : (b + 1) * head_count, :]
        latest = [tk_ref[b : b + 1, lanes[g]].astype(F32) for g in range(kv_count)]
        latest = jnp.concatenate([jnp.broadcast_to(v, (group, HEAD_WIDTH)) for v in latest])
        fresh.append(jnp.sum(query * latest, axis=1, keepdims=True) * inv_root)
        query = query.astype(BF16)
        for g in range(kv_count):
            at = b * head_count + g * group
            scored[at : at + group, :] = lax.dot_general(
                query[g * group : (g + 1) * group],
                keys[b, :, lanes[g]],
                (((1,), (1,)), ((), ())),
                preferred_element_type=F32,
            )
    for copy in copies[1] + sliced:
        copy.wait()
    for copy in stored:
        copy.start()
    probs, fresh_probs = [], []
    for b in range(seq_count):
        scores = scored[b * head_count : (b + 1) * head_count, :]
        scores = jnp.where(positions < len_ref[b], scores * inv_root, -jnp.inf)
        highest = jnp.maximum(jnp.max(scores, axis=1, keepdims=True), fresh[b])
        cached_exp = jnp.exp(scores - highest)
        fresh_exp = jnp.exp(fresh[b] - highest)
        share = 1.0 / (jnp.sum(cached_exp, axis=1, keepdims=True) + fresh_exp)
        probs.append((cached_exp * share).astype(BF16))
        fresh_probs.append((fresh_exp * share).astype(BF16).astype(F32))
    for b in range(seq_count):
        for g in range(kv_count):
            heads = slice(g * group, (g + 1) * group)
            out = jnp.dot(probs[b][heads], values[b, :, lanes[g]], preferred_element_type=F32)
            out = out + fresh_probs[b][heads] * tv_ref[b : b + 1, lanes[g]].astype(F32)
            out = pltpu.roll(out, core * (HEAD_WIDTH // 2), 1)
            for a in range(2):
                start = g * group * seq_count + a * seq_count + b
                mixed[pl.ds(start, side, stride=2 * seq_count), :] = out[a * side : (a + 1) * side]
    tile = 2 * seq_count
    for g in range(kv_count):
        for y in range(side):
            for part, source in enumerate((y, y ^ 1)):
                at = (g * side + source) * tile
                near = mixed[at : at + tile, :]
                far = pltpu.roll(near, seq_count, 0)
                out_ref[2 * g * side + y, :, lanes[part]] = near.astype(BF16)
                out_ref[(2 * g + 1) * side + y, :, lanes[part]] = far.astype(BF16)
        sent = pl.ds(2 * g * side, 2 * side)
        stored.append(
            pltpu.make_async_copy(out_ref.at[sent], out_hbm.at[sent], few.at[len(small) + 8 + g])
        )
        stored[-1].start()
    for copy in stored:
        copy.wait()


def attend(queries, token_keys, token_values, kv_len, stored_keys, stored_values, out_weight):
    seq_count, feature_total = queries.shape
    heads = feature_total // HEAD_WIDTH
    rows, cols = out_weight.shape
    return pl.pallas_call(
        attend_body,
        name="attend",
        out_shape=[pltpu.HBM((heads, 2 * seq_count, 2 * HEAD_WIDTH), BF16)]
        + [pltpu.HBM((rows, cols // 4), BF16)] * 4,
        in_specs=[IN_HBM] * 7,
        out_specs=[IN_HBM] * 5,
        scratch_shapes=[
            pltpu.VMEM(queries.shape, BF16),
            pltpu.VMEM(token_keys.shape, BF16),
            pltpu.VMEM(token_values.shape, BF16),
            pltpu.SMEM(kv_len.shape, jnp.int32),
            pltpu.VMEM(stored_keys.shape, BF16),
            pltpu.VMEM(stored_values.shape, BF16),
            pltpu.VMEM((4, rows, cols // 4), BF16),
            pltpu.VMEM((seq_count * heads, HEAD_WIDTH), F32),
            pltpu.VMEM((seq_count * heads, HEAD_WIDTH), F32),
            pltpu.VMEM((seq_count * heads, stored_keys.shape[1]), F32),
            pltpu.VMEM((heads, 2 * seq_count, 2 * HEAD_WIDTH), BF16),
            pltpu.SemaphoreType.DMA((2, seq_count)),
            pltpu.SemaphoreType.DMA((16,)),
        ],
        compiler_params=pltpu.CompilerParams(vmem_limit_bytes=8 * MIB),
    )(
        *map(
            in_hbm,
            (queries, token_keys, token_values, kv_len, stored_keys, stored_values, out_weight),
        )
    )


def copy_all(pairs, sems):
    copies = [pltpu.make_async_copy(*pair, sems.at[j]) for j, pair in enumerate(pairs)]
    for copy in copies:
        copy.start()
    for copy in copies:
        copy.wait()


def stack_body(*refs):
    own, other, out_ref, sems = refs[:4], refs[4:8], refs[8], refs[9]
    rows = own[0].shape[0]
    side = math.isqrt(lax.axis_size(CHIPS))
    _, ahead = square_place(lax.axis_index(CHIPS), side)
    pairs = []
    for j, d in enumerate((0, 3 - ahead, ahead, 3)):
        for half, source in enumerate((own[j], other[j])):
            at = pl.multiple_of((2 * d + half) * rows, rows)
            pairs.append((source, out_ref.at[pl.ds(at, rows)]))
    copy_all(pairs, sems)


def stack(own, other):
    rows, cols = own[0].shape
    return pl.pallas_call(
        stack_body,
        name="stack",
        out_shape=pltpu.VMEM((8 * rows, cols), BF16),
        in_specs=[IN_HBM] * 8,
        out_specs=IN_VMEM,
        scratch_shapes=[pltpu.SemaphoreType.DMA((8,))],
        compiler_params=pltpu.CompilerParams(vmem_limit_bytes=2 * MIB),
    )(*map(in_hbm, own), *map(in_hbm, other))


def halves_body(gate_hbm, up_hbm, down_hbm, kept_ref, *refs):
    outs, (tall, wide, sems) = refs[:2], refs[2:]
    core = lax.axis_index(CORES)
    count = kept_ref.shape[0]
    half, both = tall.shape
    units = both // 2
    given = pl.ds(pl.multiple_of((1 - core) * half, half), half)
    kept = pl.ds(pl.multiple_of(core * half, half), count)
    left, right = slice(0, units), slice(units, both)
    pairs = (
        (gate_hbm.at[0, given, :], tall.at[:, left]),
        (up_hbm.at[0, given, :], tall.at[:, right]),
        (down_hbm.at[0, :, given], wide),
        (gate_hbm.at[0, kept, :], kept_ref.at[:, left]),
        (up_hbm.at[0, kept, :], kept_ref.at[:, right]),
        (tall, outs[0]),
        (wide, outs[1]),
    )
    copies = [pltpu.make_async_copy(*pair, sems.at[j]) for j, pair in enumerate(pairs)]
    for copy in copies[:5]:
        copy.start()
    for copy in copies[:2]:
        copy.wait()
    copies[5].start()
    copies[2].wait()
    copies[6].start()
    for copy in copies[3:]:
        copy.wait()


def halves(w_gate, w_up, w_down, kept_share):
    _, width, units = w_gate.shape
    tall, wide = (width // 2, 2 * units), (units, width // 2)
    return pl.pallas_call(
        halves_body,
        name="halves",
        out_shape=[
            pltpu.VMEM((int(width // 2 * kept_share), 2 * units), BF16),
            pltpu.HBM(tall, BF16),
            pltpu.HBM(wide, BF16),
        ],
        in_specs=[IN_HBM] * 3,
        out_specs=[IN_VMEM] + [IN_HBM] * 2,
        scratch_shapes=[
            pltpu.VMEM(tall, BF16),
            pltpu.VMEM(wide, BF16),
            pltpu.SemaphoreType.DMA((7,)),
        ],
        compiler_params=pltpu.CompilerParams(vmem_limit_bytes=6 * MIB),
    )(*map(in_hbm, (w_gate, w_up, w_down)))


def project_body(x_ref, weight_ref, out_hbm, held, sems):
    chips, tile, width = x_ref.shape
    cols = weight_ref.shape[1]
    half = cols // 2
    step = chips // 2

    def paired(first, second):
        low = lax.broadcasted_iota(jnp.int32, first.shape, 1) < tile // 2
        return (
            jnp.where(low, first, pltpu.roll(second, tile // 2, 1)),
            jnp.where(low, pltpu.roll(first, tile // 2, 1), second),
        )

    copies = []
    for j in range(2):
        sent = slice(j * step, (j + 1) * step)
        x = x_ref[sent].astype(F32).reshape(step // 2, 2, tile, width)
        x = jnp.concatenate(paired(x[:, 0], x[:, 1]), axis=2)
        x = x.reshape(step // 2 * tile, 2 * width).astype(BF16)
        sums = jnp.dot(x, weight_ref[...], preferred_element_type=F32)
        sums = sums.reshape(step // 2, tile, cols)
        sums = jnp.stack(paired(sums[:, :, :half], sums[:, :, half:]), axis=1)
        held[sent] = sums.reshape(step, tile, half).astype(BF16)
        copies.append(pltpu.make_async_copy(held.at[sent], out_hbm.at[sent], sems.at[j]))
        copies[-1].start()
    for copy in copies:
        copy.wait()


def sending_call(body, dims, in_specs, limit, chunks):
    return pl.pallas_call(
        body,
        out_shape=pltpu.HBM(dims, BF16),
        in_specs=in_specs,
        out_specs=IN_HBM,
        scratch_shapes=[pltpu.VMEM(dims, BF16), pltpu.SemaphoreType.DMA((chunks,))],
        compiler_params=pltpu.CompilerParams(vmem_limit_bytes=limit * MIB),
    )


def project(x, weight):
    dims = x.shape[0], x.shape[1], weight.shape[1] // 2
    return sending_call(project_body, dims, [IN_VMEM] * 2, 12, 2)(
        x, in_vmem(weight)
    )


def settle_body(x_ref, residual_ref, gain_ref, hidden_ref, kept_ref, given_ref, normed):
    core = lax.axis_index(CORES)
    chips, tile, half = x_ref.shape
    side = math.isqrt(chips)
    blocks = 4
    seq_count = tile // 2
    width = residual_ref.shape[1]

    def rows_of(ref, k):
        low, high = (ref[:, (2 * k + q) * half : (2 * k + q + 1) * half].astype(F32) for q in (0, 1))
        low, high = (jnp.broadcast_to(v, (seq_count, half)) for v in (low, high))
        return jnp.concatenate([low, high])

    square = jnp.zeros((tile, 1), F32)
    for k in range(blocks):
        total = rows_of(residual_ref, k)
        for x in range(k // 2, side, 2):
            for y in range(k % 2, side, 2):
                total = total + x_ref[x * side + y].astype(F32)
        hidden_ref[k] = total
        square = square + jnp.sum(total * total, axis=1, keepdims=True)
    square = jnp.broadcast_to(square, (tile, HEAD_WIDTH))
    square = square + pltpu.roll(square, seq_count, 0)
    scale = lax.rsqrt(square[:, :1] / width + 1e-06)
    for k in range(blocks):
        normed[k] = (hidden_ref[k] * scale * rows_of(gain_ref, k)).astype(BF16)
    kept_ref[...] = normed[pl.ds(core * 2, 2)]
    given_ref[...] = normed[pl.ds(2 - core * 2, 2)]


def settle(x, residual, gain):
    tile, half = x.shape[1:]
    return kernel_call(
        settle_body,
        (shape(4, tile, half, dtype=F32), shape(2, tile, half), shape(2, tile, half)),
        [IN_VMEM] * 3,
        6,
        [pltpu.VMEM((4, tile, half), BF16)],
    )(x, residual, gain)


def route_body(ids_ref, weight_ref, pick_ref, mix_ref):
    core = lax.axis_index(CORES)
    tokens, topk = ids_ref.shape
    seq_count = tokens // 2
    lanes = pick_ref.shape[1]
    lane = lax.broadcasted_iota(jnp.int32, (tokens, lanes), 1)
    row = lax.broadcasted_iota(jnp.int32, (tokens, lanes), 0)
    weight = weight_ref[...]
    mixing = weight / jnp.sum(weight, axis=1, keepdims=True)
    ids = ids_ref[...]
    hit = jnp.zeros((tokens, lanes), F32)
    share = jnp.zeros((tokens, lanes), F32)
    for k in range(topk):
        same = ids[:, k : k + 1] == lane // 8
        hit = jnp.where(same, 1.0, hit)
        share = jnp.where(same, mixing[:, k : k + 1], share)
    rank = jnp.zeros((tokens, lanes), F32)
    for t in range(tokens - 1):
        rank = rank + jnp.where(row > t, jnp.broadcast_to(hit[t : t + 1], (tokens, lanes)), 0.0)
    taken = jnp.where(rank == (lane % 2).astype(F32), hit, 0.0)
    share = share * taken
    own_low = (row < seq_count) == (core == 0)
    quarter = lane // 2 % 4
    for src in range(2):
        low = own_low if src == 0 else jnp.logical_not(own_low)
        chosen = jnp.where(low, taken, pltpu.roll(taken, seq_count, 0))
        shares = jnp.where(low, share, pltpu.roll(share, seq_count, 0))
        for kk in range(2):
            at = (src * 2 + kk) * tokens
            mine = quarter == kk * 2 + row // seq_count
            pick_ref[at : at + tokens, :] = jnp.where(mine, chosen, 0.0).astype(BF16)
            value = jnp.where(mine, shares, 0.0)
            coarse = value.astype(BF16)
            mix_ref[at : at + tokens, :] = coarse
            mix_ref[4 * tokens + at : 5 * tokens + at, :] = (value - coarse.astype(F32)).astype(BF16)


def route(expert_ids, route_weight, chips):
    tokens = expert_ids.shape[0]
    return kernel_call(
        route_body, (shape(4 * tokens, 8 * chips), shape(8 * tokens, 8 * chips)), [IN_VMEM] * 2, 4
    )(expert_ids, route_weight)


def dispatch_body(kept_ref, other_ref, pick_ref, gate_hbm, up_hbm, out_hbm, rest_ref, held, sems):
    count, both = rest_ref.shape
    units = both // 2
    half = gate_hbm.shape[1] // 2
    end = (lax.axis_index(CORES) + 1) * half
    late = pl.ds(pl.multiple_of(end - count, count), count)
    copies = [
        pltpu.make_async_copy(gate_hbm.at[0, late, :], rest_ref.at[:, :units], sems.at[2]),
        pltpu.make_async_copy(up_hbm.at[0, late, :], rest_ref.at[:, units:], sems.at[3]),
    ]
    for copy in copies:
        copy.start()
    pieces = [r[...].reshape(-1, r.shape[2]) for r in (kept_ref, other_ref)]
    tokens = jnp.concatenate(pieces)
    chips, tile, part = held.shape
    step = chips // 2
    for j in range(2):
        rows = lax.dot_general(
            pick_ref[:, j * step * tile : (j + 1) * step * tile],
            tokens,
            (((0,), (0,)), ((), ())),
            preferred_element_type=F32,
        )
        sent = slice(j * step, (j + 1) * step)
        held[sent] = rows.astype(BF16).reshape(step, tile, part)
        copies.append(pltpu.make_async_copy(held.at[sent], out_hbm.at[sent], sems.at[j]))
        copies[-1].start()
    for copy in copies:
        copy.wait()


def dispatch(kept, other, pick, w_gate, w_up, late):
    tile, part = kept.shape[1:]
    dims = pick.shape[1] // tile, tile, part
    return pl.pallas_call(
        dispatch_body,
        name="dispatch",
        out_shape=[pltpu.HBM(dims, BF16), pltpu.VMEM((late, 2 * w_gate.shape[2]), BF16)],
        in_specs=[IN_VMEM] * 3 + [IN_HBM] * 2,
        out_specs=[IN_HBM, IN_VMEM],
        scratch_shapes=[pltpu.VMEM(dims, BF16), pltpu.SemaphoreType.DMA((4,))],
        compiler_params=pltpu.CompilerParams(vmem_limit_bytes=6 * MIB),
    )(kept, other, pick, in_hbm(w_gate), in_hbm(w_up))


def slot_order(size, back=False):
    sorted_row = lax.broadcasted_iota(jnp.int32, (size, size), 1 if back else 0)
    row = lax.broadcasted_iota(jnp.int32, (size, size), 0 if back else 1)
    slot = sorted_row % (size // 4)
    quarter = sorted_row // (size // 4)
    return jnp.where(row == slot // 2 * 8 + quarter * 2 + slot % 2, 1.0, 0.0).astype(BF16)


def gate_body(x_ref, kept_ref, rest_ref, moved_ref, part_ref, sent_ref):
    chips, tile, part = x_ref.shape
    count, both = kept_ref.shape
    size = 256
    groups = chips * tile // size
    order = slot_order(size)
    slots = size // 4
    sorted_rows = []
    for g in range(groups):
        rows = x_ref[g * size // tile : (g + 1) * size // tile].reshape(size, part)
        sorted_rows.append(jnp.dot(order, rows, preferred_element_type=F32).astype(BF16))
    quarters = [
        jnp.concatenate([r[p * slots : (p + 1) * slots] for r in sorted_rows]) for p in range(4)
    ]
    x = jnp.concatenate(quarters, axis=1)
    own = jnp.dot(x[:, :count], kept_ref[...], preferred_element_type=F32)
    own = own + jnp.dot(x[:, count:], rest_ref[...], preferred_element_type=F32)
    part_ref[:, :both] = own
    sent_ref[:, both:] = own.astype(BF16)
    other = jnp.dot(x, moved_ref[...], preferred_element_type=F32)
    part_ref[:, both:] = other
    sent_ref[:, :both] = other.astype(BF16)


def gate_up(x, kept, rest, moved):
    chips, tile, _ = x.shape
    dims = chips * tile // 4, 2 * kept.shape[1]
    return pl.pallas_call(
        gate_body,
        name="gate_up",
        out_shape=[pltpu.VMEM(dims, F32), pltpu.VMEM(dims, BF16)],
        in_specs=[IN_VMEM] * 4,
        out_specs=[IN_VMEM] * 2,
        compiler_params=pltpu.CompilerParams(vmem_limit_bytes=6 * MIB),
    )(x, in_vmem(kept), in_vmem(rest), in_vmem(moved))


def fetch_body(down_hbm, after_ref, out_ref, sem):
    del after_ref
    half = out_ref.shape[1]
    kept = pl.ds(pl.multiple_of(lax.axis_index(CORES) * half, half), half)
    copy = pltpu.make_async_copy(down_hbm.at[0, :, kept], out_ref, sem)
    copy.start()
    copy.wait()


def fetch_down(w_down, after):
    _, units, width = w_down.shape
    return pl.pallas_call(
        fetch_body,
        name="fetch_down",
        out_shape=pltpu.VMEM((units, width // 2), BF16),
        in_specs=[IN_HBM] * 2,
        out_specs=IN_VMEM,
        scratch_shapes=[pltpu.SemaphoreType.DMA],
        compiler_params=pltpu.CompilerParams(vmem_limit_bytes=MIB),
    )(in_hbm(w_down), after)


def down_body(part_ref, arrived_ref, first_ref, rest_ref, out_hbm, held, sems):
    chips, tile, part = held.shape
    size = 256
    groups = chips * tile // size
    order = slot_order(size, back=True)
    slots = size // 4
    units = first_ref.shape[0]

    def act(at):
        gate, up = (
            part_ref[:, j : j + units] + arrived_ref[:, j : j + units].astype(F32)
            for j in (at, at + units)
        )
        return (gate / (1.0 + jnp.exp(-gate)) * up).astype(BF16)

    hidden = act(0), act(2 * units)
    quarters = []
    for p in range(4):
        lanes = slice(p * part, (p + 1) * part)
        value = jnp.dot(hidden[0], first_ref[:, lanes], preferred_element_type=F32)
        value = value + jnp.dot(hidden[1], rest_ref[:, lanes], preferred_element_type=F32)
        quarters.append(value.astype(BF16))
    copies = []
    for g in range(groups):
        rows = jnp.concatenate([v[g * slots : (g + 1) * slots] for v in quarters])
        rows = jnp.dot(order, rows, preferred_element_type=F32).astype(BF16)
        sent = slice(g * size // tile, (g + 1) * size // tile)
        held[sent] = rows.reshape(size // tile, tile, part)
        copies.append(pltpu.make_async_copy(held.at[sent], out_hbm.at[sent], sems.at[g]))
        copies[-1].start()
    for copy in copies:
        copy.wait()


def down(part, arrived, first, rest, tile):
    dims = part.shape[0] * 4 // tile, tile, first.shape[1] // 4
    return sending_call(down_body, dims, [IN_VMEM] * 4, 8, 2)(
        part, arrived, in_vmem(first), in_vmem(rest)
    )


def combine_body(x_ref, mix_ref, own_ref, other_ref):
    x = x_ref[...].reshape(-1, x_ref.shape[2])
    rows = jnp.dot(mix_ref[...], x, preferred_element_type=F32)
    count = rows.shape[0] // 2
    rows = rows[:count] + rows[count:]
    own_ref[...] = rows[: count // 2].reshape(own_ref.shape)
    other_ref[...] = rows[count // 2 :].reshape(other_ref.shape)


def combine(x, mix):
    out = shape(2, x.shape[1], x.shape[2], dtype=F32)
    return kernel_call(combine_body, (out, out), [IN_VMEM] * 2, 4)(x, mix)


def finish_body(hidden_ref, own_ref, other_ref, out_ref, total):
    core = lax.axis_index(CORES)
    blocks, tile, half = hidden_ref.shape
    total[pl.ds(core * 2, 2)] = own_ref[...]
    total[pl.ds(2 - core * 2, 2)] = other_ref[...]
    for k in range(blocks):
        value = (hidden_ref[k] + total[k]).astype(BF16)
        for q in range(2):
            at = (2 * k + q) * half
            out_ref[:, at : at + half] = value[q * tile // 2 : (q + 1) * tile // 2]


def finish(hidden, own, other):
    blocks, tile, half = hidden.shape
    return kernel_call(
        finish_body, shape(tile // 2, 2 * blocks * half), [IN_VMEM] * 3, 2, [pltpu.VMEM(hidden.shape, F32)]
    )(hidden, own, other)


def on_device(
    queries,
    token_keys,
    token_values,
    stored_keys,
    stored_values,
    kv_len,
    residual,
    out_weight,
    norm_gain,
    expert_ids,
    route_weight,
    w_gate,
    w_up,
    w_down,
):
    chips = lax.axis_size(CHIPS)
    side = math.isqrt(chips)
    outgoing, *pieces = attend(
        queries, token_keys, token_values, kv_len, stored_keys, stored_values, out_weight
    )
    own = pieces[:1] + [
        lax.ppermute(piece, CHIPS, square_step(side, way))
        for piece, way in zip(pieces[1:], (1, -1, 0), strict=True)
    ]
    tokens = lax.all_to_all(outgoing, CHIPS, 0, 0, tiled=True)
    other = [swapped(piece) for piece in own]
    weight = stack(own, other)
    kept, gate_given, down_given = halves(w_gate, w_up, w_down, 0.75)
    gate_moved, down_moved = swapped(gate_given), swapped(down_given)
    pick, mix = route(expert_ids, route_weight, chips)

    sums = project(tokens, weight)
    came_back = lax.all_to_all(sums, CHIPS, 0, 0, tiled=True)
    hidden, normed, normed_given = settle(came_back, residual, norm_gain[None])
    normed_other = swapped(normed_given)
    late = w_gate.shape[1] // 2 - kept.shape[0]
    outgoing, rest = dispatch(normed, normed_other, pick, w_gate, w_up, late)
    incoming = lax.all_to_all(outgoing, CHIPS, 0, 0, tiled=True)
    part, sent = gate_up(incoming, kept, rest, gate_moved)
    down_kept = fetch_down(w_down, part)
    expert_out = down(part, swapped(sent), down_kept, down_moved, incoming.shape[1])
    returned = lax.all_to_all(expert_out, CHIPS, 0, 0, tiled=True)
    moe_own, moe_given = combine(returned, mix)
    return finish(hidden, moe_own, swapped(moe_given))


def solution(mesh):
    in_specs = (
        P(("groups", "expert", "replica"), None),
        P(("groups", "expert", "replica"), None),
        P(("groups", "expert", "replica"), None),
        P(("groups", "expert", "replica"), None, None),
        P(("groups", "expert", "replica"), None, None),
        P(("groups", "expert", "replica")),
        P(("groups", "expert", "replica"), None),
        P(("expert", "replica"), None),
        P(),
        P(("groups", "expert"), None),
        P(("groups", "expert"), None),
        P("expert", None, "replica"),
        P("expert", None, "replica"),
        P("expert", "replica", None),
    )
    out_specs = P(("groups", "expert", "replica"), None)
    return jax.shard_map(
        on_device, mesh=mesh, in_specs=in_specs, out_specs=out_specs, check_vma=False
    )
```

```python
import math

import jax
import jax.numpy as jnp
from jax import lax
from jax.experimental import pallas as pl
from jax.experimental.pallas import tpu as pltpu
from jax.sharding import PartitionSpec as P

HEAD_WIDTH = 128
CHIPS, CORES = "expert", "replica"
F32, BF16 = jnp.float32, jnp.bfloat16
IN_VMEM = pl.BlockSpec(memory_space=pltpu.VMEM)
IN_SMEM = pl.BlockSpec(memory_space=pltpu.SMEM)
IN_HBM = pl.BlockSpec(memory_space=pltpu.HBM)


def swapped(x):
    return lax.ppermute(x, CORES, [(0, 1), (1, 0)])


def square_place(chip, side):
    x, y = chip // side % 2, chip % 2
    return x * 2 + y, 1 + (x ^ y)


def square_step(side, way):
    steps = []
    for x in range(side):
        for y in range(side):
            along_y = {1: (x ^ y) & 1 == 0, -1: (x ^ y) & 1 == 1}.get(way)
            dx, dy = (1, 1) if way == 0 else ((0, 1) if along_y else (1, 0))
            steps.append((x * side + y, (x ^ dx) * side + (y ^ dy)))
    return steps


def first_member(chips):
    return chips - 2


def exchanged(x):
    chips = lax.axis_size(CHIPS)
    members = [(k + first_member(chips)) % chips for k in range(chips)]
    return lax.all_to_all(x, CHIPS, 0, 0, tiled=True, axis_index_groups=[members])


MIB = 1 << 20


def in_hbm(x):
    return pltpu.with_memory_space_constraint(x, pltpu.HBM)


def in_vmem(x):
    return pltpu.with_memory_space_constraint(x, pltpu.VMEM)


def kernel_call(body, outs, in_specs, limit, scratch=()):
    return pl.pallas_call(
        body,
        out_shape=outs,
        in_specs=in_specs,
        out_specs=jax.tree.map(lambda _: IN_VMEM, outs),
        scratch_shapes=list(scratch),
        compiler_params=pltpu.CompilerParams(vmem_limit_bytes=limit * MIB),
    )


def shape(*dims, dtype=BF16):
    return jax.ShapeDtypeStruct(dims, dtype)


def attend_body(
    q_hbm,
    tk_hbm,
    tv_hbm,
    len_hbm,
    keys_hbm,
    values_hbm,
    weight_hbm,
    out_hbm,
    piece_own,
    piece_next,
    piece_last,
    piece_diagonal,
    q_ref,
    tk_ref,
    tv_ref,
    len_ref,
    keys,
    values,
    pieces,
    rows,
    mixed,
    scored,
    out_ref,
    sems,
    few,
):
    core = lax.axis_index(CORES)
    seq_count, cache_len, kv_width = keys_hbm.shape
    kv_count = kv_width // HEAD_WIDTH
    head_count = q_hbm.shape[1] // HEAD_WIDTH
    group = head_count // kv_count
    side = group // 2
    small = [
        pltpu.make_async_copy(source, target, few.at[j])
        for j, (source, target) in enumerate(
            ((q_hbm, q_ref), (tk_hbm, tk_ref), (tv_hbm, tv_ref), (len_hbm, len_ref))
        )
    ]
    for copy in small:
        copy.start()
    copies = [
        [pltpu.make_async_copy(source.at[b], target.at[b], sems.at[j, b]) for b in range(seq_count)]
        for j, (source, target) in enumerate(((keys_hbm, keys), (values_hbm, values)))
    ]
    for copy in copies[0] + copies[1]:
        copy.start()
    chip = lax.axis_index(CHIPS)
    place, ahead = square_place(chip, side)
    sliced, stored = [], []
    for j, (d, piece) in enumerate(
        ((0, piece_own), (ahead, piece_next), (3 - ahead, piece_last), (3, piece_diagonal))
    ):
        cols = piece.shape[1]
        at = pl.multiple_of((place ^ d) * cols, cols)
        source = weight_hbm.at[:, pl.ds(at, cols)]
        sliced.append(pltpu.make_async_copy(source, pieces.at[j], few.at[len(small) + j]))
        stored.append(pltpu.make_async_copy(pieces.at[j], piece, few.at[len(small) + 4 + j]))
        sliced[-1].start()
    for copy in small:
        copy.wait()
    for h in range(head_count):
        piece = q_ref[:, h * HEAD_WIDTH : (h + 1) * HEAD_WIDTH].astype(F32)
        rows[pl.ds(h, seq_count, stride=head_count), :] = piece
    inv_root = 1.0 / math.sqrt(HEAD_WIDTH)
    positions = lax.broadcasted_iota(jnp.int32, (head_count, cache_len), 1)
    lanes = [slice(g * HEAD_WIDTH, (g + 1) * HEAD_WIDTH) for g in range(kv_count)]
    fresh, probs, fresh_probs = {}, {}, {}

    def score(b):
        query = rows[b * head_count : (b + 1) * head_count, :]
        latest = [tk_ref[b : b + 1, lanes[g]].astype(F32) for g in range(kv_count)]
        latest = jnp.concatenate([jnp.broadcast_to(v, (group, HEAD_WIDTH)) for v in latest])
        fresh[b] = jnp.sum(query * latest, axis=1, keepdims=True) * inv_root
        query = query.astype(BF16)
        for g in range(kv_count):
            at = b * head_count + g * group
            scored[at : at + group, :] = lax.dot_general(
                query[g * group : (g + 1) * group],
                keys[b, :, lanes[g]],
                (((1,), (1,)), ((), ())),
                preferred_element_type=F32,
            )

    def weigh(b):
        scores = scored[b * head_count : (b + 1) * head_count, :]
        scores = jnp.where(positions < len_ref[b], scores * inv_root, -jnp.inf)
        highest = jnp.maximum(jnp.max(scores, axis=1, keepdims=True), fresh[b])
        cached_exp = jnp.exp(scores - highest)
        fresh_exp = jnp.exp(fresh[b] - highest)
        share = 1.0 / (jnp.sum(cached_exp, axis=1, keepdims=True) + fresh_exp)
        probs[b] = (cached_exp * share).astype(BF16)
        fresh_probs[b] = (fresh_exp * share).astype(BF16).astype(F32)

    def mix(b):
        for g in range(kv_count):
            heads = slice(g * group, (g + 1) * group)
            out = jnp.dot(probs[b][heads], values[b, :, lanes[g]], preferred_element_type=F32)
            out = out + fresh_probs[b][heads] * tv_ref[b : b + 1, lanes[g]].astype(F32)
            out = pltpu.roll(out, core * (HEAD_WIDTH // 2), 1)
            for a in range(2):
                start = g * group * seq_count + a * seq_count + b
                mixed[pl.ds(start, side, stride=2 * seq_count), :] = out[a * side : (a + 1) * side]

    for copy in copies[0][:2]:
        copy.wait()
    score(0); score(1)
    for copy in copies[0][2:]:
        copy.wait()
    score(2); score(3)
    weigh(0); weigh(1)
    for copy in copies[1][:2]:
        copy.wait()
    mix(0); mix(1); weigh(2); weigh(3)
    for copy in copies[1][2:] + sliced:
        copy.wait()
    for copy in stored:
        copy.start()
    mix(2); mix(3)
    tile = 2 * seq_count
    for g in range(kv_count):
        for y in range(side):
            for part, source in enumerate((y, y ^ 1)):
                at = (g * side + source) * tile
                near = mixed[at : at + tile, :]
                far = pltpu.roll(near, seq_count, 0)
                out_ref[2 * g * side + y, :, lanes[part]] = near.astype(BF16)
                out_ref[(2 * g + 1) * side + y, :, lanes[part]] = far.astype(BF16)
        sent = pl.ds(2 * g * side, 2 * side)
        stored.append(
            pltpu.make_async_copy(out_ref.at[sent], out_hbm.at[sent], few.at[len(small) + 8 + g])
        )
        stored[-1].start()
    for copy in stored:
        copy.wait()


def attend(queries, token_keys, token_values, kv_len, stored_keys, stored_values, out_weight):
    seq_count, feature_total = queries.shape
    heads = feature_total // HEAD_WIDTH
    rows, cols = out_weight.shape
    return pl.pallas_call(
        attend_body,
        name="attend",
        out_shape=[pltpu.HBM((heads, 2 * seq_count, 2 * HEAD_WIDTH), BF16)]
        + [pltpu.HBM((rows, cols // 4), BF16)] * 4,
        in_specs=[IN_HBM] * 7,
        out_specs=[IN_HBM] * 5,
        scratch_shapes=[
            pltpu.VMEM(queries.shape, BF16),
            pltpu.VMEM(token_keys.shape, BF16),
            pltpu.VMEM(token_values.shape, BF16),
            pltpu.SMEM(kv_len.shape, jnp.int32),
            pltpu.VMEM(stored_keys.shape, BF16),
            pltpu.VMEM(stored_values.shape, BF16),
            pltpu.VMEM((4, rows, cols // 4), BF16),
            pltpu.VMEM((seq_count * heads, HEAD_WIDTH), F32),
            pltpu.VMEM((seq_count * heads, HEAD_WIDTH), F32),
            pltpu.VMEM((seq_count * heads, stored_keys.shape[1]), F32),
            pltpu.VMEM((heads, 2 * seq_count, 2 * HEAD_WIDTH), BF16),
            pltpu.SemaphoreType.DMA((2, seq_count)),
            pltpu.SemaphoreType.DMA((16,)),
        ],
        compiler_params=pltpu.CompilerParams(vmem_limit_bytes=8 * MIB),
    )(
        *map(
            in_hbm,
            (queries, token_keys, token_values, kv_len, stored_keys, stored_values, out_weight),
        )
    )


def copy_all(pairs, sems):
    copies = [pltpu.make_async_copy(*pair, sems.at[j]) for j, pair in enumerate(pairs)]
    for copy in copies:
        copy.start()
    for copy in copies:
        copy.wait()


def stack_body(*refs):
    own, other, out_ref, sems = refs[:4], refs[4:8], refs[8], refs[9]
    rows = own[0].shape[0]
    side = math.isqrt(lax.axis_size(CHIPS))
    _, ahead = square_place(lax.axis_index(CHIPS), side)
    pairs = []
    for j, d in enumerate((0, 3 - ahead, ahead, 3)):
        for half, source in enumerate((own[j], other[j])):
            at = pl.multiple_of((2 * d + half) * rows, rows)
            pairs.append((source, out_ref.at[pl.ds(at, rows)]))
    copy_all(pairs, sems)


def stack(own, other):
    rows, cols = own[0].shape
    return pl.pallas_call(
        stack_body,
        name="stack",
        out_shape=pltpu.VMEM((8 * rows, cols), BF16),
        in_specs=[IN_HBM] * 8,
        out_specs=IN_VMEM,
        scratch_shapes=[pltpu.SemaphoreType.DMA((8,))],
        compiler_params=pltpu.CompilerParams(vmem_limit_bytes=2 * MIB),
    )(*map(in_hbm, own), *map(in_hbm, other))


def halves_body(gate_hbm, up_hbm, down_hbm, kept_ref, *refs):
    outs, (tall, wide, sems) = refs[:2], refs[2:]
    core = lax.axis_index(CORES)
    count = kept_ref.shape[0]
    half, both = tall.shape
    units = both // 2
    given = pl.ds(pl.multiple_of((1 - core) * half, half), half)
    kept = pl.ds(pl.multiple_of(core * half, half), count)
    left, right = slice(0, units), slice(units, both)
    pairs = (
        (gate_hbm.at[0, given, :], tall.at[:, left]),
        (up_hbm.at[0, given, :], tall.at[:, right]),
        (down_hbm.at[0, :, given], wide),
        (gate_hbm.at[0, kept, :], kept_ref.at[:, left]),
        (up_hbm.at[0, kept, :], kept_ref.at[:, right]),
        (tall, outs[0]),
        (wide, outs[1]),
    )
    copies = [pltpu.make_async_copy(*pair, sems.at[j]) for j, pair in enumerate(pairs)]
    for copy in copies[:5]:
        copy.start()
    for copy in copies[:2]:
        copy.wait()
    copies[5].start()
    copies[2].wait()
    copies[6].start()
    for copy in copies[3:]:
        copy.wait()


def halves(w_gate, w_up, w_down, kept_share):
    _, width, units = w_gate.shape
    tall, wide = (width // 2, 2 * units), (units, width // 2)
    return pl.pallas_call(
        halves_body,
        name="halves",
        out_shape=[
            pltpu.VMEM((int(width // 2 * kept_share), 2 * units), BF16),
            pltpu.HBM(tall, BF16),
            pltpu.HBM(wide, BF16),
        ],
        in_specs=[IN_HBM] * 3,
        out_specs=[IN_VMEM] + [IN_HBM] * 2,
        scratch_shapes=[
            pltpu.VMEM(tall, BF16),
            pltpu.VMEM(wide, BF16),
            pltpu.SemaphoreType.DMA((7,)),
        ],
        compiler_params=pltpu.CompilerParams(vmem_limit_bytes=6 * MIB),
    )(*map(in_hbm, (w_gate, w_up, w_down)))


def project_body(x_ref, weight_ref, out_hbm, held, sems):
    chips, tile, width = x_ref.shape
    cols = weight_ref.shape[1]
    half = cols // 2
    step = chips // 2

    def paired(first, second):
        low = lax.broadcasted_iota(jnp.int32, first.shape, 1) < tile // 2
        return (
            jnp.where(low, first, pltpu.roll(second, tile // 2, 1)),
            jnp.where(low, pltpu.roll(first, tile // 2, 1), second),
        )

    copies = []
    shift = chips - first_member(chips)
    for j in range(2):
        sent = slice(j * step, (j + 1) * step)
        x = x_ref[sent].astype(F32).reshape(step // 2, 2, tile, width)
        x = jnp.concatenate(paired(x[:, 0], x[:, 1]), axis=2)
        x = x.reshape(step // 2 * tile, 2 * width).astype(BF16)
        sums = jnp.dot(x, weight_ref[...], preferred_element_type=F32)
        sums = sums.reshape(step // 2, tile, cols)
        sums = jnp.stack(paired(sums[:, :, :half], sums[:, :, half:]), axis=1)
        held[sent] = sums.reshape(step, tile, half).astype(BF16)
        last = min((j + 1) * step, chips - shift)
        for begin, end, to in ((j * step, last, j * step + shift), (last, (j + 1) * step, 0)):
            if end > begin:
                copies.append(
                    pltpu.make_async_copy(
                        held.at[begin:end], out_hbm.at[to : to + end - begin], sems.at[len(copies)]
                    )
                )
                copies[-1].start()
    for copy in copies:
        copy.wait()


def sending_call(body, dims, in_specs, limit, chunks):
    return pl.pallas_call(
        body,
        out_shape=pltpu.HBM(dims, BF16),
        in_specs=in_specs,
        out_specs=IN_HBM,
        scratch_shapes=[pltpu.VMEM(dims, BF16), pltpu.SemaphoreType.DMA((chunks,))],
        compiler_params=pltpu.CompilerParams(vmem_limit_bytes=limit * MIB),
    )


def project(x, weight):
    dims = x.shape[0], x.shape[1], weight.shape[1] // 2
    return sending_call(project_body, dims, [IN_VMEM] * 2, 12, 3)(
        x, in_vmem(weight)
    )


def settle_body(x_ref, residual_ref, gain_ref, hidden_ref, kept_ref, given_ref, normed):
    core = lax.axis_index(CORES)
    chips, tile, half = x_ref.shape
    side = math.isqrt(chips)
    blocks = 4
    seq_count = tile // 2
    width = residual_ref.shape[1]

    def rows_of(ref, k):
        low, high = (ref[:, (2 * k + q) * half : (2 * k + q + 1) * half].astype(F32) for q in (0, 1))
        low, high = (jnp.broadcast_to(v, (seq_count, half)) for v in (low, high))
        return jnp.concatenate([low, high])

    square = jnp.zeros((tile, 1), F32)
    for k in range(blocks):
        total = rows_of(residual_ref, k)
        for x in range(k // 2, side, 2):
            for y in range(k % 2, side, 2):
                place = (x * side + y - first_member(chips)) % chips
                total = total + x_ref[place].astype(F32)
        hidden_ref[k] = total
        square = square + jnp.sum(total * total, axis=1, keepdims=True)
    square = jnp.broadcast_to(square, (tile, HEAD_WIDTH))
    square = square + pltpu.roll(square, seq_count, 0)
    scale = lax.rsqrt(square[:, :1] / width + 1e-06)
    for k in range(blocks):
        normed[k] = (hidden_ref[k] * scale * rows_of(gain_ref, k)).astype(BF16)
    kept_ref[...] = normed[pl.ds(core * 2, 2)]
    given_ref[...] = normed[pl.ds(2 - core * 2, 2)]


def settle(x, residual, gain):
    tile, half = x.shape[1:]
    return kernel_call(
        settle_body,
        (shape(4, tile, half, dtype=F32), shape(2, tile, half), shape(2, tile, half)),
        [IN_VMEM] * 3,
        6,
        [pltpu.VMEM((4, tile, half), BF16)],
    )(x, residual, gain)


def route_body(ids_ref, weight_ref, pick_ref, mix_ref):
    core = lax.axis_index(CORES)
    tokens, topk = ids_ref.shape
    seq_count = tokens // 2
    lanes = pick_ref.shape[1]
    lane = lax.broadcasted_iota(jnp.int32, (tokens, lanes), 1)
    row = lax.broadcasted_iota(jnp.int32, (tokens, lanes), 0)
    chips = lanes // 8
    expert = lane // 8 + first_member(chips)
    expert = jnp.where(expert < chips, expert, expert - chips)
    weight = weight_ref[...]
    mixing = weight / jnp.sum(weight, axis=1, keepdims=True)
    ids = ids_ref[...]
    hit = jnp.zeros((tokens, lanes), F32)
    share = jnp.zeros((tokens, lanes), F32)
    for k in range(topk):
        same = ids[:, k : k + 1] == expert
        hit = jnp.where(same, 1.0, hit)
        share = jnp.where(same, mixing[:, k : k + 1], share)
    rank = jnp.zeros((tokens, lanes), F32)
    for t in range(tokens - 1):
        rank = rank + jnp.where(row > t, jnp.broadcast_to(hit[t : t + 1], (tokens, lanes)), 0.0)
    taken = jnp.where(rank == (lane % 2).astype(F32), hit, 0.0)
    share = share * taken
    own_low = (row < seq_count) == (core == 0)
    quarter = lane // 2 % 4
    for src in range(2):
        low = own_low if src == 0 else jnp.logical_not(own_low)
        chosen = jnp.where(low, taken, pltpu.roll(taken, seq_count, 0))
        shares = jnp.where(low, share, pltpu.roll(share, seq_count, 0))
        for kk in range(2):
            at = (src * 2 + kk) * tokens
            mine = quarter == kk * 2 + row // seq_count
            pick_ref[at : at + tokens, :] = jnp.where(mine, chosen, 0.0).astype(BF16)
            value = jnp.where(mine, shares, 0.0)
            coarse = value.astype(BF16)
            mix_ref[at : at + tokens, :] = coarse
            mix_ref[4 * tokens + at : 5 * tokens + at, :] = (value - coarse.astype(F32)).astype(BF16)


def route(expert_ids, route_weight, chips):
    tokens = expert_ids.shape[0]
    return kernel_call(
        route_body, (shape(4 * tokens, 8 * chips), shape(8 * tokens, 8 * chips)), [IN_VMEM] * 2, 4
    )(expert_ids, route_weight)


def dispatch_body(kept_ref, other_ref, pick_ref, gate_hbm, up_hbm, out_hbm, rest_ref, held, sems):
    count, both = rest_ref.shape
    units = both // 2
    half = gate_hbm.shape[1] // 2
    end = (lax.axis_index(CORES) + 1) * half
    late = pl.ds(pl.multiple_of(end - count, count), count)
    copies = [
        pltpu.make_async_copy(gate_hbm.at[0, late, :], rest_ref.at[:, :units], sems.at[2]),
        pltpu.make_async_copy(up_hbm.at[0, late, :], rest_ref.at[:, units:], sems.at[3]),
    ]
    for copy in copies:
        copy.start()
    pieces = [r[...].reshape(-1, r.shape[2]) for r in (kept_ref, other_ref)]
    tokens = jnp.concatenate(pieces)
    chips, tile, part = held.shape
    step = chips // 2
    for j in range(2):
        rows = lax.dot_general(
            pick_ref[:, j * step * tile : (j + 1) * step * tile],
            tokens,
            (((0,), (0,)), ((), ())),
            preferred_element_type=F32,
        )
        sent = slice(j * step, (j + 1) * step)
        held[sent] = rows.astype(BF16).reshape(step, tile, part)
        copies.append(pltpu.make_async_copy(held.at[sent], out_hbm.at[sent], sems.at[j]))
        copies[-1].start()
    for copy in copies:
        copy.wait()


def dispatch(kept, other, pick, w_gate, w_up, late):
    tile, part = kept.shape[1:]
    dims = pick.shape[1] // tile, tile, part
    return pl.pallas_call(
        dispatch_body,
        name="dispatch",
        out_shape=[pltpu.HBM(dims, BF16), pltpu.VMEM((late, 2 * w_gate.shape[2]), BF16)],
        in_specs=[IN_VMEM] * 3 + [IN_HBM] * 2,
        out_specs=[IN_HBM, IN_VMEM],
        scratch_shapes=[pltpu.VMEM(dims, BF16), pltpu.SemaphoreType.DMA((4,))],
        compiler_params=pltpu.CompilerParams(vmem_limit_bytes=6 * MIB),
    )(kept, other, pick, in_hbm(w_gate), in_hbm(w_up))


def slot_order(size, back=False):
    sorted_row = lax.broadcasted_iota(jnp.int32, (size, size), 1 if back else 0)
    row = lax.broadcasted_iota(jnp.int32, (size, size), 0 if back else 1)
    slot = sorted_row % (size // 4)
    quarter = sorted_row // (size // 4)
    return jnp.where(row == slot // 2 * 8 + quarter * 2 + slot % 2, 1.0, 0.0).astype(BF16)


def gate_body(x_ref, kept_ref, rest_ref, moved_ref, part_ref, sent_ref):
    chips, tile, part = x_ref.shape
    count, both = kept_ref.shape
    size = 256
    groups = chips * tile // size
    order = slot_order(size)
    slots = size // 4
    sorted_rows = []
    for g in range(groups):
        rows = x_ref[g * size // tile : (g + 1) * size // tile].reshape(size, part)
        sorted_rows.append(jnp.dot(order, rows, preferred_element_type=F32).astype(BF16))
    quarters = [
        jnp.concatenate([r[p * slots : (p + 1) * slots] for r in sorted_rows]) for p in range(4)
    ]
    x = jnp.concatenate(quarters, axis=1)
    own = jnp.dot(x[:, :count], kept_ref[...], preferred_element_type=F32)
    own = own + jnp.dot(x[:, count:], rest_ref[...], preferred_element_type=F32)
    part_ref[:, :both] = own
    sent_ref[:, both:] = own.astype(BF16)
    other = jnp.dot(x, moved_ref[...], preferred_element_type=F32)
    part_ref[:, both:] = other
    sent_ref[:, :both] = other.astype(BF16)


def gate_up(x, kept, rest, moved):
    chips, tile, _ = x.shape
    dims = chips * tile // 4, 2 * kept.shape[1]
    return pl.pallas_call(
        gate_body,
        name="gate_up",
        out_shape=[pltpu.VMEM(dims, F32), pltpu.VMEM(dims, BF16)],
        in_specs=[IN_VMEM] * 4,
        out_specs=[IN_VMEM] * 2,
        compiler_params=pltpu.CompilerParams(vmem_limit_bytes=6 * MIB),
    )(x, in_vmem(kept), in_vmem(rest), in_vmem(moved))


def fetch_body(down_hbm, after_ref, out_ref, sem):
    del after_ref
    half = out_ref.shape[1]
    kept = pl.ds(pl.multiple_of(lax.axis_index(CORES) * half, half), half)
    copy = pltpu.make_async_copy(down_hbm.at[0, :, kept], out_ref, sem)
    copy.start()
    copy.wait()


def fetch_down(w_down, after):
    _, units, width = w_down.shape
    return pl.pallas_call(
        fetch_body,
        name="fetch_down",
        out_shape=pltpu.VMEM((units, width // 2), BF16),
        in_specs=[IN_HBM] * 2,
        out_specs=IN_VMEM,
        scratch_shapes=[pltpu.SemaphoreType.DMA],
        compiler_params=pltpu.CompilerParams(vmem_limit_bytes=MIB),
    )(in_hbm(w_down), after)


def down_body(part_ref, arrived_ref, first_ref, rest_ref, out_hbm, held, sems):
    chips, tile, part = held.shape
    size = 256
    groups = chips * tile // size
    order = slot_order(size, back=True)
    slots = size // 4
    units = first_ref.shape[0]

    def act(at):
        gate, up = (
            part_ref[:, j : j + units] + arrived_ref[:, j : j + units].astype(F32)
            for j in (at, at + units)
        )
        return (gate / (1.0 + jnp.exp(-gate)) * up).astype(BF16)

    hidden = act(0), act(2 * units)
    quarters = []
    for p in range(4):
        lanes = slice(p * part, (p + 1) * part)
        value = jnp.dot(hidden[0], first_ref[:, lanes], preferred_element_type=F32)
        value = value + jnp.dot(hidden[1], rest_ref[:, lanes], preferred_element_type=F32)
        quarters.append(value.astype(BF16))
    copies = []
    for g in range(groups):
        rows = jnp.concatenate([v[g * slots : (g + 1) * slots] for v in quarters])
        rows = jnp.dot(order, rows, preferred_element_type=F32).astype(BF16)
        sent = slice(g * size // tile, (g + 1) * size // tile)
        held[sent] = rows.reshape(size // tile, tile, part)
        copies.append(pltpu.make_async_copy(held.at[sent], out_hbm.at[sent], sems.at[g]))
        copies[-1].start()
    for copy in copies:
        copy.wait()


def down(part, arrived, first, rest, tile):
    dims = part.shape[0] * 4 // tile, tile, first.shape[1] // 4
    return sending_call(down_body, dims, [IN_VMEM] * 4, 8, 2)(
        part, arrived, in_vmem(first), in_vmem(rest)
    )


def combine_body(x_ref, mix_ref, own_ref, other_ref):
    x = x_ref[...].reshape(-1, x_ref.shape[2])
    rows = jnp.dot(mix_ref[...], x, preferred_element_type=F32)
    count = rows.shape[0] // 2
    rows = rows[:count] + rows[count:]
    own_ref[...] = rows[: count // 2].reshape(own_ref.shape)
    other_ref[...] = rows[count // 2 :].reshape(other_ref.shape)


def combine(x, mix):
    out = shape(2, x.shape[1], x.shape[2], dtype=F32)
    return kernel_call(combine_body, (out, out), [IN_VMEM] * 2, 4)(x, mix)


def finish_body(hidden_ref, own_ref, other_ref, out_ref, total):
    core = lax.axis_index(CORES)
    blocks, tile, half = hidden_ref.shape
    total[pl.ds(core * 2, 2)] = own_ref[...]
    total[pl.ds(2 - core * 2, 2)] = other_ref[...]
    for k in range(blocks):
        value = (hidden_ref[k] + total[k]).astype(BF16)
        for q in range(2):
            at = (2 * k + q) * half
            out_ref[:, at : at + half] = value[q * tile // 2 : (q + 1) * tile // 2]


def finish(hidden, own, other):
    blocks, tile, half = hidden.shape
    return kernel_call(
        finish_body, shape(tile // 2, 2 * blocks * half), [IN_VMEM] * 3, 2, [pltpu.VMEM(hidden.shape, F32)]
    )(hidden, own, other)


def on_device(
    queries,
    token_keys,
    token_values,
    stored_keys,
    stored_values,
    kv_len,
    residual,
    out_weight,
    norm_gain,
    expert_ids,
    route_weight,
    w_gate,
    w_up,
    w_down,
):
    chips = lax.axis_size(CHIPS)
    side = math.isqrt(chips)
    outgoing, *pieces = attend(
        queries, token_keys, token_values, kv_len, stored_keys, stored_values, out_weight
    )
    own = pieces[:1] + [
        lax.ppermute(piece, CHIPS, square_step(side, way))
        for piece, way in zip(pieces[1:], (1, -1, 0), strict=True)
    ]
    tokens = lax.all_to_all(outgoing, CHIPS, 0, 0, tiled=True)
    other = [swapped(piece) for piece in own]
    weight = stack(own, other)
    kept, gate_given, down_given = halves(w_gate, w_up, w_down, 0.75)
    gate_moved, down_moved = swapped(gate_given), swapped(down_given)
    pick, mix = route(expert_ids, route_weight, chips)

    sums = project(tokens, weight)
    came_back = exchanged(sums)
    hidden, normed, normed_given = settle(came_back, residual, norm_gain[None])
    normed_other = swapped(normed_given)
    late = w_gate.shape[1] // 2 - kept.shape[0]
    outgoing, rest = dispatch(normed, normed_other, pick, w_gate, w_up, late)
    incoming = exchanged(outgoing)
    part, sent = gate_up(incoming, kept, rest, gate_moved)
    down_kept = fetch_down(w_down, part)
    expert_out = down(part, swapped(sent), down_kept, down_moved, incoming.shape[1])
    returned = exchanged(expert_out)
    moe_own, moe_given = combine(returned, mix)
    return finish(hidden, moe_own, swapped(moe_given))


def solution(mesh):
    in_specs = (
        P(("groups", "expert", "replica"), None),
        P(("groups", "expert", "replica"), None),
        P(("groups", "expert", "replica"), None),
        P(("groups", "expert", "replica"), None, None),
        P(("groups", "expert", "replica"), None, None),
        P(("groups", "expert", "replica")),
        P(("groups", "expert", "replica"), None),
        P(("expert", "replica"), None),
        P(),
        P(("groups", "expert"), None),
        P(("groups", "expert"), None),
        P("expert", None, "replica"),
        P("expert", None, "replica"),
        P("expert", "replica", None),
    )
    out_specs = P(("groups", "expert", "replica"), None)
    return jax.shard_map(
        on_device, mesh=mesh, in_specs=in_specs, out_specs=out_specs, check_vma=False
    )
```

```python
import math

import jax
import jax.numpy as jnp
from jax import lax
from jax.experimental import pallas as pl
from jax.experimental.pallas import tpu as pltpu
from jax.sharding import PartitionSpec as P

HEAD_WIDTH = 128
CHIPS, CORES = "expert", "replica"
F32, BF16 = jnp.float32, jnp.bfloat16
IN_VMEM = pl.BlockSpec(memory_space=pltpu.VMEM)
IN_SMEM = pl.BlockSpec(memory_space=pltpu.SMEM)
IN_HBM = pl.BlockSpec(memory_space=pltpu.HBM)


def swapped(x):
    return lax.ppermute(x, CORES, [(0, 1), (1, 0)])


def square_place(chip, side):
    x, y = chip // side % 2, chip % 2
    return x * 2 + y, 1 + (x ^ y)


def square_step(side, way):
    steps = []
    for x in range(side):
        for y in range(side):
            along_y = {1: (x ^ y) & 1 == 0, -1: (x ^ y) & 1 == 1}.get(way)
            dx, dy = (1, 1) if way == 0 else ((0, 1) if along_y else (1, 0))
            steps.append((x * side + y, (x ^ dx) * side + (y ^ dy)))
    return steps


def first_member(chips):
    return chips - 2


def exchanged(x):
    chips = lax.axis_size(CHIPS)
    members = [(k + first_member(chips)) % chips for k in range(chips)]
    return lax.all_to_all(x, CHIPS, 0, 0, tiled=True, axis_index_groups=[members])


MIB = 1 << 20


def in_hbm(x):
    return pltpu.with_memory_space_constraint(x, pltpu.HBM)


def in_vmem(x):
    return pltpu.with_memory_space_constraint(x, pltpu.VMEM)


def kernel_call(body, outs, in_specs, limit, scratch=()):
    return pl.pallas_call(
        body,
        out_shape=outs,
        in_specs=in_specs,
        out_specs=jax.tree.map(lambda _: IN_VMEM, outs),
        scratch_shapes=list(scratch),
        compiler_params=pltpu.CompilerParams(vmem_limit_bytes=limit * MIB),
    )


def shape(*dims, dtype=BF16):
    return jax.ShapeDtypeStruct(dims, dtype)


def attend_body(
    q_hbm,
    tk_hbm,
    tv_hbm,
    len_hbm,
    keys_hbm,
    values_hbm,
    weight_hbm,
    out_hbm,
    piece_own,
    piece_next,
    piece_last,
    piece_diagonal,
    q_ref,
    tk_ref,
    tv_ref,
    len_ref,
    keys,
    values,
    pieces,
    rows,
    mixed,
    scored,
    out_ref,
    sems,
    few,
):
    core = lax.axis_index(CORES)
    seq_count, cache_len, kv_width = keys_hbm.shape
    kv_count = kv_width // HEAD_WIDTH
    head_count = q_hbm.shape[1] // HEAD_WIDTH
    group = head_count // kv_count
    side = group // 2
    small = [
        pltpu.make_async_copy(source, target, few.at[j])
        for j, (source, target) in enumerate(
            ((q_hbm, q_ref), (tk_hbm, tk_ref), (tv_hbm, tv_ref), (len_hbm, len_ref))
        )
    ]
    for copy in small:
        copy.start()
    copies = [
        [pltpu.make_async_copy(source.at[b], target.at[b], sems.at[j, b]) for b in range(seq_count)]
        for j, (source, target) in enumerate(((keys_hbm, keys), (values_hbm, values)))
    ]
    for copy in copies[0] + copies[1]:
        copy.start()
    chip = lax.axis_index(CHIPS)
    place, ahead = square_place(chip, side)
    sliced, stored = [], []
    for j, (d, piece) in enumerate(
        ((0, piece_own), (ahead, piece_next), (3 - ahead, piece_last), (3, piece_diagonal))
    ):
        cols = piece.shape[1]
        at = pl.multiple_of((place ^ d) * cols, cols)
        source = weight_hbm.at[:, pl.ds(at, cols)]
        sliced.append(pltpu.make_async_copy(source, pieces.at[j], few.at[len(small) + j]))
        stored.append(pltpu.make_async_copy(pieces.at[j], piece, few.at[len(small) + 4 + j]))
        sliced[-1].start()
    for copy in small:
        copy.wait()
    for h in range(head_count):
        piece = q_ref[:, h * HEAD_WIDTH : (h + 1) * HEAD_WIDTH].astype(F32)
        rows[pl.ds(h, seq_count, stride=head_count), :] = piece
    inv_root = 1.0 / math.sqrt(HEAD_WIDTH)
    positions = lax.broadcasted_iota(jnp.int32, (head_count, cache_len), 1)
    lanes = [slice(g * HEAD_WIDTH, (g + 1) * HEAD_WIDTH) for g in range(kv_count)]
    fresh, probs, fresh_probs = {}, {}, {}

    def score(b):
        query = rows[b * head_count : (b + 1) * head_count, :]
        latest = [tk_ref[b : b + 1, lanes[g]].astype(F32) for g in range(kv_count)]
        latest = jnp.concatenate([jnp.broadcast_to(v, (group, HEAD_WIDTH)) for v in latest])
        fresh[b] = jnp.sum(query * latest, axis=1, keepdims=True) * inv_root
        query = query.astype(BF16)
        for g in range(kv_count):
            at = b * head_count + g * group
            scored[at : at + group, :] = lax.dot_general(
                query[g * group : (g + 1) * group],
                keys[b, :, lanes[g]],
                (((1,), (1,)), ((), ())),
                preferred_element_type=F32,
            )

    def weigh(b):
        scores = scored[b * head_count : (b + 1) * head_count, :]
        scores = jnp.where(positions < len_ref[b], scores * inv_root, -jnp.inf)
        highest = jnp.maximum(jnp.max(scores, axis=1, keepdims=True), fresh[b])
        cached_exp = jnp.exp(scores - highest)
        fresh_exp = jnp.exp(fresh[b] - highest)
        share = 1.0 / (jnp.sum(cached_exp, axis=1, keepdims=True) + fresh_exp)
        probs[b] = (cached_exp * share).astype(BF16)
        fresh_probs[b] = (fresh_exp * share).astype(BF16).astype(F32)

    def mix(b):
        for g in range(kv_count):
            heads = slice(g * group, (g + 1) * group)
            out = jnp.dot(probs[b][heads], values[b, :, lanes[g]], preferred_element_type=F32)
            out = out + fresh_probs[b][heads] * tv_ref[b : b + 1, lanes[g]].astype(F32)
            out = pltpu.roll(out, core * (HEAD_WIDTH // 2), 1)
            for a in range(2):
                start = g * group * seq_count + a * seq_count + b
                mixed[pl.ds(start, side, stride=2 * seq_count), :] = out[a * side : (a + 1) * side]

    for copy in copies[0][:2]:
        copy.wait()
    score(0); score(1)
    for copy in copies[0][2:]:
        copy.wait()
    score(2); score(3)
    weigh(0); weigh(1)
    for copy in copies[1][:2]:
        copy.wait()
    mix(0); mix(1); weigh(2); weigh(3)
    for copy in copies[1][2:] + sliced:
        copy.wait()
    for copy in stored:
        copy.start()
    mix(2); mix(3)
    tile = 2 * seq_count
    for g in range(kv_count):
        for y in range(side):
            for part, source in enumerate((y, y ^ 1)):
                at = (g * side + source) * tile
                near = mixed[at : at + tile, :]
                far = pltpu.roll(near, seq_count, 0)
                out_ref[2 * g * side + y, :, lanes[part]] = near.astype(BF16)
                out_ref[(2 * g + 1) * side + y, :, lanes[part]] = far.astype(BF16)
        sent = pl.ds(2 * g * side, 2 * side)
        stored.append(
            pltpu.make_async_copy(out_ref.at[sent], out_hbm.at[sent], few.at[len(small) + 8 + g])
        )
        stored[-1].start()
    for copy in stored:
        copy.wait()


def attend(queries, token_keys, token_values, kv_len, stored_keys, stored_values, out_weight):
    seq_count, feature_total = queries.shape
    heads = feature_total // HEAD_WIDTH
    rows, cols = out_weight.shape
    return pl.pallas_call(
        attend_body,
        name="attend",
        out_shape=[pltpu.HBM((heads, 2 * seq_count, 2 * HEAD_WIDTH), BF16)]
        + [pltpu.HBM((rows, cols // 4), BF16)] * 4,
        in_specs=[IN_HBM] * 7,
        out_specs=[IN_HBM] * 5,
        scratch_shapes=[
            pltpu.VMEM(queries.shape, BF16),
            pltpu.VMEM(token_keys.shape, BF16),
            pltpu.VMEM(token_values.shape, BF16),
            pltpu.SMEM(kv_len.shape, jnp.int32),
            pltpu.VMEM(stored_keys.shape, BF16),
            pltpu.VMEM(stored_values.shape, BF16),
            pltpu.VMEM((4, rows, cols // 4), BF16),
            pltpu.VMEM((seq_count * heads, HEAD_WIDTH), F32),
            pltpu.VMEM((seq_count * heads, HEAD_WIDTH), F32),
            pltpu.VMEM((seq_count * heads, stored_keys.shape[1]), F32),
            pltpu.VMEM((heads, 2 * seq_count, 2 * HEAD_WIDTH), BF16),
            pltpu.SemaphoreType.DMA((2, seq_count)),
            pltpu.SemaphoreType.DMA((16,)),
        ],
        compiler_params=pltpu.CompilerParams(vmem_limit_bytes=8 * MIB),
    )(
        *map(
            in_hbm,
            (queries, token_keys, token_values, kv_len, stored_keys, stored_values, out_weight),
        )
    )


def copy_all(pairs, sems):
    copies = [pltpu.make_async_copy(*pair, sems.at[j]) for j, pair in enumerate(pairs)]
    for copy in copies:
        copy.start()
    for copy in copies:
        copy.wait()


def stack_body(*refs):
    own, other, out_ref, sems = refs[:4], refs[4:8], refs[8], refs[9]
    rows = own[0].shape[0]
    side = math.isqrt(lax.axis_size(CHIPS))
    _, ahead = square_place(lax.axis_index(CHIPS), side)
    pairs = []
    for j, d in enumerate((0, 3 - ahead, ahead, 3)):
        for half, source in enumerate((own[j], other[j])):
            at = pl.multiple_of((2 * d + half) * rows, rows)
            pairs.append((source, out_ref.at[pl.ds(at, rows)]))
    copy_all(pairs, sems)


def stack(own, other):
    rows, cols = own[0].shape
    return pl.pallas_call(
        stack_body,
        name="stack",
        out_shape=pltpu.VMEM((8 * rows, cols), BF16),
        in_specs=[IN_HBM] * 8,
        out_specs=IN_VMEM,
        scratch_shapes=[pltpu.SemaphoreType.DMA((8,))],
        compiler_params=pltpu.CompilerParams(vmem_limit_bytes=2 * MIB),
    )(*map(in_hbm, own), *map(in_hbm, other))


def halves_body(gate_hbm, up_hbm, down_hbm, kept_ref, *refs):
    outs, (tall, wide, sems) = refs[:2], refs[2:]
    core = lax.axis_index(CORES)
    count = kept_ref.shape[0]
    half, both = tall.shape
    units = both // 2
    given = pl.ds(pl.multiple_of((1 - core) * half, half), half)
    kept = pl.ds(pl.multiple_of(core * half, half), count)
    left, right = slice(0, units), slice(units, both)
    pairs = (
        (gate_hbm.at[0, given, :], tall.at[:, left]),
        (up_hbm.at[0, given, :], tall.at[:, right]),
        (down_hbm.at[0, :, given], wide),
        (gate_hbm.at[0, kept, :], kept_ref.at[:, left]),
        (up_hbm.at[0, kept, :], kept_ref.at[:, right]),
        (tall, outs[0]),
        (wide, outs[1]),
    )
    copies = [pltpu.make_async_copy(*pair, sems.at[j]) for j, pair in enumerate(pairs)]
    for copy in copies[:5]:
        copy.start()
    for copy in copies[:2]:
        copy.wait()
    copies[5].start()
    copies[2].wait()
    copies[6].start()
    for copy in copies[3:]:
        copy.wait()


def halves(w_gate, w_up, w_down, kept_share):
    _, width, units = w_gate.shape
    tall, wide = (width // 2, 2 * units), (units, width // 2)
    return pl.pallas_call(
        halves_body,
        name="halves",
        out_shape=[
            pltpu.VMEM((int(width // 2 * kept_share), 2 * units), BF16),
            pltpu.HBM(tall, BF16),
            pltpu.HBM(wide, BF16),
        ],
        in_specs=[IN_HBM] * 3,
        out_specs=[IN_VMEM] + [IN_HBM] * 2,
        scratch_shapes=[
            pltpu.VMEM(tall, BF16),
            pltpu.VMEM(wide, BF16),
            pltpu.SemaphoreType.DMA((7,)),
        ],
        compiler_params=pltpu.CompilerParams(vmem_limit_bytes=6 * MIB),
    )(*map(in_hbm, (w_gate, w_up, w_down)))


def project_body(x_ref, weight_ref, out_hbm, held, sems):
    chips, tile, width = x_ref.shape
    cols = weight_ref.shape[1]
    half = cols // 2
    step = chips // 2

    def paired(first, second):
        low = lax.broadcasted_iota(jnp.int32, first.shape, 1) < tile // 2
        return (
            jnp.where(low, first, pltpu.roll(second, tile // 2, 1)),
            jnp.where(low, pltpu.roll(first, tile // 2, 1), second),
        )

    copies = []
    shift = chips - first_member(chips)
    for j in range(2):
        sent = slice(j * step, (j + 1) * step)
        x = x_ref[sent].astype(F32).reshape(step // 2, 2, tile, width)
        x = jnp.concatenate(paired(x[:, 0], x[:, 1]), axis=2)
        x = x.reshape(step // 2 * tile, 2 * width).astype(BF16)
        sums = jnp.dot(x, weight_ref[...], preferred_element_type=F32)
        sums = sums.reshape(step // 2, tile, cols)
        sums = jnp.stack(paired(sums[:, :, :half], sums[:, :, half:]), axis=1)
        held[sent] = sums.reshape(step, tile, half).astype(BF16)
        last = min((j + 1) * step, chips - shift)
        for begin, end, to in ((j * step, last, j * step + shift), (last, (j + 1) * step, 0)):
            if end > begin:
                copies.append(
                    pltpu.make_async_copy(
                        held.at[begin:end], out_hbm.at[to : to + end - begin], sems.at[len(copies)]
                    )
                )
                copies[-1].start()
    for copy in copies:
        copy.wait()


def sending_call(body, dims, in_specs, limit, chunks):
    return pl.pallas_call(
        body,
        out_shape=pltpu.HBM(dims, BF16),
        in_specs=in_specs,
        out_specs=IN_HBM,
        scratch_shapes=[pltpu.VMEM(dims, BF16), pltpu.SemaphoreType.DMA((chunks,))],
        compiler_params=pltpu.CompilerParams(vmem_limit_bytes=limit * MIB),
    )


def project(x, weight):
    dims = x.shape[0], x.shape[1], weight.shape[1] // 2
    return sending_call(project_body, dims, [IN_VMEM] * 2, 12, 3)(
        x, in_vmem(weight)
    )


def settle_body(x_ref, residual_ref, gain_ref, hidden_ref, kept_ref, given_ref, normed):
    core = lax.axis_index(CORES)
    chips, tile, half = x_ref.shape
    side = math.isqrt(chips)
    blocks = 4
    seq_count = tile // 2
    width = residual_ref.shape[1]

    def rows_of(ref, k):
        low, high = (ref[:, (2 * k + q) * half : (2 * k + q + 1) * half].astype(F32) for q in (0, 1))
        low, high = (jnp.broadcast_to(v, (seq_count, half)) for v in (low, high))
        return jnp.concatenate([low, high])

    square = jnp.zeros((tile, 1), F32)
    for k in range(blocks):
        total = rows_of(residual_ref, k)
        for x in range(k // 2, side, 2):
            for y in range(k % 2, side, 2):
                place = (x * side + y - first_member(chips)) % chips
                total = total + x_ref[place].astype(F32)
        hidden_ref[k] = total
        square = square + jnp.sum(total * total, axis=1, keepdims=True)
    square = jnp.broadcast_to(square, (tile, HEAD_WIDTH))
    square = square + pltpu.roll(square, seq_count, 0)
    scale = lax.rsqrt(square[:, :1] / width + 1e-06)
    for k in range(blocks):
        normed[k] = (hidden_ref[k] * scale * rows_of(gain_ref, k)).astype(BF16)
    kept_ref[...] = normed[pl.ds(core * 2, 2)]
    given_ref[...] = normed[pl.ds(2 - core * 2, 2)]


def settle(x, residual, gain):
    tile, half = x.shape[1:]
    return kernel_call(
        settle_body,
        (shape(4, tile, half, dtype=F32), shape(2, tile, half), shape(2, tile, half)),
        [IN_VMEM] * 3,
        6,
        [pltpu.VMEM((4, tile, half), BF16)],
    )(x, residual, gain)


def route_body(ids_ref, weight_ref, pick_ref, mix_ref):
    core = lax.axis_index(CORES)
    tokens, topk = ids_ref.shape
    seq_count = tokens // 2
    lanes = pick_ref.shape[1]
    lane = lax.broadcasted_iota(jnp.int32, (tokens, lanes), 1)
    row = lax.broadcasted_iota(jnp.int32, (tokens, lanes), 0)
    chips = lanes // 8
    expert = lane // 8 + first_member(chips)
    expert = jnp.where(expert < chips, expert, expert - chips)
    weight = weight_ref[...]
    mixing = weight / jnp.sum(weight, axis=1, keepdims=True)
    ids = ids_ref[...]
    hit = jnp.zeros((tokens, lanes), F32)
    share = jnp.zeros((tokens, lanes), F32)
    for k in range(topk):
        same = ids[:, k : k + 1] == expert
        hit = jnp.where(same, 1.0, hit)
        share = jnp.where(same, mixing[:, k : k + 1], share)
    rank = jnp.zeros((tokens, lanes), F32)
    for t in range(tokens - 1):
        rank = rank + jnp.where(row > t, jnp.broadcast_to(hit[t : t + 1], (tokens, lanes)), 0.0)
    taken = jnp.where(rank == (lane % 2).astype(F32), hit, 0.0)
    share = share * taken
    own_low = (row < seq_count) == (core == 0)
    quarter = lane // 2 % 4
    for src in range(2):
        low = own_low if src == 0 else jnp.logical_not(own_low)
        chosen = jnp.where(low, taken, pltpu.roll(taken, seq_count, 0))
        shares = jnp.where(low, share, pltpu.roll(share, seq_count, 0))
        for kk in range(2):
            at = (src * 2 + kk) * tokens
            mine = quarter == kk * 2 + row // seq_count
            pick_ref[at : at + tokens, :] = jnp.where(mine, chosen, 0.0).astype(BF16)
            value = jnp.where(mine, shares, 0.0)
            coarse = value.astype(BF16)
            mix_ref[at : at + tokens, :] = coarse
            mix_ref[4 * tokens + at : 5 * tokens + at, :] = (value - coarse.astype(F32)).astype(BF16)


def route(expert_ids, route_weight, chips):
    tokens = expert_ids.shape[0]
    return kernel_call(
        route_body, (shape(4 * tokens, 8 * chips), shape(8 * tokens, 8 * chips)), [IN_VMEM] * 2, 4
    )(expert_ids, route_weight)


def dispatch_body(kept_ref, other_ref, pick_ref, gate_hbm, up_hbm, out_hbm, rest_ref, held, sems):
    count, both = rest_ref.shape
    units = both // 2
    half = gate_hbm.shape[1] // 2
    end = (lax.axis_index(CORES) + 1) * half
    late = pl.ds(pl.multiple_of(end - count, count), count)
    copies = [
        pltpu.make_async_copy(gate_hbm.at[0, late, :], rest_ref.at[:, :units], sems.at[2]),
        pltpu.make_async_copy(up_hbm.at[0, late, :], rest_ref.at[:, units:], sems.at[3]),
    ]
    for copy in copies:
        copy.start()
    pieces = [r[...].reshape(-1, r.shape[2]) for r in (kept_ref, other_ref)]
    tokens = jnp.concatenate(pieces)
    chips, tile, part = held.shape
    step = chips // 2
    for j in range(2):
        rows = lax.dot_general(
            pick_ref[:, j * step * tile : (j + 1) * step * tile],
            tokens,
            (((0,), (0,)), ((), ())),
            preferred_element_type=F32,
        )
        sent = slice(j * step, (j + 1) * step)
        held[sent] = rows.astype(BF16).reshape(step, tile, part)
        copies.append(pltpu.make_async_copy(held.at[sent], out_hbm.at[sent], sems.at[j]))
        copies[-1].start()
    for copy in copies:
        copy.wait()


def dispatch(kept, other, pick, w_gate, w_up, late):
    tile, part = kept.shape[1:]
    dims = pick.shape[1] // tile, tile, part
    return pl.pallas_call(
        dispatch_body,
        name="dispatch",
        out_shape=[pltpu.HBM(dims, BF16), pltpu.VMEM((late, 2 * w_gate.shape[2]), BF16)],
        in_specs=[IN_VMEM] * 3 + [IN_HBM] * 2,
        out_specs=[IN_HBM, IN_VMEM],
        scratch_shapes=[pltpu.VMEM(dims, BF16), pltpu.SemaphoreType.DMA((4,))],
        compiler_params=pltpu.CompilerParams(vmem_limit_bytes=6 * MIB),
    )(kept, other, pick, in_hbm(w_gate), in_hbm(w_up))


def slot_order(size, back=False):
    sorted_row = lax.broadcasted_iota(jnp.int32, (size, size), 1 if back else 0)
    row = lax.broadcasted_iota(jnp.int32, (size, size), 0 if back else 1)
    slot = sorted_row % (size // 4)
    quarter = sorted_row // (size // 4)
    return jnp.where(row == slot // 2 * 8 + quarter * 2 + slot % 2, 1.0, 0.0).astype(BF16)


def gate_body(x_ref, kept_ref, rest_ref, moved_ref, part_ref, sent_ref):
    chips, tile, part = x_ref.shape
    count, both = kept_ref.shape
    size = 256
    groups = chips * tile // size
    order = slot_order(size)
    slots = size // 4
    sorted_rows = []
    for g in range(groups):
        rows = x_ref[g * size // tile : (g + 1) * size // tile].reshape(size, part)
        sorted_rows.append(jnp.dot(order, rows, preferred_element_type=F32).astype(BF16))
    quarters = [
        jnp.concatenate([r[p * slots : (p + 1) * slots] for r in sorted_rows]) for p in range(4)
    ]
    x = jnp.concatenate(quarters, axis=1)
    own = jnp.dot(x[:, :count], kept_ref[...], preferred_element_type=F32)
    own = own + jnp.dot(x[:, count:], rest_ref[...], preferred_element_type=F32)
    part_ref[:, :both] = own
    sent_ref[:, both:] = own.astype(BF16)
    other = jnp.dot(x, moved_ref[...], preferred_element_type=F32)
    part_ref[:, both:] = other
    sent_ref[:, :both] = other.astype(BF16)


def gate_up(x, kept, rest, moved):
    chips, tile, _ = x.shape
    dims = chips * tile // 4, 2 * kept.shape[1]
    return pl.pallas_call(
        gate_body,
        name="gate_up",
        out_shape=[pltpu.VMEM(dims, F32), pltpu.VMEM(dims, BF16)],
        in_specs=[IN_VMEM] * 4,
        out_specs=[IN_VMEM] * 2,
        compiler_params=pltpu.CompilerParams(vmem_limit_bytes=6 * MIB),
    )(x, in_vmem(kept), in_vmem(rest), in_vmem(moved))


def fetch_body(down_hbm, after_ref, out_ref, sem):
    del after_ref
    half = out_ref.shape[1]
    kept = pl.ds(pl.multiple_of(lax.axis_index(CORES) * half, half), half)
    copy = pltpu.make_async_copy(down_hbm.at[0, :, kept], out_ref, sem)
    copy.start()
    copy.wait()


def fetch_down(w_down, after):
    _, units, width = w_down.shape
    return pl.pallas_call(
        fetch_body,
        name="fetch_down",
        out_shape=pltpu.VMEM((units, width // 2), BF16),
        in_specs=[IN_HBM] * 2,
        out_specs=IN_VMEM,
        scratch_shapes=[pltpu.SemaphoreType.DMA],
        compiler_params=pltpu.CompilerParams(vmem_limit_bytes=MIB),
    )(in_hbm(w_down), after)


def down_body(part_ref, arrived_ref, first_ref, rest_ref, out_hbm, held, sems):
    chips, tile, part = held.shape
    size = 256
    groups = chips * tile // size
    order = slot_order(size, back=True)
    slots = size // 4
    units = first_ref.shape[0]

    def act(at):
        gate, up = (
            part_ref[:, j : j + units] + arrived_ref[:, j : j + units].astype(F32)
            for j in (at, at + units)
        )
        return (gate / (1.0 + jnp.exp(-gate)) * up).astype(BF16)

    hidden = jnp.concatenate([act(0), act(2 * units)], axis=1)
    quarters = []
    for p in range(4):
        lanes = slice(p * part, (p + 1) * part)
        weight = jnp.concatenate([first_ref[:, lanes], rest_ref[:, lanes]])
        value = jnp.dot(hidden, weight, preferred_element_type=F32)
        quarters.append(value.astype(BF16))
    copies = []
    for g in range(groups):
        rows = jnp.concatenate([v[g * slots : (g + 1) * slots] for v in quarters])
        rows = jnp.dot(order, rows, preferred_element_type=F32).astype(BF16)
        sent = slice(g * size // tile, (g + 1) * size // tile)
        held[sent] = rows.reshape(size // tile, tile, part)
        copies.append(pltpu.make_async_copy(held.at[sent], out_hbm.at[sent], sems.at[g]))
        copies[-1].start()
    for copy in copies:
        copy.wait()


def down(part, arrived, first, rest, tile):
    dims = part.shape[0] * 4 // tile, tile, first.shape[1] // 4
    return sending_call(down_body, dims, [IN_VMEM] * 4, 8, 2)(
        part, arrived, in_vmem(first), in_vmem(rest)
    )


def combine_body(x_ref, mix_ref, own_ref, other_ref):
    x = x_ref[...].reshape(-1, x_ref.shape[2])
    rows = jnp.dot(mix_ref[...], x, preferred_element_type=F32)
    count = rows.shape[0] // 2
    rows = rows[:count] + rows[count:]
    own_ref[...] = rows[: count // 2].reshape(own_ref.shape)
    other_ref[...] = rows[count // 2 :].reshape(other_ref.shape)


def combine(x, mix):
    out = shape(2, x.shape[1], x.shape[2], dtype=F32)
    return kernel_call(combine_body, (out, out), [IN_VMEM] * 2, 4)(x, mix)


def finish_body(hidden_ref, own_ref, other_ref, out_ref, total):
    core = lax.axis_index(CORES)
    blocks, tile, half = hidden_ref.shape
    total[pl.ds(core * 2, 2)] = own_ref[...]
    total[pl.ds(2 - core * 2, 2)] = other_ref[...]
    for k in range(blocks):
        value = (hidden_ref[k] + total[k]).astype(BF16)
        for q in range(2):
            at = (2 * k + q) * half
            out_ref[:, at : at + half] = value[q * tile // 2 : (q + 1) * tile // 2]


def finish(hidden, own, other):
    blocks, tile, half = hidden.shape
    return kernel_call(
        finish_body, shape(tile // 2, 2 * blocks * half), [IN_VMEM] * 3, 2, [pltpu.VMEM(hidden.shape, F32)]
    )(hidden, own, other)


def on_device(
    queries,
    token_keys,
    token_values,
    stored_keys,
    stored_values,
    kv_len,
    residual,
    out_weight,
    norm_gain,
    expert_ids,
    route_weight,
    w_gate,
    w_up,
    w_down,
):
    chips = lax.axis_size(CHIPS)
    side = math.isqrt(chips)
    outgoing, *pieces = attend(
        queries, token_keys, token_values, kv_len, stored_keys, stored_values, out_weight
    )
    own = list(pieces)
    for j, way in ((1, 1), (3, 0), (2, -1)):
        own[j] = lax.ppermute(pieces[j], CHIPS, square_step(side, way))
    tokens = lax.all_to_all(outgoing, CHIPS, 0, 0, tiled=True)
    other = [swapped(piece) for piece in own]
    weight = stack(own, other)
    kept, gate_given, down_given = halves(w_gate, w_up, w_down, 0.875)
    gate_moved, down_moved = swapped(gate_given), swapped(down_given)
    pick, mix = route(expert_ids, route_weight, chips)

    sums = project(tokens, weight)
    came_back = exchanged(sums)
    hidden, normed, normed_given = settle(came_back, residual, norm_gain[None])
    normed_other = swapped(normed_given)
    late = w_gate.shape[1] // 2 - kept.shape[0]
    outgoing, rest = dispatch(normed, normed_other, pick, w_gate, w_up, late)
    incoming = exchanged(outgoing)
    part, sent = gate_up(incoming, kept, rest, gate_moved)
    down_kept = fetch_down(w_down, part)
    expert_out = down(part, swapped(sent), down_kept, down_moved, incoming.shape[1])
    returned = exchanged(expert_out)
    moe_own, moe_given = combine(returned, mix)
    return finish(hidden, moe_own, swapped(moe_given))


def solution(mesh):
    in_specs = (
        P(("groups", "expert", "replica"), None),
        P(("groups", "expert", "replica"), None),
        P(("groups", "expert", "replica"), None),
        P(("groups", "expert", "replica"), None, None),
        P(("groups", "expert", "replica"), None, None),
        P(("groups", "expert", "replica")),
        P(("groups", "expert", "replica"), None),
        P(("expert", "replica"), None),
        P(),
        P(("groups", "expert"), None),
        P(("groups", "expert"), None),
        P("expert", None, "replica"),
        P("expert", None, "replica"),
        P("expert", "replica", None),
    )
    out_specs = P(("groups", "expert", "replica"), None)
    return jax.shard_map(
        on_device, mesh=mesh, in_specs=in_specs, out_specs=out_specs, check_vma=False
    )
```

```python
import math

import jax
import jax.numpy as jnp
from jax import lax
from jax.experimental import pallas as pl
from jax.experimental.pallas import tpu as pltpu
from jax.sharding import PartitionSpec as P

HEAD_WIDTH = 128
CHIPS, CORES = "expert", "replica"
F32, BF16 = jnp.float32, jnp.bfloat16
IN_VMEM = pl.BlockSpec(memory_space=pltpu.VMEM)
IN_SMEM = pl.BlockSpec(memory_space=pltpu.SMEM)
IN_HBM = pl.BlockSpec(memory_space=pltpu.HBM)


def swapped(x):
    return lax.ppermute(x, CORES, [(0, 1), (1, 0)])


def square_place(chip, side):
    x, y = chip // side % 2, chip % 2
    return x * 2 + y, 1 + (x ^ y)


def square_step(side, way):
    steps = []
    for x in range(side):
        for y in range(side):
            along_y = {1: (x ^ y) & 1 == 0, -1: (x ^ y) & 1 == 1}.get(way)
            dx, dy = (1, 1) if way == 0 else ((0, 1) if along_y else (1, 0))
            steps.append((x * side + y, (x ^ dx) * side + (y ^ dy)))
    return steps


def first_member(chips):
    return chips - 2


def exchanged(x):
    chips = lax.axis_size(CHIPS)
    members = [(k + first_member(chips)) % chips for k in range(chips)]
    return lax.all_to_all(x, CHIPS, 0, 0, tiled=True, axis_index_groups=[members])


MIB = 1 << 20


def in_hbm(x):
    return pltpu.with_memory_space_constraint(x, pltpu.HBM)


def in_vmem(x):
    return pltpu.with_memory_space_constraint(x, pltpu.VMEM)


def kernel_call(body, outs, in_specs, limit, scratch=()):
    return pl.pallas_call(
        body,
        out_shape=outs,
        in_specs=in_specs,
        out_specs=jax.tree.map(lambda _: IN_VMEM, outs),
        scratch_shapes=list(scratch),
        compiler_params=pltpu.CompilerParams(vmem_limit_bytes=limit * MIB),
    )


def shape(*dims, dtype=BF16):
    return jax.ShapeDtypeStruct(dims, dtype)


def attend_body(
    q_hbm,
    tk_hbm,
    tv_hbm,
    len_hbm,
    keys_hbm,
    values_hbm,
    weight_hbm,
    out_hbm,
    piece_own,
    piece_next,
    piece_last,
    piece_diagonal,
    q_ref,
    tk_ref,
    tv_ref,
    len_ref,
    keys,
    values,
    pieces,
    rows,
    mixed,
    scored,
    out_ref,
    sems,
    few,
):
    core = lax.axis_index(CORES)
    seq_count, cache_len, kv_width = keys_hbm.shape
    kv_count = kv_width // HEAD_WIDTH
    head_count = q_hbm.shape[1] // HEAD_WIDTH
    group = head_count // kv_count
    side = group // 2
    small = [
        pltpu.make_async_copy(source, target, few.at[j])
        for j, (source, target) in enumerate(
            ((q_hbm, q_ref), (tk_hbm, tk_ref), (tv_hbm, tv_ref), (len_hbm, len_ref))
        )
    ]
    for copy in small:
        copy.start()
    copies = [
        [pltpu.make_async_copy(source.at[b], target.at[b], sems.at[j, b]) for b in range(seq_count)]
        for j, (source, target) in enumerate(((keys_hbm, keys), (values_hbm, values)))
    ]
    for copy in copies[0] + copies[1]:
        copy.start()
    chip = lax.axis_index(CHIPS)
    place, ahead = square_place(chip, side)
    sliced, stored = [], []
    for j, (d, piece) in enumerate(
        ((0, piece_own), (ahead, piece_next), (3 - ahead, piece_last), (3, piece_diagonal))
    ):
        cols = piece.shape[1]
        at = pl.multiple_of((place ^ d) * cols, cols)
        source = weight_hbm.at[:, pl.ds(at, cols)]
        sliced.append(pltpu.make_async_copy(source, pieces.at[j], few.at[len(small) + j]))
        stored.append(pltpu.make_async_copy(pieces.at[j], piece, few.at[len(small) + 4 + j]))
        sliced[-1].start()
    for copy in small:
        copy.wait()
    for h in range(head_count):
        piece = q_ref[:, h * HEAD_WIDTH : (h + 1) * HEAD_WIDTH].astype(F32)
        rows[pl.ds(h, seq_count, stride=head_count), :] = piece
    inv_root = 1.0 / math.sqrt(HEAD_WIDTH)
    positions = lax.broadcasted_iota(jnp.int32, (head_count, cache_len), 1)
    lanes = [slice(g * HEAD_WIDTH, (g + 1) * HEAD_WIDTH) for g in range(kv_count)]
    fresh, probs, fresh_probs = {}, {}, {}

    def score(b):
        query = rows[b * head_count : (b + 1) * head_count, :]
        latest = [tk_ref[b : b + 1, lanes[g]].astype(F32) for g in range(kv_count)]
        latest = jnp.concatenate([jnp.broadcast_to(v, (group, HEAD_WIDTH)) for v in latest])
        fresh[b] = jnp.sum(query * latest, axis=1, keepdims=True) * inv_root
        query = query.astype(BF16)
        for g in range(kv_count):
            at = b * head_count + g * group
            scored[at : at + group, :] = lax.dot_general(
                query[g * group : (g + 1) * group],
                keys[b, :, lanes[g]],
                (((1,), (1,)), ((), ())),
                preferred_element_type=F32,
            )

    def weigh(b):
        scores = scored[b * head_count : (b + 1) * head_count, :]
        scores = jnp.where(positions < len_ref[b], scores * inv_root, -jnp.inf)
        highest = jnp.maximum(jnp.max(scores, axis=1, keepdims=True), fresh[b])
        cached_exp = jnp.exp(scores - highest)
        fresh_exp = jnp.exp(fresh[b] - highest)
        share = 1.0 / (jnp.sum(cached_exp, axis=1, keepdims=True) + fresh_exp)
        probs[b] = (cached_exp * share).astype(BF16)
        fresh_probs[b] = (fresh_exp * share).astype(BF16).astype(F32)

    def mix(b):
        for g in range(kv_count):
            heads = slice(g * group, (g + 1) * group)
            out = jnp.dot(probs[b][heads], values[b, :, lanes[g]], preferred_element_type=F32)
            out = out + fresh_probs[b][heads] * tv_ref[b : b + 1, lanes[g]].astype(F32)
            out = pltpu.roll(out, core * (HEAD_WIDTH // 2), 1)
            for a in range(2):
                start = g * group * seq_count + a * seq_count + b
                mixed[pl.ds(start, side, stride=2 * seq_count), :] = out[a * side : (a + 1) * side]

    for copy in copies[0][:2]:
        copy.wait()
    score(0); score(1)
    for copy in copies[0][2:]:
        copy.wait()
    score(2); score(3)
    weigh(0); weigh(1)
    for copy in copies[1][:2]:
        copy.wait()
    mix(0); mix(1); weigh(2); weigh(3)
    for copy in copies[1][2:] + sliced:
        copy.wait()
    for copy in stored:
        copy.start()
    mix(2); mix(3)
    tile = 2 * seq_count
    for g in range(kv_count):
        for y in range(side):
            for part, source in enumerate((y, y ^ 1)):
                at = (g * side + source) * tile
                near = mixed[at : at + tile, :]
                far = pltpu.roll(near, seq_count, 0)
                out_ref[2 * g * side + y, :, lanes[part]] = near.astype(BF16)
                out_ref[(2 * g + 1) * side + y, :, lanes[part]] = far.astype(BF16)
        sent = pl.ds(2 * g * side, 2 * side)
        stored.append(
            pltpu.make_async_copy(out_ref.at[sent], out_hbm.at[sent], few.at[len(small) + 8 + g])
        )
        stored[-1].start()
    for copy in stored:
        copy.wait()


def attend(queries, token_keys, token_values, kv_len, stored_keys, stored_values, out_weight):
    seq_count, feature_total = queries.shape
    heads = feature_total // HEAD_WIDTH
    rows, cols = out_weight.shape
    return pl.pallas_call(
        attend_body,
        name="attend",
        out_shape=[pltpu.HBM((heads, 2 * seq_count, 2 * HEAD_WIDTH), BF16)]
        + [pltpu.HBM((rows, cols // 4), BF16)] * 4,
        in_specs=[IN_HBM] * 7,
        out_specs=[IN_HBM] * 5,
        scratch_shapes=[
            pltpu.VMEM(queries.shape, BF16),
            pltpu.VMEM(token_keys.shape, BF16),
            pltpu.VMEM(token_values.shape, BF16),
            pltpu.SMEM(kv_len.shape, jnp.int32),
            pltpu.VMEM(stored_keys.shape, BF16),
            pltpu.VMEM(stored_values.shape, BF16),
            pltpu.VMEM((4, rows, cols // 4), BF16),
            pltpu.VMEM((seq_count * heads, HEAD_WIDTH), F32),
            pltpu.VMEM((seq_count * heads, HEAD_WIDTH), F32),
            pltpu.VMEM((seq_count * heads, stored_keys.shape[1]), F32),
            pltpu.VMEM((heads, 2 * seq_count, 2 * HEAD_WIDTH), BF16),
            pltpu.SemaphoreType.DMA((2, seq_count)),
            pltpu.SemaphoreType.DMA((16,)),
        ],
        compiler_params=pltpu.CompilerParams(vmem_limit_bytes=8 * MIB),
    )(
        *map(
            in_hbm,
            (queries, token_keys, token_values, kv_len, stored_keys, stored_values, out_weight),
        )
    )


def copy_all(pairs, sems):
    copies = [pltpu.make_async_copy(*pair, sems.at[j]) for j, pair in enumerate(pairs)]
    for copy in copies:
        copy.start()
    for copy in copies:
        copy.wait()


def stack_body(*refs):
    own, other, out_ref, sems = refs[:4], refs[4:8], refs[8], refs[9]
    rows = own[0].shape[0]
    side = math.isqrt(lax.axis_size(CHIPS))
    _, ahead = square_place(lax.axis_index(CHIPS), side)
    pairs = []
    for j, d in enumerate((0, 3 - ahead, ahead, 3)):
        for half, source in enumerate((own[j], other[j])):
            at = pl.multiple_of((2 * d + half) * rows, rows)
            pairs.append((source, out_ref.at[pl.ds(at, rows)]))
    copy_all(pairs, sems)


def stack(own, other):
    rows, cols = own[0].shape
    return pl.pallas_call(
        stack_body,
        name="stack",
        out_shape=pltpu.VMEM((8 * rows, cols), BF16),
        in_specs=[IN_HBM] * 8,
        out_specs=IN_VMEM,
        scratch_shapes=[pltpu.SemaphoreType.DMA((8,))],
        compiler_params=pltpu.CompilerParams(vmem_limit_bytes=2 * MIB),
    )(*map(in_hbm, own), *map(in_hbm, other))


def halves_body(gate_hbm, up_hbm, down_hbm, kept_ref, *refs):
    outs, (tall, wide, sems) = refs[:2], refs[2:]
    core = lax.axis_index(CORES)
    count = kept_ref.shape[0]
    half, both = tall.shape
    units = both // 2
    given = pl.ds(pl.multiple_of((1 - core) * half, half), half)
    kept = pl.ds(pl.multiple_of(core * half, half), count)
    left, right = slice(0, units), slice(units, both)
    pairs = (
        (gate_hbm.at[0, given, :], tall.at[:, left]),
        (up_hbm.at[0, given, :], tall.at[:, right]),
        (down_hbm.at[0, :, given], wide),
        (gate_hbm.at[0, kept, :], kept_ref.at[:, left]),
        (up_hbm.at[0, kept, :], kept_ref.at[:, right]),
        (tall, outs[0]),
        (wide, outs[1]),
    )
    copies = [pltpu.make_async_copy(*pair, sems.at[j]) for j, pair in enumerate(pairs)]
    for copy in copies[:5]:
        copy.start()
    for copy in copies[:2]:
        copy.wait()
    copies[5].start()
    copies[2].wait()
    copies[6].start()
    for copy in copies[3:]:
        copy.wait()


def halves(w_gate, w_up, w_down, kept_share):
    _, width, units = w_gate.shape
    tall, wide = (width // 2, 2 * units), (units, width // 2)
    return pl.pallas_call(
        halves_body,
        name="halves",
        out_shape=[
            pltpu.VMEM((int(width // 2 * kept_share), 2 * units), BF16),
            pltpu.HBM(tall, BF16),
            pltpu.HBM(wide, BF16),
        ],
        in_specs=[IN_HBM] * 3,
        out_specs=[IN_VMEM] + [IN_HBM] * 2,
        scratch_shapes=[
            pltpu.VMEM(tall, BF16),
            pltpu.VMEM(wide, BF16),
            pltpu.SemaphoreType.DMA((7,)),
        ],
        compiler_params=pltpu.CompilerParams(vmem_limit_bytes=6 * MIB),
    )(*map(in_hbm, (w_gate, w_up, w_down)))


def project_body(x_ref, weight_ref, out_hbm, held, sems):
    chips, tile, width = x_ref.shape
    cols = weight_ref.shape[1]
    half = cols // 2
    step = chips // 2

    def paired(first, second):
        low = lax.broadcasted_iota(jnp.int32, first.shape, 1) < tile // 2
        return (
            jnp.where(low, first, pltpu.roll(second, tile // 2, 1)),
            jnp.where(low, pltpu.roll(first, tile // 2, 1), second),
        )

    copies = []
    shift = chips - first_member(chips)
    for j in range(2):
        sent = slice(j * step, (j + 1) * step)
        x = x_ref[sent].astype(F32).reshape(step // 2, 2, tile, width)
        x = jnp.concatenate(paired(x[:, 0], x[:, 1]), axis=2)
        x = x.reshape(step // 2 * tile, 2 * width).astype(BF16)
        sums = jnp.dot(x, weight_ref[...], preferred_element_type=F32)
        sums = sums.reshape(step // 2, tile, cols)
        sums = jnp.stack(paired(sums[:, :, :half], sums[:, :, half:]), axis=1)
        held[sent] = sums.reshape(step, tile, half).astype(BF16)
        last = min((j + 1) * step, chips - shift)
        for begin, end, to in ((j * step, last, j * step + shift), (last, (j + 1) * step, 0)):
            if end > begin:
                copies.append(
                    pltpu.make_async_copy(
                        held.at[begin:end], out_hbm.at[to : to + end - begin], sems.at[len(copies)]
                    )
                )
                copies[-1].start()
    for copy in copies:
        copy.wait()


def sending_call(body, dims, in_specs, limit, chunks):
    return pl.pallas_call(
        body,
        out_shape=pltpu.HBM(dims, BF16),
        in_specs=in_specs,
        out_specs=IN_HBM,
        scratch_shapes=[pltpu.VMEM(dims, BF16), pltpu.SemaphoreType.DMA((chunks,))],
        compiler_params=pltpu.CompilerParams(vmem_limit_bytes=limit * MIB),
    )


def project(x, weight):
    dims = x.shape[0], x.shape[1], weight.shape[1] // 2
    return sending_call(project_body, dims, [IN_VMEM] * 2, 12, 3)(
        x, in_vmem(weight)
    )


def settle_body(x_ref, residual_ref, gain_ref, hidden_ref, kept_ref, given_ref, normed):
    core = lax.axis_index(CORES)
    chips, tile, half = x_ref.shape
    side = math.isqrt(chips)
    blocks = 4
    seq_count = tile // 2
    width = residual_ref.shape[1]

    def rows_of(ref, k):
        low, high = (ref[:, (2 * k + q) * half : (2 * k + q + 1) * half].astype(F32) for q in (0, 1))
        low, high = (jnp.broadcast_to(v, (seq_count, half)) for v in (low, high))
        return jnp.concatenate([low, high])

    square = jnp.zeros((tile, 1), F32)
    for k in range(blocks):
        total = rows_of(residual_ref, k)
        for x in range(k // 2, side, 2):
            for y in range(k % 2, side, 2):
                place = (x * side + y - first_member(chips)) % chips
                total = total + x_ref[place].astype(F32)
        hidden_ref[k] = total
        square = square + jnp.sum(total * total, axis=1, keepdims=True)
    square = jnp.broadcast_to(square, (tile, HEAD_WIDTH))
    square = square + pltpu.roll(square, seq_count, 0)
    scale = lax.rsqrt(square[:, :1] / width + 1e-06)
    for k in range(blocks):
        normed[k] = (hidden_ref[k] * scale * rows_of(gain_ref, k)).astype(BF16)
    kept_ref[...] = normed[pl.ds(core * 2, 2)]
    given_ref[...] = normed[pl.ds(2 - core * 2, 2)]


def settle(x, residual, gain):
    tile, half = x.shape[1:]
    return kernel_call(
        settle_body,
        (shape(4, tile, half, dtype=F32), shape(2, tile, half), shape(2, tile, half)),
        [IN_VMEM] * 3,
        6,
        [pltpu.VMEM((4, tile, half), BF16)],
    )(x, residual, gain)


def route_body(ids_ref, weight_ref, pick_ref, mix_ref):
    core = lax.axis_index(CORES)
    tokens, topk = ids_ref.shape
    seq_count = tokens // 2
    lanes = pick_ref.shape[1]
    lane = lax.broadcasted_iota(jnp.int32, (tokens, lanes), 1)
    row = lax.broadcasted_iota(jnp.int32, (tokens, lanes), 0)
    chips = lanes // 8
    expert = lane // 8 + first_member(chips)
    expert = jnp.where(expert < chips, expert, expert - chips)
    weight = weight_ref[...]
    mixing = weight / jnp.sum(weight, axis=1, keepdims=True)
    ids = ids_ref[...]
    hit = jnp.zeros((tokens, lanes), F32)
    share = jnp.zeros((tokens, lanes), F32)
    for k in range(topk):
        same = ids[:, k : k + 1] == expert
        hit = jnp.where(same, 1.0, hit)
        share = jnp.where(same, mixing[:, k : k + 1], share)
    rank = jnp.zeros((tokens, lanes), F32)
    for t in range(tokens - 1):
        rank = rank + jnp.where(row > t, jnp.broadcast_to(hit[t : t + 1], (tokens, lanes)), 0.0)
    taken = jnp.where(rank == (lane % 2).astype(F32), hit, 0.0)
    share = share * taken
    own_low = (row < seq_count) == (core == 0)
    quarter = lane // 2 % 4
    for src in range(2):
        low = own_low if src == 0 else jnp.logical_not(own_low)
        chosen = jnp.where(low, taken, pltpu.roll(taken, seq_count, 0))
        shares = jnp.where(low, share, pltpu.roll(share, seq_count, 0))
        for kk in range(2):
            at = (src * 2 + kk) * tokens
            mine = quarter == kk * 2 + row // seq_count
            pick_ref[at : at + tokens, :] = jnp.where(mine, chosen, 0.0).astype(BF16)
            value = jnp.where(mine, shares, 0.0)
            coarse = value.astype(BF16)
            mix_ref[at : at + tokens, :] = coarse
            mix_ref[4 * tokens + at : 5 * tokens + at, :] = (value - coarse.astype(F32)).astype(BF16)


def route(expert_ids, route_weight, chips):
    tokens = expert_ids.shape[0]
    return kernel_call(
        route_body, (shape(4 * tokens, 8 * chips), shape(8 * tokens, 8 * chips)), [IN_VMEM] * 2, 4
    )(expert_ids, route_weight)


def dispatch_body(kept_ref, other_ref, pick_ref, gate_hbm, up_hbm, out_hbm, rest_ref, held, sems):
    count, both = rest_ref.shape
    units = both // 2
    half = gate_hbm.shape[1] // 2
    end = (lax.axis_index(CORES) + 1) * half
    late = pl.ds(pl.multiple_of(end - count, count), count)
    copies = [
        pltpu.make_async_copy(gate_hbm.at[0, late, :], rest_ref.at[:, :units], sems.at[2]),
        pltpu.make_async_copy(up_hbm.at[0, late, :], rest_ref.at[:, units:], sems.at[3]),
    ]
    for copy in copies:
        copy.start()
    pieces = [r[...].reshape(-1, r.shape[2]) for r in (kept_ref, other_ref)]
    tokens = jnp.concatenate(pieces)
    chips, tile, part = held.shape
    step = chips // 2
    for j in range(2):
        rows = lax.dot_general(
            pick_ref[:, j * step * tile : (j + 1) * step * tile],
            tokens,
            (((0,), (0,)), ((), ())),
            preferred_element_type=F32,
        )
        sent = slice(j * step, (j + 1) * step)
        held[sent] = rows.astype(BF16).reshape(step, tile, part)
        copies.append(pltpu.make_async_copy(held.at[sent], out_hbm.at[sent], sems.at[j]))
        copies[-1].start()
    for copy in copies:
        copy.wait()


def dispatch(kept, other, pick, w_gate, w_up, late):
    tile, part = kept.shape[1:]
    dims = pick.shape[1] // tile, tile, part
    return pl.pallas_call(
        dispatch_body,
        name="dispatch",
        out_shape=[pltpu.HBM(dims, BF16), pltpu.VMEM((late, 2 * w_gate.shape[2]), BF16)],
        in_specs=[IN_VMEM] * 3 + [IN_HBM] * 2,
        out_specs=[IN_HBM, IN_VMEM],
        scratch_shapes=[pltpu.VMEM(dims, BF16), pltpu.SemaphoreType.DMA((4,))],
        compiler_params=pltpu.CompilerParams(vmem_limit_bytes=6 * MIB),
    )(kept, other, pick, in_hbm(w_gate), in_hbm(w_up))


def slot_order(size, back=False):
    sorted_row = lax.broadcasted_iota(jnp.int32, (size, size), 1 if back else 0)
    row = lax.broadcasted_iota(jnp.int32, (size, size), 0 if back else 1)
    slot = sorted_row % (size // 4)
    quarter = sorted_row // (size // 4)
    return jnp.where(row == slot // 2 * 8 + quarter * 2 + slot % 2, 1.0, 0.0).astype(BF16)


def gate_body(x_ref, kept_ref, rest_ref, moved_ref, part_ref, sent_ref):
    chips, tile, part = x_ref.shape
    count, both = kept_ref.shape
    size = 256
    groups = chips * tile // size
    order = slot_order(size)
    slots = size // 4
    sorted_rows = []
    for g in range(groups):
        rows = x_ref[g * size // tile : (g + 1) * size // tile].reshape(size, part)
        sorted_rows.append(jnp.dot(order, rows, preferred_element_type=F32).astype(BF16))
    quarters = [
        jnp.concatenate([r[p * slots : (p + 1) * slots] for r in sorted_rows]) for p in range(4)
    ]
    x = jnp.concatenate(quarters, axis=1)
    own = jnp.dot(x[:, :count], kept_ref[...], preferred_element_type=F32)
    own = own + jnp.dot(x[:, count:], rest_ref[...], preferred_element_type=F32)
    part_ref[:, :both] = own
    sent_ref[:, both:] = own.astype(BF16)
    other = jnp.dot(x, moved_ref[...], preferred_element_type=F32)
    part_ref[:, both:] = other
    sent_ref[:, :both] = other.astype(BF16)


def gate_up(x, kept, rest, moved):
    chips, tile, _ = x.shape
    dims = chips * tile // 4, 2 * kept.shape[1]
    return pl.pallas_call(
        gate_body,
        name="gate_up",
        out_shape=[pltpu.VMEM(dims, F32), pltpu.VMEM(dims, BF16)],
        in_specs=[IN_VMEM] * 4,
        out_specs=[IN_VMEM] * 2,
        compiler_params=pltpu.CompilerParams(vmem_limit_bytes=6 * MIB),
    )(x, in_vmem(kept), in_vmem(rest), in_vmem(moved))


def fetch_body(down_hbm, after_ref, out_ref, sem):
    del after_ref
    half = out_ref.shape[1]
    kept = pl.ds(pl.multiple_of(lax.axis_index(CORES) * half, half), half)
    copy = pltpu.make_async_copy(down_hbm.at[0, :, kept], out_ref, sem)
    copy.start()
    copy.wait()


def fetch_down(w_down, after):
    _, units, width = w_down.shape
    return pl.pallas_call(
        fetch_body,
        name="fetch_down",
        out_shape=pltpu.VMEM((units, width // 2), BF16),
        in_specs=[IN_HBM] * 2,
        out_specs=IN_VMEM,
        scratch_shapes=[pltpu.SemaphoreType.DMA],
        compiler_params=pltpu.CompilerParams(vmem_limit_bytes=MIB),
    )(in_hbm(w_down), after)


def down_body(part_ref, arrived_ref, first_ref, rest_ref, out_hbm, held, sems):
    chips, tile, part = held.shape
    size = 256
    groups = chips * tile // size
    order = slot_order(size, back=True)
    slots = size // 4
    units = first_ref.shape[0]

    def act(at):
        gate, up = (
            part_ref[:, j : j + units] + arrived_ref[:, j : j + units].astype(F32)
            for j in (at, at + units)
        )
        return (gate / (1.0 + jnp.exp(-gate)) * up).astype(BF16)

    hidden = jnp.concatenate([act(0), act(2 * units)], axis=1)
    quarters = []
    for p in range(4):
        lanes = slice(p * part, (p + 1) * part)
        weight = jnp.concatenate([first_ref[:, lanes], rest_ref[:, lanes]])
        value = jnp.dot(hidden, weight, preferred_element_type=F32)
        quarters.append(value.astype(BF16))
    copies = []
    for g in range(groups):
        rows = jnp.concatenate([v[g * slots : (g + 1) * slots] for v in quarters])
        rows = jnp.dot(order, rows, preferred_element_type=F32).astype(BF16)
        sent = slice(g * size // tile, (g + 1) * size // tile)
        held[sent] = rows.reshape(size // tile, tile, part)
        copies.append(pltpu.make_async_copy(held.at[sent], out_hbm.at[sent], sems.at[g]))
        copies[-1].start()
    for copy in copies:
        copy.wait()


def down(part, arrived, first, rest, tile):
    dims = part.shape[0] * 4 // tile, tile, first.shape[1] // 4
    return sending_call(down_body, dims, [IN_VMEM] * 4, 8, 2)(
        part, arrived, in_vmem(first), in_vmem(rest)
    )


def combine_body(x_ref, mix_ref, own_ref, other_ref):
    x = x_ref[...].reshape(-1, x_ref.shape[2])
    rows = jnp.dot(mix_ref[...], x, preferred_element_type=F32)
    count = rows.shape[0] // 2
    rows = rows[:count] + rows[count:]
    own_ref[...] = rows[: count // 2].reshape(own_ref.shape)
    other_ref[...] = rows[count // 2 :].reshape(other_ref.shape)


def combine(x, mix):
    out = shape(2, x.shape[1], x.shape[2], dtype=F32)
    return kernel_call(combine_body, (out, out), [IN_VMEM] * 2, 4)(x, mix)


def finish_body(hidden_ref, own_ref, other_ref, out_ref, total):
    core = lax.axis_index(CORES)
    blocks, tile, half = hidden_ref.shape
    total[pl.ds(core * 2, 2)] = own_ref[...]
    total[pl.ds(2 - core * 2, 2)] = other_ref[...]
    for k in range(blocks):
        value = (hidden_ref[k] + total[k]).astype(BF16)
        for q in range(2):
            at = (2 * k + q) * half
            out_ref[:, at : at + half] = value[q * tile // 2 : (q + 1) * tile // 2]


def finish(hidden, own, other):
    blocks, tile, half = hidden.shape
    return kernel_call(
        finish_body, shape(tile // 2, 2 * blocks * half), [IN_VMEM] * 3, 2, [pltpu.VMEM(hidden.shape, F32)]
    )(hidden, own, other)


def on_device(
    queries,
    token_keys,
    token_values,
    stored_keys,
    stored_values,
    kv_len,
    residual,
    out_weight,
    norm_gain,
    expert_ids,
    route_weight,
    w_gate,
    w_up,
    w_down,
):
    chips = lax.axis_size(CHIPS)
    side = math.isqrt(chips)
    outgoing, *pieces = attend(
        queries, token_keys, token_values, kv_len, stored_keys, stored_values, out_weight
    )
    own = pieces[:1] + [
        lax.ppermute(piece, CHIPS, square_step(side, way))
        for piece, way in zip(pieces[1:], (1, -1, 0), strict=True)
    ]
    tokens = lax.all_to_all(outgoing, CHIPS, 0, 0, tiled=True)
    other = [swapped(piece) for piece in own]
    weight = stack(own, other)
    kept, gate_given, down_given = halves(w_gate, w_up, w_down, 0.75)
    gate_moved, down_moved = swapped(gate_given), swapped(down_given)
    pick, mix = route(expert_ids, route_weight, chips)

    sums = project(tokens, weight)
    came_back = exchanged(sums)
    hidden, normed, normed_given = settle(came_back, residual, norm_gain[None])
    normed_other = swapped(normed_given)
    late = w_gate.shape[1] // 2 - kept.shape[0]
    outgoing, rest = dispatch(normed, normed_other, pick, w_gate, w_up, late)
    incoming = exchanged(outgoing)
    part, sent = gate_up(incoming, kept, rest, gate_moved)
    down_kept = fetch_down(w_down, part)
    expert_out = down(part, swapped(sent), down_kept, down_moved, incoming.shape[1])
    returned = exchanged(expert_out)
    moe_own, moe_given = combine(returned, mix)
    return finish(hidden, moe_own, swapped(moe_given))


def solution(mesh):
    in_specs = (
        P(("groups", "expert", "replica"), None),
        P(("groups", "expert", "replica"), None),
        P(("groups", "expert", "replica"), None),
        P(("groups", "expert", "replica"), None, None),
        P(("groups", "expert", "replica"), None, None),
        P(("groups", "expert", "replica")),
        P(("groups", "expert", "replica"), None),
        P(("expert", "replica"), None),
        P(),
        P(("groups", "expert"), None),
        P(("groups", "expert"), None),
        P("expert", None, "replica"),
        P("expert", None, "replica"),
        P("expert", "replica", None),
    )
    out_specs = P(("groups", "expert", "replica"), None)
    return jax.shard_map(
        on_device, mesh=mesh, in_specs=in_specs, out_specs=out_specs, check_vma=False
    )
```
